256 devices in a mesh: space: 128 (over x, y, z), slab: 2 (over core).
Axes of the slice: x: 4, y: 4, z: 8, core: 2. Of those that a mesh axis runs over, the one named last changes fastest.
Arguments:
- phases: float32 [8, 1536, 24, 384], P(None, 'space', 'slab'), may hold values from 0 to 1
- mobility: float32 [8], replicated, may hold values from 0.02 to 0.08
- active: int32 [128, 2, 32, 8], P('space', 'slab'), may hold values from 0 to 1, as said below
- variants: float32 [8, 3], replicated, may hold values from -4 to 4
Outputs:
- evolved: float32 [8, 1536, 24, 384], P(None, 'space', 'slab')
- displacement: float32 [3, 384, 24, 1536], P(None, 'space', 'slab')
The draws below stay inside these ranges and needn't reach their ends.
Inputs may be any that keep to these rules, and one draw needn't show every extreme that they name: 1 marks an order parameter that evolves in that brick; the share of active ones differs strongly between brick indices along the first dimension.
All inputs are finite; a program needn't handle non-finite values.
Results may differ from the reference program's by a relative error of at most 0.00016.
Values sent between devices are 32-bit elements; how exact they have to be, the bound alone decides.
No kernel may reach another device: no remote copies, remote signals or barrier semaphores. Data moves between devices by JAX's collectives and lax.ppermute only.
A program may use at most 128 MiB of HBM per device.

```python
import math
import jax
import jax.numpy as jnp
from jax import lax

P_SIZE = 8
BRICK = 12
STEPS = 3
ITERS = 4
NI = 1536
NJ = 24
NK = 384


def draw_active(key, part):
    rows_first = NI // BRICK
    rows_second = NJ // BRICK
    rows_third = NK // BRICK
    order_key, score_key = jax.random.split(jax.random.fold_in(key, 7))
    ranking = jax.random.permutation(order_key, rows_first).astype(jnp.int32)
    highest = max(rows_first - 1, 1)
    cutoff = 50 + 950 * (ranking * ranking // highest) * ranking // highest // highest
    scores = jax.random.randint(score_key, (rows_first, rows_second, rows_third, P_SIZE), 0, 1000)
    return (scores < cutoff[:, None, None, None]).astype(jnp.int32)


def block_scale(rng, shape, pieces, smallest, high):
    def one(axis_at, shards_of):
        draws = jax.random.uniform(jax.random.fold_in(jax.random.fold_in(rng, 6), axis_at), (shards_of,), jnp.float32, smallest / len(pieces), high / len(pieces))
        return jnp.repeat(jnp.exp(draws), shape[axis_at] // shards_of).reshape((-1,) + (1,) * (len(shape) - axis_at - 1))

    loudness = one(*pieces[0])
    for cut in pieces[1:]:
        loudness = loudness * one(*cut)
    return loudness


def normal_values(key, extent, spread, most, held_as=jnp.bfloat16):
    return jnp.clip(spread * jax.random.normal(key, extent, jnp.float32), -most, most).astype(held_as)


def setup_inputs(seed: int = 0) -> dict:
    arg_keys = jax.random.split(jax.random.key(seed), 5)
    phases = jnp.clip(1.0 * jax.random.uniform(arg_keys[0], (P_SIZE, NI, NJ, NK), jnp.float32) ** block_scale(arg_keys[0], (P_SIZE, NI, NJ, NK), ((1, 128), (2, 2)), -0.2, 0.2), 0.0, 1.0)
    mobility = jnp.clip(jnp.exp(jax.random.uniform(arg_keys[1], (P_SIZE,), jnp.float32, math.log(0.02), math.log(0.08))), 0.02, 0.08)
    active = draw_active(jax.random.fold_in(arg_keys[4], 71), 0)
    variants = normal_values(arg_keys[3], (P_SIZE, 3), 1.0, 4.0, jnp.float32)
    return {"phases": phases, "mobility": mobility, "active": active, "variants": variants}


PAIR_ENERGY = 1.5
DIAGONAL_SHIFT = 3.0
SPECTRUM_CENTRE = 12.0
SPECTRUM_RADIUS = 9.0


def relax(fields, padded, speeds):
    summed = (padded[:, 2:, 1:-1, 1:-1] + padded[:, :-2, 1:-1, 1:-1] + padded[:, 1:-1, 2:, 1:-1]
              + padded[:, 1:-1, :-2, 1:-1] + padded[:, 1:-1, 1:-1, 2:] + padded[:, 1:-1, 1:-1, :-2])
    laplace = summed - 6.0 * fields
    squares = jnp.sum(fields * fields, axis=0)
    driving = fields * fields * fields - fields + 2.0 * PAIR_ENERGY * fields * (squares - fields * fields) - laplace
    return fields - speeds * driving


def coefficients(fields, variants):
    squared = fields * fields
    summed = jnp.sum(squared, axis=0)
    saturation = summed / (1.0 + summed)
    excess = 0.5 * saturation
    lame_first = 1.5 + saturation
    strain = jnp.einsum("pabc,pk->kabc", squared, variants, precision=lax.Precision.HIGHEST)
    dilation = strain[0] + strain[1] + strain[2]
    stress = lame_first * dilation + 2.0 * (1.0 + excess) * strain
    return jnp.concatenate([excess[None], stress], axis=0)


def shifted(padded, along, offset):
    slicer = [slice(None)] * padded.ndim
    for dimension in range(padded.ndim - 3, padded.ndim):
        lowest = 1 + (offset if dimension == padded.ndim + along else 0)
        slicer[dimension] = slice(lowest, padded.shape[dimension] - 2 + lowest)
    return padded[tuple(slicer)]


def stiffness(padded, excess_pad):
    centre = shifted(padded, -1, 0)
    excess = shifted(excess_pad, -1, 0)
    summed = DIAGONAL_SHIFT * centre
    for along in (-3, -2, -1):
        for offset in (-1, 1):
            weight = 1.0 + 0.5 * (excess + shifted(excess_pad, along, offset))
            summed = summed + weight * (centre - shifted(padded, along, offset))
    return summed


def chebyshev(forcing, operate):
    ratio_now = SPECTRUM_RADIUS / SPECTRUM_CENTRE
    residual = forcing
    direction = forcing / SPECTRUM_CENTRE
    solution = jnp.zeros_like(forcing)
    for counter in range(ITERS):
        solution = solution + direction
        residual = residual - operate(direction)
        ratio_next = 1.0 / (2.0 * SPECTRUM_CENTRE / SPECTRUM_RADIUS - ratio_now)
        direction = ratio_next * ratio_now * direction + (2.0 * ratio_next / SPECTRUM_RADIUS) * residual
        ratio_now = ratio_next
    return solution + direction


def reference(phases, mobility, active, variants):
    flags = jnp.transpose(active.astype(jnp.float32), (3, 0, 1, 2))
    flags = jnp.repeat(jnp.repeat(jnp.repeat(flags, BRICK, axis=1), BRICK, axis=2), BRICK, axis=3)
    speeds = mobility[:, None, None, None] * flags
    fields = phases
    for counter in range(STEPS):
        padded = jnp.pad(fields, ((0, 0), (1, 1), (1, 1), (1, 1)))
        fields = relax(fields, padded, speeds)
    owned = coefficients(jnp.transpose(fields, (0, 3, 2, 1)), variants)
    padded = jnp.pad(owned, ((0, 0), (1, 1), (1, 1), (1, 1)))
    excess_pad = padded[0]
    forcing = jnp.stack([0.5 * (shifted(padded[1 + component], along, 1) - shifted(padded[1 + component], along, -1))
                         for component, along in enumerate((-1, -2, -3))])

    def operate(direction):
        return stiffness(jnp.pad(direction, ((0, 0), (1, 1), (1, 1), (1, 1))), excess_pad)

    return fields, chebyshev(forcing, operate)
```

```python
import functools

import jax
import jax.numpy as jnp
from jax import lax
from jax.experimental import pallas as pl
from jax.experimental.pallas import tpu as pltpu
from jax.sharding import PartitionSpec as P

STEPS = 3
ITERS = 4
DIAGONAL_SHIFT = 3.0
SPECTRUM_CENTRE = 12.0
SPECTRUM_RADIUS = 9.0

B = 12
F = 8
K = 384
H = 3
W = B + H
GO = ITERS + 1
HIGHEST = lax.Precision.HIGHEST
VMEM = pl.BlockSpec(memory_space=pltpu.VMEM)


def roll(x, shift, axis):
    return pltpu.roll(x, shift % x.shape[axis], axis)


def relax_kernel(
    ph, low, high, across, corner, own_speed, mix, ev, coef, down, up, first, second, speed
):
    slab = lax.axis_index("slab")
    own = 1 + H * slab
    other = 1 + B * (1 - slab)
    zero = jnp.zeros((F, K), jnp.float32)
    lane = lax.broadcasted_iota(jnp.int32, (F, K), 1)

    speed[0, 0] = low[H * B]
    speed[0, 1] = corner[H * H]
    speed[1, 0] = own_speed[...]
    speed[1, 1] = across[H * B]
    speed[2, 0] = high[H * B]
    speed[2, 1] = corner[2 * H * H + 1]

    def clear(a, _):
        for buf in (first, second):
            buf[a, 0] = zero
            buf[a, W + 1] = zero
        return 0

    lax.fori_loop(0, B + 2 * H, clear, 0)

    def fill(i, _):
        for j in range(B):
            first[H + i, own + j] = ph[i, j]
        for t in range(H):
            first[H + i, other + t] = across[H * i + t]
        return 0

    lax.fori_loop(0, B, fill, 0)
    for a in range(H):
        for j in range(B):
            first[a, own + j] = low[B * a + j]
            first[H + B + a, own + j] = high[B * a + j]
        for t in range(H):
            first[a, other + t] = corner[H * a + t]
            first[H + B + a, other + t] = corner[H * H + 1 + H * a + t]

    def update(x, around, s):
        square = x * x
        total = square + roll(square, 4, 0)
        total = total + roll(total, 2, 0)
        total = total + roll(total, 1, 0)
        left = jnp.where(lane == 0, 0.0, roll(x, 1, 1))
        right = jnp.where(lane == K - 1, 0.0, roll(x, -1, 1))
        summed = around + (left + right)
        return x - s * (x * (5.0 + 3.0 * total - 2.0 * square) - summed)

    def window_step(src, dst, depth):
        def plane(a, _):
            group = (a >= H).astype(jnp.int32) + (a >= H + B).astype(jnp.int32)
            before = src[a, 0]
            x = src[a, 1]
            for w in range(W):
                after = src[a, w + 2]
                whose = slab if w < H else (1 - slab if w >= B else 0)
                around = (before + after) + (src[a - 1, w + 1] + src[a + 1, w + 1])
                dst[a, w + 1] = update(x, around, speed[group, whose])
                before, x = x, after
            return 0

        lax.fori_loop(depth, B + 2 * H - depth, plane, 0)

    window_step(first, second, 1)
    window_step(second, first, 2)

    row = lax.broadcasted_iota(jnp.int32, (4 * B, K), 0)
    is_excess = (row >= B) & (row < 2 * B)

    def last_plane(i, _):
        a = i + H
        before = first[a, own - 1]
        x = first[a, own]
        for j in range(B):
            after = first[a, own + j + 1]
            around = (before + after) + (first[a - 1, own + j] + first[a + 1, own + j])
            ev[i, j] = update(x, around, own_speed[...])
            before, x = x, after
        values = ev[i].reshape(B * F, K)
        mixed = jnp.dot(
            mix[...], values * values, precision=HIGHEST, preferred_element_type=jnp.float32
        )
        total = mixed[: 4 * B]
        strain = mixed[4 * B : 8 * B]
        dilation = mixed[8 * B :]
        saturation = total / (1.0 + total)
        excess = 0.5 * saturation
        stress = (1.5 + saturation) * dilation + 2.0 * (1.0 + excess) * strain
        coef[i] = jnp.where(is_excess, excess, stress)
        return 0

    lax.fori_loop(0, B, last_plane, 0)
    for t in range(ITERS):
        down[4 * B * t : 4 * B * (t + 1)] = coef[t]
        up[4 * B * t : 4 * B * (t + 1)] = coef[B - ITERS + t]
    down[4 * B * ITERS :] = coef[ITERS, :16]
    up[4 * B * ITERS :] = coef[B - ITERS - 1, :16]


def solve_kernel(
    coef, low, high, o_coef, o_low, o_high, out,
    s0, s1, s2, ex, dia, wi, wjp, wjm, wkp, wkm, dir_a, dir_b, res, sol, rows,
):
    slab = lax.axis_index("slab")
    place = lax.axis_index("space")
    count = lax.axis_size("space")
    bottom = slab == 0
    J = 2 * B
    N = B + 2 * GO
    row = lax.broadcasted_iota(jnp.int32, (J, K), 0)
    lane = lax.broadcasted_iota(jnp.int32, (J, K), 1)

    def joined(mine, others):
        lo = jnp.where(bottom, mine, others)
        hi = jnp.where(bottom, others, mine)
        n = mine.shape[0] // B
        return [
            jnp.concatenate([lo[B * c : B * c + B], hi[B * c : B * c + B]], 0) for c in range(n)
        ]

    def put(a, mine, others):
        s0[a], ex[a], s1[a], s2[a] = joined(mine, others)

    def put_own(i, _):
        put(i + GO, coef[i], o_coef[i])
        return 0

    lax.fori_loop(0, B, put_own, 0)
    for t in range(ITERS):
        part = slice(4 * B * t, 4 * B * (t + 1))
        put(1 + t, low[part], o_low[part])
        put(GO + B + t, high[part], o_high[part])
    tail = slice(4 * B * ITERS, 4 * B * ITERS + 16)
    (s0[0],) = joined(low[tail], o_low[tail])
    (s0[N - 1],) = joined(high[tail], o_high[tail])

    def next_j(x):
        return jnp.where(row == J - 1, 0.0, roll(x, -1, 0))

    def last_j(x):
        return jnp.where(row == 0, 0.0, roll(x, 1, 0))

    def next_k(x):
        return jnp.where(lane == K - 1, 0.0, roll(x, -1, 1))

    def last_k(x):
        return jnp.where(lane == 0, 0.0, roll(x, 1, 1))

    def force(a, _):
        forcing = (
            0.5 * (s0[a + 1] - s0[a - 1]),
            0.5 * (next_j(s1[a]) - last_j(s1[a])),
            0.5 * (next_k(s2[a]) - last_k(s2[a])),
        )
        for c in range(3):
            dir_a[c, a] = forcing[c] / SPECTRUM_CENTRE
            res[c, a] = forcing[c]
        return 0

    lax.fori_loop(1, N - 1, force, 0)

    wi[1] = 1.0 + 0.5 * (ex[1] + ex[2])

    def weigh(a, _):
        e = ex[a]
        i_next = 1.0 + 0.5 * (e + ex[a + 1])
        i_last = 1.0 + 0.5 * (e + ex[a - 1])
        j_next = 1.0 + 0.5 * (e + next_j(e))
        j_last = 1.0 + 0.5 * (e + last_j(e))
        k_next = 1.0 + 0.5 * (e + next_k(e))
        k_last = 1.0 + 0.5 * (e + last_k(e))
        dia[a] = DIAGONAL_SHIFT + ((i_next + i_last) + (j_next + j_last) + (k_next + k_last))
        wi[a] = i_next
        wjp[a] = jnp.where(row == J - 1, 0.0, j_next)
        wjm[a] = jnp.where(row == 0, 0.0, j_last)
        wkp[a] = jnp.where(lane == K - 1, 0.0, k_next)
        wkm[a] = jnp.where(lane == 0, 0.0, k_last)
        return 0

    lax.fori_loop(2, N - 2, weigh, 0)

    @pl.when(place == 0)
    def _():
        wi[GO - 1] = jnp.zeros((J, K), jnp.float32)

    @pl.when(place == count - 1)
    def _():
        wi[GO + B - 1] = jnp.zeros((J, K), jnp.float32)

    def apply(src, c, a):
        v = src[c, a]
        r = res[c, a] - dia[a] * v
        r = r + wi[a] * src[c, a + 1]
        r = r + wi[a - 1] * src[c, a - 1]
        r = r + wjp[a] * roll(v, -1, 0)
        r = r + wjm[a] * roll(v, 1, 0)
        r = r + wkp[a] * roll(v, -1, 1)
        r = r + wkm[a] * roll(v, 1, 1)
        return v, r

    ratio = SPECTRUM_RADIUS / SPECTRUM_CENTRE
    src, dst = dir_a, dir_b
    for t in range(ITERS):
        ratio_next = 1.0 / (2.0 * SPECTRUM_CENTRE / SPECTRUM_RADIUS - ratio)
        keep, gain = ratio_next * ratio, 2.0 * ratio_next / SPECTRUM_RADIUS
        ratio = ratio_next
        if t == ITERS - 1:
            break

        def plane(a, _, src=src, dst=dst, keep=keep, gain=gain, t=t, inner=False):
            for c in range(3):
                v, r = apply(src, c, a)
                res[c, a] = r
                dst[c, a] = keep * v + gain * r
                if inner:
                    sol[c, a - GO] = v if t == 0 else sol[c, a - GO] + v
            return 0

        lax.fori_loop(2 + t, GO, plane, 0)
        lax.fori_loop(GO, GO + B, functools.partial(plane, inner=True), 0)
        lax.fori_loop(GO + B, N - 2 - t, plane, 0)
        src, dst = dst, src

    third = lax.broadcasted_iota(jnp.int32, (B, K), 1) % 3
    target = lax.broadcasted_iota(jnp.int32, (K // 3, K), 0)
    source = lax.broadcasted_iota(jnp.int32, (K // 3, K), 1) // 3
    pick = jnp.where(target == source, 1.0, 0.0)
    rows[9 * B :] = jnp.zeros((128 - 9 * B, K), jnp.float32)

    def finish(i, _):
        a = i + GO
        for c in range(3):
            v, r = apply(src, c, a)
            total = sol[c, i] + v + (keep * v + gain * r)
            mine = jnp.where(bottom, total[:B], total[B:])
            for q in range(3):
                g = 3 * c + q
                rows[B * g : B * g + B] = jnp.where(third == q, mine, 0.0)
        moved = lax.dot_general(
            pick,
            rows[...],
            (((1,), (1,)), ((), ())),
            precision=HIGHEST,
            preferred_element_type=jnp.float32,
        )
        out[pl.ds(i, K // 3, stride=B), :] = moved
        return 0

    lax.fori_loop(0, B, finish, 0)


def unpack_kernel(got, out):
    tiles = got.shape[0] // 128
    for t in range(tiles):
        turned = got[128 * t : 128 * (t + 1), :].T
        for c in range(3):
            for q in range(3):
                g = 3 * c + q
                out[c, q, :, 128 * t : 128 * (t + 1)] = turned[B * g : B * g + B]


def call(kernel, shapes, inputs, scratch=(), name=None):
    return pl.pallas_call(
        kernel,
        out_shape=[jax.ShapeDtypeStruct(s, jnp.float32) for s in shapes],
        in_specs=[VMEM] * len(inputs),
        out_specs=[VMEM] * len(shapes),
        scratch_shapes=[pltpu.VMEM(s, jnp.float32) for s in scratch],
        compiler_params=pltpu.CompilerParams(vmem_limit_bytes=58 * 1024 * 1024),
        name=name,
    )(*inputs)


def shards(phases, mobility, active, variants):
    count = lax.axis_size("space")
    slab = lax.axis_index("slab")
    upward = [(i, i + 1) for i in range(count - 1)]
    downward = [(b, a) for a, b in upward]
    swap = [(0, 1), (1, 0)]

    ph = jnp.transpose(phases, (1, 2, 0, 3))
    flags = jnp.repeat(active[0, 0].astype(jnp.float32).T, B, axis=1)
    speed = mobility[:, None] * flags

    def edge(array, start):
        return lax.dynamic_slice_in_dim(array, start, H, axis=1).reshape(-1, F, K)

    start = (B - H) * (1 - slab)
    low = lax.ppermute(
        jnp.concatenate([ph[B - H :].reshape(H * B, F, K), speed[None]]), "space", upward
    )
    high = lax.ppermute(
        jnp.concatenate([ph[:H].reshape(H * B, F, K), speed[None]]), "space", downward
    )
    across = lax.ppermute(jnp.concatenate([edge(ph, start), speed[None]]), "slab", swap)
    corner = lax.ppermute(
        jnp.concatenate(
            [
                edge(low[: H * B].reshape(H, B, F, K), start),
                low[H * B :],
                edge(high[: H * B].reshape(H, B, F, K), start),
                high[H * B :],
            ]
        ),
        "slab",
        swap,
    )

    by_field = jnp.concatenate([variants.T[:1], jnp.zeros((1, F)), variants.T[1:]])
    table = jnp.stack(
        [
            jnp.ones((4, F), jnp.float32),
            by_field,
            jnp.broadcast_to(jnp.sum(variants, axis=1), (4, F)),
        ]
    )
    mix = (table[:, :, None, None, :] * jnp.eye(B)[None, None, :, :, None]).reshape(12 * B, B * F)

    block = (B + 2 * H, W + 2, F, K)
    message = (4 * B * ITERS + 16, K)
    evolved, coef, down, up = call(
        relax_kernel,
        [(B, B, F, K), (B, 4 * B, K), message, message],
        [ph, low, high, across, corner, speed, mix],
        [block, block, (3, 2, F, K)],
        name="relax",
    )
    low = lax.ppermute(up, "space", upward)
    high = lax.ppermute(down, "space", downward)
    o_coef = lax.ppermute(coef, "slab", swap)
    both = lax.ppermute(jnp.stack([low, high]), "slab", swap)
    J, N = 2 * B, B + 2 * GO
    (packed,) = call(
        solve_kernel,
        [(K // 3 * B, 128)],
        [coef, low, high, o_coef, both[0], both[1]],
        [(N, J, K)] * 10 + [(3, N, J, K)] * 3 + [(3, B, J, K), (128, K)],
        name="solve",
    )
    arrived = lax.all_to_all(packed.reshape(count, 1, B * 128), "space", 0, 0, tiled=True)
    (displacement,) = call(
        unpack_kernel, [(3, K // count, B, count * B)], [arrived.reshape(count * B, 128)], name="unpack"
    )
    return jnp.transpose(evolved, (2, 0, 1, 3)), displacement


def solution(mesh):
    placed = (P(None, "space", "slab", None), P(), P("space", "slab", None, None), P())
    return jax.shard_map(
        shards,
        mesh=mesh,
        in_specs=placed,
        out_specs=(P(None, "space", "slab", None), P(None, "space", "slab", None)),
        check_vma=False,
    )
```

```python
import functools

import jax
import jax.numpy as jnp
from jax import lax
from jax.experimental import pallas as pl
from jax.experimental.pallas import tpu as pltpu
from jax.sharding import PartitionSpec as P

STEPS = 3
ITERS = 4
DIAGONAL_SHIFT = 3.0
SPECTRUM_CENTRE = 12.0
SPECTRUM_RADIUS = 9.0

B = 12
F = 8
K = 384
H = 3
W = B + H
GO = ITERS + 1
HIGHEST = lax.Precision.HIGHEST
VMEM = pl.BlockSpec(memory_space=pltpu.VMEM)


def roll(x, shift, axis):
    return pltpu.roll(x, shift % x.shape[axis], axis)


def parity():
    even = 1 - lax.axis_index("space") % 2
    return even, 1 - even


def pack_kernel(ph, mobility, active, to_near, to_far, to_other, sems):
    even, odd = parity()
    start = (B - H) * (1 - lax.axis_index("slab"))
    copies = []
    for t in range(H):
        for message, top in ((to_near, even), (to_far, odd)):
            source = ph.at[(B - H) * top + t]
            copies.append((source, message.at[pl.ds(B * t, B)]))
    for i in range(B):
        copies.append((ph.at[i, pl.ds(start, H)], to_other.at[pl.ds(H * i, H)]))
    copies = [pltpu.make_async_copy(a, b, sems.at[n]) for n, (a, b) in enumerate(copies)]
    for copy in copies:
        copy.start()
    scaled = active[...].astype(jnp.float32) * mobility[...]
    bricks = K // B
    brick = lax.broadcasted_iota(jnp.int32, (bricks, K), 0)
    spread = jnp.where(brick == lax.broadcasted_iota(jnp.int32, (bricks, K), 1) // B, 1.0, 0.0)
    speed = lax.dot_general(
        scaled,
        spread,
        (((0,), (0,)), ((), ())),
        precision=HIGHEST,
        preferred_element_type=jnp.float32,
    )
    for message in (to_near, to_far, to_other):
        message[H * B] = speed
    for copy in copies:
        copy.wait()


def relax_kernel(
    ph, mine, near, far, across, c_near, c_far, mix, ev, coef, m_near, m_far, first, second, speed
):
    even, odd = parity()
    halos = ((near, c_near, even), (far, c_far, odd))
    own_speed = mine.at[H * B]
    slab = lax.axis_index("slab")
    own = 1 + H * slab
    other = 1 + B * (1 - slab)
    zero = jnp.zeros((F, K), jnp.float32)
    lane = lax.broadcasted_iota(jnp.int32, (F, K), 1)

    for halo, corner, top in halos:
        speed[2 * top, 0] = halo[H * B]
        speed[2 * top, 1] = corner[H * H]
    speed[1, 0] = own_speed[...]
    speed[1, 1] = across[H * B]

    def clear(a, _):
        for buf in (first, second):
            buf[a, 0] = zero
            buf[a, W + 1] = zero
        return 0

    lax.fori_loop(0, B + 2 * H, clear, 0)

    def fill(i, _):
        for j in range(B):
            first[H + i, own + j] = ph[i, j]
        for t in range(H):
            first[H + i, other + t] = across[H * i + t]
        return 0

    lax.fori_loop(0, B, fill, 0)
    for halo, corner, top in halos:
        for a in range(H):
            for j in range(B):
                first[(H + B) * top + a, own + j] = halo[B * a + j]
            for t in range(H):
                first[(H + B) * top + a, other + t] = corner[H * a + t]

    def update(x, around, s):
        square = x * x
        total = square + roll(square, 4, 0)
        total = total + roll(total, 2, 0)
        total = total + roll(total, 1, 0)
        left = jnp.where(lane == 0, 0.0, roll(x, 1, 1))
        right = jnp.where(lane == K - 1, 0.0, roll(x, -1, 1))
        summed = around + (left + right)
        return x - s * (x * (5.0 + 3.0 * total - 2.0 * square) - summed)

    def window_step(src, dst, depth):
        def plane(a, _):
            group = (a >= H).astype(jnp.int32) + (a >= H + B).astype(jnp.int32)
            before = src[a, 0]
            x = src[a, 1]
            for w in range(W):
                after = src[a, w + 2]
                whose = slab if w < H else (1 - slab if w >= B else 0)
                around = (before + after) + (src[a - 1, w + 1] + src[a + 1, w + 1])
                dst[a, w + 1] = update(x, around, speed[group, whose])
                before, x = x, after
            return 0

        lax.fori_loop(depth, B + 2 * H - depth, plane, 0)

    window_step(first, second, 1)
    window_step(second, first, 2)

    row = lax.broadcasted_iota(jnp.int32, (4 * B, K), 0)
    is_excess = (row >= B) & (row < 2 * B)

    def last_plane(i, _):
        a = i + H
        before = first[a, own - 1]
        x = first[a, own]
        for j in range(B):
            after = first[a, own + j + 1]
            around = (before + after) + (first[a - 1, own + j] + first[a + 1, own + j])
            ev[i, j] = update(x, around, own_speed[...])
            before, x = x, after
        values = ev[i].reshape(B * F, K)
        mixed = jnp.dot(
            mix[...], values * values, precision=HIGHEST, preferred_element_type=jnp.float32
        )
        total = mixed[: 4 * B]
        strain = mixed[4 * B : 8 * B]
        dilation = mixed[8 * B :]
        saturation = total / (1.0 + total)
        excess = 0.5 * saturation
        stress = (1.5 + saturation) * dilation + 2.0 * (1.0 + excess) * strain
        coef[i] = jnp.where(is_excess, excess, stress)
        return 0

    lax.fori_loop(0, B, last_plane, 0)
    for message, top in ((m_near, even), (m_far, odd)):
        for t in range(ITERS):
            message[4 * B * t : 4 * B * (t + 1)] = coef[(B - ITERS) * top + t]
        message[4 * B * ITERS :] = coef[ITERS + (B - 2 * ITERS - 1) * top, :16]


def solve_kernel(
    coef, near, far, o_coef, o_near, o_far, out,
    s0, s1, s2, ex, dia, wi, wjp, wjm, wkp, wkm, dir_a, dir_b, res, sol, rows, flat,
):
    even, odd = parity()
    slab = lax.axis_index("slab")
    place = lax.axis_index("space")
    count = lax.axis_size("space")
    bottom = slab == 0
    J = 2 * B
    N = B + 2 * GO
    row = lax.broadcasted_iota(jnp.int32, (J, K), 0)
    lane = lax.broadcasted_iota(jnp.int32, (J, K), 1)

    def joined(mine, others):
        lo = jnp.where(bottom, mine, others)
        hi = jnp.where(bottom, others, mine)
        n = mine.shape[0] // B
        return [
            jnp.concatenate([lo[B * c : B * c + B], hi[B * c : B * c + B]], 0) for c in range(n)
        ]

    def put(a, mine, others):
        s0[a], ex[a], s1[a], s2[a] = joined(mine, others)

    def put_own(i, _):
        put(i + GO, coef[i], o_coef[i])
        return 0

    lax.fori_loop(0, B, put_own, 0)
    tail = slice(4 * B * ITERS, 4 * B * ITERS + 16)
    for halo, others, top in ((near, o_near, even), (far, o_far, odd)):
        for t in range(ITERS):
            part = slice(4 * B * t, 4 * B * (t + 1))
            put(1 + t + (GO + B - 1) * top, halo[part], others[part])
        (s0[(N - 1) * top],) = joined(halo[tail], others[tail])

    def next_j(x):
        return jnp.where(row == J - 1, 0.0, roll(x, -1, 0))

    def last_j(x):
        return jnp.where(row == 0, 0.0, roll(x, 1, 0))

    def next_k(x):
        return jnp.where(lane == K - 1, 0.0, roll(x, -1, 1))

    def last_k(x):
        return jnp.where(lane == 0, 0.0, roll(x, 1, 1))

    def force(a, _):
        forcing = (
            0.5 * (s0[a + 1] - s0[a - 1]),
            0.5 * (next_j(s1[a]) - last_j(s1[a])),
            0.5 * (next_k(s2[a]) - last_k(s2[a])),
        )
        for c in range(3):
            dir_a[c, a] = forcing[c] / SPECTRUM_CENTRE
            res[c, a] = forcing[c]
        return 0

    lax.fori_loop(1, N - 1, force, 0)

    wi[1] = 1.0 + 0.5 * (ex[1] + ex[2])

    def weigh(a, _):
        e = ex[a]
        i_next = 1.0 + 0.5 * (e + ex[a + 1])
        i_last = 1.0 + 0.5 * (e + ex[a - 1])
        j_next = 1.0 + 0.5 * (e + next_j(e))
        j_last = 1.0 + 0.5 * (e + last_j(e))
        k_next = 1.0 + 0.5 * (e + next_k(e))
        k_last = 1.0 + 0.5 * (e + last_k(e))
        dia[a] = DIAGONAL_SHIFT + ((i_next + i_last) + (j_next + j_last) + (k_next + k_last))
        wi[a] = i_next
        wjp[a] = jnp.where(row == J - 1, 0.0, j_next)
        wjm[a] = jnp.where(row == 0, 0.0, j_last)
        wkp[a] = jnp.where(lane == K - 1, 0.0, k_next)
        wkm[a] = jnp.where(lane == 0, 0.0, k_last)
        return 0

    lax.fori_loop(2, N - 2, weigh, 0)

    @pl.when(place == 0)
    def _():
        wi[GO - 1] = jnp.zeros((J, K), jnp.float32)

    @pl.when(place == count - 1)
    def _():
        wi[GO + B - 1] = jnp.zeros((J, K), jnp.float32)

    def apply(src, c, a):
        v = src[c, a]
        r = res[c, a] - dia[a] * v
        r = r + wi[a] * src[c, a + 1]
        r = r + wi[a - 1] * src[c, a - 1]
        r = r + wjp[a] * roll(v, -1, 0)
        r = r + wjm[a] * roll(v, 1, 0)
        r = r + wkp[a] * roll(v, -1, 1)
        r = r + wkm[a] * roll(v, 1, 1)
        return v, r

    ratio = SPECTRUM_RADIUS / SPECTRUM_CENTRE
    src, dst = dir_a, dir_b
    for t in range(ITERS):
        ratio_next = 1.0 / (2.0 * SPECTRUM_CENTRE / SPECTRUM_RADIUS - ratio)
        keep, gain = ratio_next * ratio, 2.0 * ratio_next / SPECTRUM_RADIUS
        ratio = ratio_next
        if t == ITERS - 1:
            break

        def plane(a, _, src=src, dst=dst, keep=keep, gain=gain, t=t, inner=False):
            for c in range(3):
                v, r = apply(src, c, a)
                res[c, a] = r
                dst[c, a] = keep * v + gain * r
                if inner:
                    sol[c, a - GO] = v if t == 0 else sol[c, a - GO] + v
            return 0

        lax.fori_loop(2 + t, GO, plane, 0)
        lax.fori_loop(GO, GO + B, functools.partial(plane, inner=True), 0)
        lax.fori_loop(GO + B, N - 2 - t, plane, 0)
        src, dst = dst, src

    third = lax.broadcasted_iota(jnp.int32, (B, K), 1) % 3
    target = lax.broadcasted_iota(jnp.int32, (K // 3, K), 0)
    source = lax.broadcasted_iota(jnp.int32, (K // 3, K), 1) // 3
    pick = jnp.where(target == source, 1.0, 0.0)
    rows[9 * B :] = jnp.zeros((128 - 9 * B, K), jnp.float32)

    def finish(i, _):
        a = i + GO
        for c in range(3):
            v, r = apply(src, c, a)
            total = sol[c, i] + v + (keep * v + gain * r)
            mine = jnp.where(bottom, total[:B], total[B:])
            for q in range(3):
                g = 3 * c + q
                rows[B * g : B * g + B] = jnp.where(third == q, mine, 0.0)
        moved = lax.dot_general(
            pick,
            rows[...],
            (((1,), (1,)), ((), ())),
            precision=HIGHEST,
            preferred_element_type=jnp.float32,
        )
        flat[pl.ds(i, K // 3, stride=B), :] = moved
        return 0

    lax.fori_loop(0, B, finish, 0)
    for n in range(out.shape[0]):
        out[n] = flat[B * n : B * (n + 1), :]


def unpack_kernel(got, out, flat):
    for n in range(got.shape[0]):
        flat[B * n : B * (n + 1), :] = got[n]
    for t in range(flat.shape[0] // 128):
        turned = flat[128 * t : 128 * (t + 1), :].T
        for c in range(3):
            for q in range(3):
                g = 3 * c + q
                out[c, q, :, 128 * t : 128 * (t + 1)] = turned[B * g : B * g + B]


def call(kernel, shapes, inputs, scratch=(), name=None, grant=8, in_specs=None, extra=()):
    return pl.pallas_call(
        kernel,
        out_shape=[jax.ShapeDtypeStruct(s, jnp.float32) for s in shapes],
        in_specs=in_specs or [VMEM] * len(inputs),
        out_specs=[VMEM] * len(shapes),
        scratch_shapes=[pltpu.VMEM(s, jnp.float32) for s in scratch] + list(extra),
        compiler_params=pltpu.CompilerParams(vmem_limit_bytes=grant * 1024 * 1024),
        name=name,
    )(*inputs)


def shards(phases, mobility, active, variants):
    count = lax.axis_size("space")
    slab = lax.axis_index("slab")

    def pairs(first):
        forward = [(i, i + 1) for i in range(first, count - 1, 2)]
        return forward + [(b, a) for a, b in forward]

    def exchange(to_near, to_far):
        return lax.ppermute(to_near, "space", pairs(0)), lax.ppermute(to_far, "space", pairs(1))

    def swap(array):
        return lax.ppermute(array, "slab", [(0, 1), (1, 0)])

    ph = jnp.transpose(phases, (1, 2, 0, 3))
    to_near, to_far, to_other = call(
        pack_kernel,
        [(H * B + 1, F, K)] * 3,
        [ph, mobility[None], active[0, 0]],
        name="pack",
        in_specs=[pl.BlockSpec(memory_space=pl.ANY), VMEM, VMEM],
        extra=[pltpu.SemaphoreType.DMA((2 * H + B,))],
    )
    start = (B - H) * (1 - slab)

    def corner(halo):
        part = halo[: H * B].reshape(H, B, F, K)
        part = lax.dynamic_slice_in_dim(part, start, H, axis=1).reshape(H * H, F, K)
        return jnp.concatenate([part, halo[H * B :]])

    across = swap(to_other)
    near, far = exchange(to_near, to_far)
    c_near, c_far = swap(corner(near)), swap(corner(far))

    by_field = jnp.concatenate([variants.T[:1], jnp.zeros((1, F)), variants.T[1:]])
    table = jnp.stack(
        [
            jnp.ones((4, F), jnp.float32),
            by_field,
            jnp.broadcast_to(jnp.sum(variants, axis=1), (4, F)),
        ]
    )
    mix = (table[:, :, None, None, :] * jnp.eye(B)[None, None, :, :, None]).reshape(12 * B, B * F)

    block = (B + 2 * H, W + 2, F, K)
    message = (4 * B * ITERS + 16, K)
    evolved, coef, to_near, to_far = call(
        relax_kernel,
        [(B, B, F, K), (B, 4 * B, K), message, message],
        [ph, to_other, near, far, across, c_near, c_far, mix],
        [block, block, (3, 2, F, K)],
        name="relax",
        grant=20,
    )
    o_coef = swap(coef)
    near, far = exchange(to_near, to_far)
    o_near, o_far = swap(near), swap(far)
    J, N = 2 * B, B + 2 * GO
    (packed,) = call(
        solve_kernel,
        [(K // 3, B, 128)],
        [coef, near, far, o_coef, o_near, o_far],
        [(N, J, K)] * 10 + [(3, N, J, K)] * 3 + [(3, B, J, K), (128, K), (K // 3 * B, 128)],
        name="solve",
        grant=28,
    )
    arrived = lax.all_to_all(packed, "space", 0, 0, tiled=True)
    (displacement,) = call(
        unpack_kernel,
        [(3, K // count, B, count * B)],
        [arrived],
        [(count * B, 128)],
        name="unpack",
    )
    return jnp.transpose(evolved, (2, 0, 1, 3)), displacement


def solution(mesh):
    placed = (P(None, "space", "slab", None), P(), P("space", "slab", None, None), P())
    return jax.shard_map(
        shards,
        mesh=mesh,
        in_specs=placed,
        out_specs=(P(None, "space", "slab", None), P(None, "space", "slab", None)),
        check_vma=False,
    )
```

```python
import jax
import jax.numpy as jnp
from jax import lax
from jax.experimental import pallas as pl
from jax.experimental.pallas import tpu as pltpu
from jax.sharding import PartitionSpec as P


ITERS = 4
DIAGONAL_SHIFT = 3.0
SPECTRUM_CENTRE = 12.0
SPECTRUM_RADIUS = 9.0

B = 12
F = 8
K = 384
H = 3
W = B + H
GO = ITERS + 1
HIGHEST = lax.Precision.HIGHEST
VMEM = pl.BlockSpec(memory_space=pltpu.VMEM)
HBM = pl.BlockSpec(memory_space=pltpu.HBM)


def roll(x, shift, axis):
    return pltpu.roll(x, shift % x.shape[axis], axis)


def parity():
    even = 1 - lax.axis_index("space") % 2
    return even, 1 - even


def pack_kernel(ph, mobility, active, to_near, to_far, to_other, sems):
    even, odd = parity()
    start = (B - H) * (1 - lax.axis_index("slab"))
    copies = []
    for t in range(H):
        for message, top in ((to_far, odd), (to_near, even)):
            source = ph.at[(B - H) * top + t]
            copies.append((source, message.at[pl.ds(B * t, B)]))
    for i in range(B):
        copies.append((ph.at[i, pl.ds(start, H)], to_other.at[pl.ds(H * i, H)]))
    copies = [pltpu.make_async_copy(a, b, sems.at[n]) for n, (a, b) in enumerate(copies)]
    for copy in copies:
        copy.start()
    bricks = K // B
    brick = lax.broadcasted_iota(jnp.int32, (bricks, K), 0)
    spread = jnp.where(brick == lax.broadcasted_iota(jnp.int32, (bricks, K), 1) // B, 1.0, 0.0)
    flags = jnp.dot(
        active[...].astype(jnp.float32), spread, preferred_element_type=jnp.float32
    )
    field = lax.broadcasted_iota(jnp.int32, (F, F), 0)
    rates = jnp.where(field == lax.broadcasted_iota(jnp.int32, (F, F), 1), mobility[...], 0.0)
    speed = flags * jnp.sum(rates, axis=1, keepdims=True)
    for message in (to_near, to_far, to_other):
        message[H * B] = speed
    for copy in copies:
        copy.wait()


def update(x, around, s):
    lane = lax.broadcasted_iota(jnp.int32, (F, K), 1)
    square = x * x
    total = square + roll(square, 4, 0)
    total = total + roll(total, 2, 0)
    total = total + roll(total, 1, 0)
    left = jnp.where(lane == 0, 0.0, roll(x, 1, 1))
    right = jnp.where(lane == K - 1, 0.0, roll(x, -1, 1))
    summed = around + (left + right)
    return x - s * (x * (5.0 + 3.0 * total - 2.0 * square) - summed)


def window_step(src, dst, speed, count, place):
    slab = lax.axis_index("slab")

    def plane(n, _):
        a = place(n)
        group = (a >= H).astype(jnp.int32) + (a >= H + B).astype(jnp.int32)
        before = src[a, 0]
        x = src[a, 1]
        for w in range(W):
            after = src[a, w + 2]
            whose = slab if w < H else (1 - slab if w >= B else 0)
            around = (before + after) + (src[a - 1, w + 1] + src[a + 1, w + 1])
            dst[a, w + 1] = update(x, around, speed[group, whose])
            before, x = x, after
        return 0

    lax.fori_loop(0, count, plane, 0)


def halves(x):
    high = x.astype(jnp.bfloat16)
    return high, (x - high.astype(jnp.float32)).astype(jnp.bfloat16)


def last_step(src, own_speed, mix, ev, coef, count, place, staged, sems):
    own = 1 + H * lax.axis_index("slab")
    row = lax.broadcasted_iota(jnp.int32, (4 * B, K), 0)
    is_excess = (row >= B) & (row < 2 * B)

    def plane(n, _):
        a = place(n)
        i = a - H
        before = src[a, own - 1]
        x = src[a, own]
        squares = []
        for j in range(B):
            after = src[a, own + j + 1]
            around = (before + after) + (src[a - 1, own + j] + src[a + 1, own + j])
            value = update(x, around, own_speed[...])
            staged[n, j] = value
            squares.append(value * value)
            before, x = x, after
        pltpu.make_async_copy(staged.at[n], ev.at[i], sems.at[n]).start()
        high, low = halves(jnp.concatenate(squares, 0))
        mixed = jnp.dot(
            mix[...],
            jnp.concatenate([high, low, high], 0),
            preferred_element_type=jnp.float32,
        )
        total = mixed[: 4 * B]
        strain = mixed[4 * B : 8 * B]
        dilation = mixed[8 * B :]
        saturation = total / (1.0 + total)
        excess = 0.5 * saturation
        stress = (1.5 + saturation) * dilation + 2.0 * (1.0 + excess) * strain
        coef[i] = jnp.where(is_excess, excess, stress)
        return 0

    lax.fori_loop(0, count, plane, 0)

    def settle(n, _):
        pltpu.make_async_copy(staged.at[n], ev.at[place(n) - H], sems.at[n]).wait()
        return 0

    lax.fori_loop(0, count, settle, 0)


def relax_inner_kernel(
    ph, mine, across, variants, first, second, ev, coef, mix, speed, staged, sems
):
    slab = lax.axis_index("slab")
    own = 1 + H * slab
    other = 1 + B * (1 - slab)
    zero = jnp.zeros((F, K), jnp.float32)
    speed[1, 0] = mine[H * B]
    speed[1, 1] = across[H * B]

    v = variants[...]
    each = jnp.concatenate([v[:1], jnp.zeros((1, F)), v[1:]], 0)
    whole = jnp.broadcast_to(v[:1] + v[1:2] + v[2:], (4, F))
    table = jnp.concatenate([jnp.ones((4, F)), each, whole], 0)
    shape = (12 * B, B * F)
    group = lax.broadcasted_iota(jnp.int32, (12 * B, 12), 0) // B
    down = jnp.where(group == lax.broadcasted_iota(jnp.int32, (12 * B, 12), 1), 1.0, 0.0)
    field = lax.broadcasted_iota(jnp.int32, (F, B * F), 1) % F
    along = jnp.where(field == lax.broadcasted_iota(jnp.int32, (F, B * F), 0), 1.0, 0.0)
    table = jnp.dot(down, table, precision=HIGHEST, preferred_element_type=jnp.float32)
    table = jnp.dot(table, along, precision=HIGHEST, preferred_element_type=jnp.float32)
    same = lax.broadcasted_iota(jnp.int32, shape, 0) % B
    same = same == lax.broadcasted_iota(jnp.int32, shape, 1) // F
    high, low = halves(jnp.where(same, table, 0.0))
    mix[...] = jnp.concatenate([high, high, low], 1)

    def clear(a, _):
        for buf in (first, second):
            buf[a, 0] = zero
            buf[a, W + 1] = zero
        return 0

    lax.fori_loop(0, B + 2 * H, clear, 0)

    def fill(i, _):
        for j in range(B):
            first[H + i, own + j] = ph[i, j]
        for t in range(H):
            first[H + i, other + t] = across[H * i + t]
        return 0

    lax.fori_loop(0, B, fill, 0)
    window_step(first, second, speed, B - 2, lambda n: H + 1 + n)
    window_step(second, first, speed, B - 4, lambda n: H + 2 + n)
    last_step(first, speed.at[1, 0], mix, ev, coef, B - 6, lambda n: H + 3 + n, staged, sems)


def relax_outer_kernel(
    near, far, c_near, c_far, mine, across, mix, first_in, second_in, ev_in, coef_in,
    first, second, ev, coef, m_near, m_far, speed, staged, sems,
):
    even, odd = parity()
    slab = lax.axis_index("slab")
    own = 1 + H * slab
    other = 1 + B * (1 - slab)
    speed[1, 0] = mine[H * B]
    speed[1, 1] = across[H * B]
    for halo, corner, top in ((near, c_near, even), (far, c_far, odd)):
        speed[2 * top, 0] = halo[H * B]
        speed[2 * top, 1] = corner[H * B]
        for a in range(H):
            for j in range(B):
                first[(H + B) * top + a, own + j] = halo[B * a + j]
            for t in range(H):
                first[(H + B) * top + a, other + t] = corner[B * a + (B - H) * slab + t]

    def ends(depth):
        jump = B + H - 2 * depth - 1
        return lambda n: depth + n + jnp.where(n >= H, jump + 1 - H, 0)

    window_step(first, second, speed, 2 * H, ends(1))
    window_step(second, first, speed, 2 * H, ends(2))
    last_step(first, speed.at[1, 0], mix, ev, coef, 2 * H, ends(3), staged, sems)
    for message, top in ((m_near, even), (m_far, odd)):
        for t in range(ITERS):
            message[4 * B * t : 4 * B * (t + 1)] = coef[(B - ITERS) * top + t]
        message[4 * B * ITERS :] = coef[ITERS + (B - 2 * ITERS - 1) * top, :16]


J = 2 * B
N = B + 2 * GO


def ratios():
    ratio = SPECTRUM_RADIUS / SPECTRUM_CENTRE
    out = []
    for _ in range(ITERS):
        ratio_next = 1.0 / (2.0 * SPECTRUM_CENTRE / SPECTRUM_RADIUS - ratio)
        out.append((ratio_next * ratio, 2.0 * ratio_next / SPECTRUM_RADIUS))
        ratio = ratio_next
    return out


def joined(mine, others):
    bottom = lax.axis_index("slab") == 0
    lo = jnp.where(bottom, mine, others)
    hi = jnp.where(bottom, others, mine)
    n = mine.shape[0] // B
    return [jnp.concatenate([lo[B * c : B * c + B], hi[B * c : B * c + B]], 0) for c in range(n)]


class Solver:
    def __init__(self, state):
        self.s0, self.s1, self.s2, self.ex = state[:4]
        self.dia, self.wi, self.wjp, self.wjm, self.wkp, self.wkm = state[4:10]
        self.even, self.odd, self.res, self.sol = state[10:]
        self.row = lax.broadcasted_iota(jnp.int32, (J, K), 0)
        self.lane = lax.broadcasted_iota(jnp.int32, (J, K), 1)

    def put(self, a, mine, others):
        self.s0[a], self.ex[a], self.s1[a], self.s2[a] = joined(mine, others)

    def next_j(self, x):
        return jnp.where(self.row == J - 1, 0.0, roll(x, -1, 0))

    def last_j(self, x):
        return jnp.where(self.row == 0, 0.0, roll(x, 1, 0))

    def next_k(self, x):
        return jnp.where(self.lane == K - 1, 0.0, roll(x, -1, 1))

    def last_k(self, x):
        return jnp.where(self.lane == 0, 0.0, roll(x, 1, 1))

    def force(self, a):
        forcing = (
            0.5 * (self.s0[a + 1] - self.s0[a - 1]),
            0.5 * (self.next_j(self.s1[a]) - self.last_j(self.s1[a])),
            0.5 * (self.next_k(self.s2[a]) - self.last_k(self.s2[a])),
        )
        for c in range(3):
            self.even[c, a] = forcing[c] / SPECTRUM_CENTRE
            self.res[c, a] = forcing[c]

    def weigh(self, a):
        e = self.ex[a]
        i_next = 1.0 + 0.5 * (e + self.ex[a + 1])
        i_last = 1.0 + 0.5 * (e + self.ex[a - 1])
        j_next = 1.0 + 0.5 * (e + self.next_j(e))
        j_last = 1.0 + 0.5 * (e + self.last_j(e))
        k_next = 1.0 + 0.5 * (e + self.next_k(e))
        k_last = 1.0 + 0.5 * (e + self.last_k(e))
        ends = (i_next + i_last) + (j_next + j_last) + (k_next + k_last)
        self.dia[a] = DIAGONAL_SHIFT + ends
        self.wi[a] = i_next
        self.wjp[a] = jnp.where(self.row == J - 1, 0.0, j_next)
        self.wjm[a] = jnp.where(self.row == 0, 0.0, j_last)
        self.wkp[a] = jnp.where(self.lane == K - 1, 0.0, k_next)
        self.wkm[a] = jnp.where(self.lane == 0, 0.0, k_last)

    def apply(self, src, c, a):
        v = src[c, a]
        r = self.res[c, a] - self.dia[a] * v
        r = r + self.wi[a] * src[c, a + 1]
        r = r + self.wi[a - 1] * src[c, a - 1]
        r = r + self.wjp[a] * roll(v, -1, 0)
        r = r + self.wjm[a] * roll(v, 1, 0)
        r = r + self.wkp[a] * roll(v, -1, 1)
        r = r + self.wkm[a] * roll(v, 1, 1)
        return v, r

    def buffers(self, t):
        return (self.even, self.odd) if t % 2 == 0 else (self.odd, self.even)

    def iterate(self, t, start, stop):
        keep, gain = ratios()[t]
        src, dst = self.buffers(t)

        def plane(a, inner):
            for c in range(3):
                v, r = self.apply(src, c, a)
                self.res[c, a] = r
                dst[c, a] = keep * v + gain * r
                if inner:
                    self.sol[c, a - GO] = v if t == 0 else self.sol[c, a - GO] + v

        low, high = min(max(start, GO), stop), max(min(stop, GO + B), start)
        loop(start, low, lambda a: plane(a, False))
        loop(low, high, lambda a: plane(a, True))
        loop(high, stop, lambda a: plane(a, False))


def loop(start, stop, body):
    if start < stop:
        lax.fori_loop(start, stop, lambda a, _: (body(a), 0)[1], 0)


def solve_inner_kernel(coef, o_coef, *state):
    solver = Solver(state)
    loop(0, B, lambda i: solver.put(i + GO, coef[i], o_coef[i]))
    loop(GO + 1, GO + B - 1, solver.force)
    loop(GO + 1, GO + B - 1, solver.weigh)
    for t in range(ITERS - 1):
        solver.iterate(t, GO + 2 + t, GO + B - 2 - t)


def solve_outer_kernel(near, far, o_near, o_far, *refs):
    state = refs[14:28]
    out, rows, flat = refs[28:]
    solver = Solver(state)
    even, odd = parity()
    place = lax.axis_index("space")
    bottom = lax.axis_index("slab") == 0
    tail = slice(4 * B * ITERS, 4 * B * ITERS + 16)
    for halo, others, top in ((near, o_near, even), (far, o_far, odd)):
        for t in range(ITERS):
            part = slice(4 * B * t, 4 * B * (t + 1))
            solver.put(1 + t + (GO + B - 1) * top, halo[part], others[part])
        (solver.s0[(N - 1) * top],) = joined(halo[tail], others[tail])

    loop(1, GO + 1, solver.force)
    loop(GO + B - 1, N - 1, solver.force)
    solver.wi[1] = 1.0 + 0.5 * (solver.ex[1] + solver.ex[2])
    loop(2, GO + 1, solver.weigh)
    loop(GO + B - 1, N - 2, solver.weigh)

    @pl.when(place == 0)
    def _():
        solver.wi[GO - 1] = jnp.zeros((J, K), jnp.float32)

    @pl.when(place == lax.axis_size("space") - 1)
    def _():
        solver.wi[GO + B - 1] = jnp.zeros((J, K), jnp.float32)

    for t in range(ITERS - 1):
        solver.iterate(t, 2 + t, GO + 2 + t)
        solver.iterate(t, GO + B - 2 - t, N - 2 - t)

    keep, gain = ratios()[ITERS - 1]
    src, _ = solver.buffers(ITERS - 1)
    third = lax.broadcasted_iota(jnp.int32, (B, K), 1) % 3
    target = lax.broadcasted_iota(jnp.int32, (K // 3, K), 0)
    source = lax.broadcasted_iota(jnp.int32, (K // 3, K), 1) // 3
    pick = jnp.where(target == source, 1.0, 0.0).astype(jnp.bfloat16)
    pick = jnp.concatenate([pick, pick, pick], 1)
    rows[9 * B :] = jnp.zeros((128 - 9 * B, K), jnp.float32)

    def finish(i):
        a = i + GO
        for c in range(3):
            v, r = solver.apply(src, c, a)
            total = solver.sol[c, i] + v + (keep * v + gain * r)
            mine = jnp.where(bottom, total[:B], total[B:])
            for q in range(3):
                g = 3 * c + q
                rows[B * g : B * g + B] = jnp.where(third == q, mine, 0.0)
        value = rows[...]
        high, low = halves(value)
        rest = value - high.astype(jnp.float32) - low.astype(jnp.float32)
        flat[pl.ds(i, K // 3, stride=B), :] = lax.dot_general(
            pick,
            jnp.concatenate([high, low, rest.astype(jnp.bfloat16)], 1),
            (((1,), (1,)), ((), ())),
            preferred_element_type=jnp.float32,
        )

    loop(0, B, finish)
    for n in range(out.shape[0]):
        out[n] = flat[B * n : B * (n + 1), :]


def unpack_kernel(got, out, flat):
    for n in range(got.shape[0]):
        flat[B * n : B * (n + 1), :] = got[n]
    for t in range(flat.shape[0] // 128):
        turned = flat[128 * t : 128 * (t + 1), :].T
        for c in range(3):
            for q in range(3):
                g = 3 * c + q
                out[c, q, :, 128 * t : 128 * (t + 1)] = turned[B * g : B * g + B]


def call(kernel, shapes, inputs, scratch=(), grant=8, extra=(), aliases={}, hbm_in=(), hbm_out=()):
    return pl.pallas_call(
        kernel,
        out_shape=[
            s if hasattr(s, "dtype") else jax.ShapeDtypeStruct(s, jnp.float32) for s in shapes
        ],
        in_specs=[HBM if n in hbm_in else VMEM for n in range(len(inputs))],
        out_specs=[HBM if n in hbm_out else VMEM for n in range(len(shapes))],
        scratch_shapes=[pltpu.VMEM(s, jnp.float32) for s in scratch] + list(extra),
        input_output_aliases=aliases,
        compiler_params=pltpu.CompilerParams(vmem_limit_bytes=int(grant * 1024 * 1024)),
    )(*inputs)


def program(phases, mobility, active, variants):
    count = lax.axis_size("space")

    def pairs(first):
        forward = [(i, i + 1) for i in range(first, count - 1, 2)]
        return forward + [(b, a) for a, b in forward]

    def exchange(to_near, to_far):
        far = lax.ppermute(to_far, "space", pairs(1))
        near = lax.ppermute(to_near, "space", pairs(0))
        return near, far

    def swap(array):
        return lax.ppermute(array, "slab", [(0, 1), (1, 0)])

    ph = jnp.transpose(phases, (1, 2, 0, 3))
    to_near, to_far, to_other = call(
        pack_kernel,
        [(H * B + 1, F, K)] * 3,
        [ph, mobility[None], active[0, 0].T],
        hbm_in=(0,),
        extra=[pltpu.SemaphoreType.DMA((2 * H + B,))],
        grant=61,
    )
    across = swap(to_other)
    near, far = exchange(to_near, to_far)
    block = (B + 2 * H, W + 2, F, K)
    coefs = (B, 4 * B, K)
    first, second, evolved, coef, mix = call(
        relax_inner_kernel,
        [block, block, (B, B, F, K), coefs, jax.ShapeDtypeStruct((12 * B, 3 * B * F), jnp.bfloat16)],
        [ph, to_other, across, variants.T],
        [(3, 2, F, K), (B - 6, B, F, K)],
        grant=4,
        extra=[pltpu.SemaphoreType.DMA((B - 6,))],
        hbm_out=(2,),
    )
    message = (4 * B * ITERS + 16, K)
    first, second, evolved, coef, to_near, to_far = call(
        relax_outer_kernel,
        [block, block, (B, B, F, K), coefs, message, message],
        [near, far, swap(near), swap(far), to_other, across, mix, first, second, evolved, coef],
        [(3, 2, F, K), (2 * H, B, F, K)],
        grant=4,
        aliases={7: 0, 8: 1, 9: 2, 10: 3},
        extra=[pltpu.SemaphoreType.DMA((2 * H,))],
        hbm_in=(9,),
        hbm_out=(2,),
    )
    o_coef = swap(coef)
    near, far = exchange(to_near, to_far)
    shapes = [(N, J, K)] * 10 + [(3, N, J, K)] * 3 + [(3, B, J, K)]
    state = call(solve_inner_kernel, shapes, [coef, o_coef], grant=4)
    packed = call(
        solve_outer_kernel,
        shapes + [(K // 3, B, 128)],
        [near, far, swap(near), swap(far), *state],
        [(128, K), (K // 3 * B, 128)],
        grant=8,
        aliases={4 + n: n for n in range(14)},
    )[-1]
    arrived = lax.all_to_all(packed, "space", 0, 0, tiled=True)
    (displacement,) = call(
        unpack_kernel, [(3, K // count, B, count * B)], [arrived], [(count * B, 128)]
    )
    return jnp.transpose(evolved, (2, 0, 1, 3)), displacement


def solution(mesh):
    placed = (P(None, "space", "slab", None), P(), P("space", "slab", None, None), P())
    return jax.shard_map(
        program,
        mesh=mesh,
        in_specs=placed,
        out_specs=(P(None, "space", "slab", None), P(None, "space", "slab", None)),
        check_vma=False,
    )
```

```python
import jax
import jax.numpy as jnp
from jax import lax
from jax.experimental import pallas as pl
from jax.experimental.pallas import tpu as pltpu
from jax.sharding import PartitionSpec as P


ITERS = 4
DIAGONAL_SHIFT = 3.0
SPECTRUM_CENTRE = 12.0
SPECTRUM_RADIUS = 9.0

B = 12
F = 8
K = 384
H = 3
W = B + H
REST = H * H + 1
GO = ITERS + 1
HIGHEST = lax.Precision.HIGHEST
VMEM = pl.BlockSpec(memory_space=pltpu.VMEM)
HBM = pl.BlockSpec(memory_space=pltpu.HBM)


def roll(x, shift, axis):
    return pltpu.roll(x, shift % x.shape[axis], axis)


def parity():
    even = 1 - lax.axis_index("space") % 2
    return even, 1 - even


def pack_kernel(ph, rates, to_near, to_far, to_other, speed_out):
    even, odd = parity()
    slab = lax.axis_index("slab")
    start = (B - H) * (1 - slab)
    for message, top in ((to_far, odd), (to_near, even)):
        for t in range(H):
            source = ph.at[(B - H) * top + t]
            message[H * t : H * (t + 1)] = source[pl.ds(start, H)]
            rest = REST + (B - H) * t
            message[rest : rest + B - H] = source[pl.ds(H * slab, B - H)]
    for i in range(B):
        to_other[H * i : H * (i + 1)] = ph[i, pl.ds(start, H)]
    bricks = K // B
    brick = lax.broadcasted_iota(jnp.int32, (bricks, K), 0)
    spread = jnp.where(brick == lax.broadcasted_iota(jnp.int32, (bricks, K), 1) // B, 1.0, 0.0)
    speed = jnp.dot(
        rates[...], spread, precision=HIGHEST, preferred_element_type=jnp.float32
    )
    to_near[REST - 1] = speed
    to_far[REST - 1] = speed
    to_other[H * B] = speed
    speed_out[...] = speed


def update(x, around, s):
    lane = lax.broadcasted_iota(jnp.int32, (F, K), 1)
    square = x * x
    total = square + roll(square, 4, 0)
    total = total + roll(total, 2, 0)
    total = total + roll(total, 1, 0)
    left = jnp.where(lane == 0, 0.0, roll(x, 1, 1))
    right = jnp.where(lane == K - 1, 0.0, roll(x, -1, 1))
    summed = around + (left + right)
    return x - s * (x * (5.0 + 3.0 * total - 2.0 * square) - summed)


def window_step(src, dst, speed, depth, count, place):
    slab = lax.axis_index("slab")

    def plane(n, _):
        a = place(n)
        group = (a >= H).astype(jnp.int32) + (a >= H + B).astype(jnp.int32)
        edge = depth * slab
        before = src[a, edge]
        x = src[a, edge + 1]
        for w in range(W - depth):
            after = src[a, edge + w + 2]
            whose = slab if w < H - depth else (1 - slab if w >= B else 0)
            around = (before + after) + (src[a - 1, edge + w + 1] + src[a + 1, edge + w + 1])
            dst[a, edge + w + 1] = update(x, around, speed[group, whose])
            before, x = x, after
        return 0

    lax.fori_loop(0, count, plane, 0)


def halves(x):
    high = x.astype(jnp.bfloat16)
    return high, (x - high.astype(jnp.float32)).astype(jnp.bfloat16)


def last_step(src, own_speed, mix, ev, coef, count, place, staged, sems):
    own = 1 + H * lax.axis_index("slab")
    row = lax.broadcasted_iota(jnp.int32, (4 * B, K), 0)
    is_excess = (row >= B) & (row < 2 * B)

    def plane(n, _):
        a = place(n)
        i = a - H
        before = src[a, own - 1]
        x = src[a, own]
        squares = []
        for j in range(B):
            after = src[a, own + j + 1]
            around = (before + after) + (src[a - 1, own + j] + src[a + 1, own + j])
            value = update(x, around, own_speed[...])
            staged[n, j] = value
            squares.append(value * value)
            before, x = x, after
        pltpu.make_async_copy(staged.at[n], ev.at[i], sems.at[n]).start()
        high, low = halves(jnp.concatenate(squares, 0))
        mixed = jnp.dot(
            mix[...],
            jnp.concatenate([high, low, high], 0),
            preferred_element_type=jnp.float32,
        )
        total = mixed[: 4 * B]
        strain = mixed[4 * B : 8 * B]
        dilation = mixed[8 * B :]
        saturation = total / (1.0 + total)
        excess = 0.5 * saturation
        stress = (1.5 + saturation) * dilation + 2.0 * (1.0 + excess) * strain
        coef[i] = jnp.where(is_excess, excess, stress)
        return 0

    lax.fori_loop(0, count, plane, 0)

    def settle(n, _):
        pltpu.make_async_copy(staged.at[n], ev.at[place(n) - H], sems.at[n]).wait()
        return 0

    lax.fori_loop(0, count, settle, 0)


def relax_inner_kernel(
    ph, mine, across, variants, first, second, ev, coef, mix, speed, staged, sems
):
    slab = lax.axis_index("slab")
    own = 1 + H * slab
    other = 1 + B * (1 - slab)
    zero = jnp.zeros((F, K), jnp.float32)
    speed[1, 0] = mine[...]
    speed[1, 1] = across[H * B]

    v = variants[...]
    each = jnp.concatenate([v[:1], jnp.zeros((1, F)), v[1:]], 0)
    whole = jnp.broadcast_to(v[:1] + v[1:2] + v[2:], (4, F))
    table = jnp.concatenate([jnp.ones((4, F)), each, whole], 0)
    shape = (12 * B, B * F)
    group = lax.broadcasted_iota(jnp.int32, (12 * B, 12), 0) // B
    down = jnp.where(group == lax.broadcasted_iota(jnp.int32, (12 * B, 12), 1), 1.0, 0.0)
    field = lax.broadcasted_iota(jnp.int32, (F, B * F), 1) % F
    along = jnp.where(field == lax.broadcasted_iota(jnp.int32, (F, B * F), 0), 1.0, 0.0)
    table = jnp.dot(down, table, precision=HIGHEST, preferred_element_type=jnp.float32)
    table = jnp.dot(table, along, precision=HIGHEST, preferred_element_type=jnp.float32)
    same = lax.broadcasted_iota(jnp.int32, shape, 0) % B
    same = same == lax.broadcasted_iota(jnp.int32, shape, 1) // F
    high, low = halves(jnp.where(same, table, 0.0))
    mix[...] = jnp.concatenate([high, high, low], 1)

    def clear(a, _):
        for buf in (first, second):
            buf[a, 0] = zero
            buf[a, W + 1] = zero
        return 0

    lax.fori_loop(0, B + 2 * H, clear, 0)

    def fill(i, _):
        for j in range(B):
            first[H + i, own + j] = ph[i, j]
        for t in range(H):
            first[H + i, other + t] = across[H * i + t]
        return 0

    lax.fori_loop(0, B, fill, 0)
    window_step(first, second, speed, 1, B - 2, lambda n: H + 1 + n)
    window_step(second, first, speed, 2, B - 4, lambda n: H + 2 + n)
    last_step(first, speed.at[1, 0], mix, ev, coef, B - 6, lambda n: H + 3 + n, staged, sems)


def relax_outer_kernel(
    near, far, c_near, c_far, mine, across, mix, first_in, second_in, ev_in, coef_in,
    first, second, ev, coef, m_near, m_far, speed, staged, sems,
):
    even, odd = parity()
    slab = lax.axis_index("slab")
    own = 1 + H * slab
    other = 1 + B * (1 - slab)
    speed[1, 0] = mine[...]
    speed[1, 1] = across[H * B]
    for halo, corner, top in ((near, c_near, even), (far, c_far, odd)):
        speed[2 * top, 0] = halo[REST - 1]
        speed[2 * top, 1] = corner[REST - 1]
        for a in range(H):
            for t in range(H):
                first[(H + B) * top + a, own + (B - H) * (1 - slab) + t] = halo[H * a + t]
                first[(H + B) * top + a, other + t] = corner[H * a + t]
            for m in range(B - H):
                first[(H + B) * top + a, own + H * slab + m] = halo[REST + (B - H) * a + m]

    def ends(depth):
        jump = B + H - 2 * depth - 1
        return lambda n: depth + n + jnp.where(n >= H, jump + 1 - H, 0)

    window_step(first, second, speed, 1, 2 * H, ends(1))
    window_step(second, first, speed, 2, 2 * H, ends(2))
    last_step(first, speed.at[1, 0], mix, ev, coef, 2 * H, ends(3), staged, sems)
    for message, top in ((m_near, even), (m_far, odd)):
        for t in range(ITERS):
            message[4 * B * t : 4 * B * (t + 1)] = coef[(B - ITERS) * top + t]
        message[4 * B * ITERS :] = coef[ITERS + (B - 2 * ITERS - 1) * top, :16]


J = B + ITERS
N = B + 2 * GO


def ratios():
    ratio = SPECTRUM_RADIUS / SPECTRUM_CENTRE
    out = []
    for _ in range(ITERS):
        ratio_next = 1.0 / (2.0 * SPECTRUM_CENTRE / SPECTRUM_RADIUS - ratio)
        out.append((ratio_next * ratio, 2.0 * ratio_next / SPECTRUM_RADIUS))
        ratio = ratio_next
    return out


def joined(mine, others):
    bottom = lax.axis_index("slab") == 0
    lo = jnp.where(bottom, mine, others)
    hi = jnp.where(bottom, others, mine)
    n = mine.shape[0] // B
    return [jnp.concatenate([lo[B * c : B * c + B], hi[B * c : B * c + B]], 0) for c in range(n)]


class Solver:
    def __init__(self, state):
        self.s0, self.s1, self.s2, self.ex = state[:4]
        self.dia, self.wi, self.wjp, self.wjm, self.wkp, self.wkm = state[4:10]
        self.even, self.odd, self.sol = state[10:]
        self.row = lax.broadcasted_iota(jnp.int32, (J, K), 0)
        self.lane = lax.broadcasted_iota(jnp.int32, (J, K), 1)

    def window(self, x):
        return jnp.where(lax.axis_index("slab") == 0, x[:J], x[2 * B - J :])

    def put(self, a, mine, others):
        s0, ex, s1, s2 = joined(mine, others)
        self.s1[a] = s1
        self.s0[a], self.ex[a], self.s2[a] = self.window(s0), self.window(ex), self.window(s2)

    def next_j(self, x):
        return jnp.where(self.row == J - 1, 0.0, roll(x, -1, 0))

    def last_j(self, x):
        return jnp.where(self.row == 0, 0.0, roll(x, 1, 0))

    def next_k(self, x):
        return jnp.where(self.lane == K - 1, 0.0, roll(x, -1, 1))

    def last_k(self, x):
        return jnp.where(self.lane == 0, 0.0, roll(x, 1, 1))

    def force(self, a):
        s1 = self.s1[a]
        row = lax.broadcasted_iota(jnp.int32, (2 * B, K), 0)
        ahead = jnp.where(row == 2 * B - 1, 0.0, roll(s1, -1, 0))
        behind = jnp.where(row == 0, 0.0, roll(s1, 1, 0))
        forcing = (
            0.5 * (self.s0[a + 1] - self.s0[a - 1]),
            0.5 * self.window(ahead - behind),
            0.5 * (self.next_k(self.s2[a]) - self.last_k(self.s2[a])),
        )
        for c in range(3):
            self.even[c, a] = forcing[c] / SPECTRUM_CENTRE

    def weigh(self, a):
        e = self.ex[a]
        i_next = 1.0 + 0.5 * (e + self.ex[a + 1])
        i_last = 1.0 + 0.5 * (e + self.ex[a - 1])
        j_next = 1.0 + 0.5 * (e + self.next_j(e))
        j_last = 1.0 + 0.5 * (e + self.last_j(e))
        k_next = 1.0 + 0.5 * (e + self.next_k(e))
        k_last = 1.0 + 0.5 * (e + self.last_k(e))
        ends = (i_next + i_last) + (j_next + j_last) + (k_next + k_last)
        self.dia[a] = DIAGONAL_SHIFT + ends
        self.wi[a] = i_next
        self.wjp[a] = jnp.where(self.row == J - 1, 0.0, j_next)
        self.wjm[a] = jnp.where(self.row == 0, 0.0, j_last)
        self.wkp[a] = jnp.where(self.lane == K - 1, 0.0, k_next)
        self.wkm[a] = jnp.where(self.lane == 0, 0.0, k_last)

    def buffers(self, t):
        return (self.even, self.odd) if t % 2 == 0 else (self.odd, self.even)

    def advance(self, t, a):
        keep, gain = ratios()[t]
        if t == 0:
            now, past = keep + SPECTRUM_CENTRE * gain, 0.0
        else:
            keep_past, gain_past = ratios()[t - 1]
            now, past = keep + gain / gain_past, gain * keep_past / gain_past
        src, dst = self.buffers(t)
        centre = now - gain * self.dia[a]
        out = []
        for c in range(3):
            v = src[c, a]
            side = self.wi[a] * src[c, a + 1] + self.wi[a - 1] * src[c, a - 1]
            side = side + (self.wjp[a] * roll(v, -1, 0) + self.wjm[a] * roll(v, 1, 0))
            side = side + (self.wkp[a] * roll(v, -1, 1) + self.wkm[a] * roll(v, 1, 1))
            new = centre * v + gain * side
            out.append((v, new - past * dst[c, a] if t else new))
        return out

    def iterate(self, t, start, stop):
        dst = self.buffers(t)[1]

        def plane(a, inner):
            for c, (v, new) in enumerate(self.advance(t, a)):
                dst[c, a] = new
                if inner:
                    self.sol[c, a - GO] = v if t == 0 else self.sol[c, a - GO] + v

        low, high = min(max(start, GO), stop), max(min(stop, GO + B), start)
        loop(start, low, lambda a: plane(a, False))
        loop(low, high, lambda a: plane(a, True))
        loop(high, stop, lambda a: plane(a, False))


def loop(start, stop, body):
    if start < stop:
        lax.fori_loop(start, stop, lambda a, _: (body(a), 0)[1], 0)


def solve_inner_kernel(coef, o_coef, *state):
    solver = Solver(state)
    loop(0, B, lambda i: solver.put(i + GO, coef[i], o_coef[i]))
    loop(GO + 1, GO + B - 1, solver.force)
    loop(GO + 1, GO + B - 1, solver.weigh)
    for t in range(ITERS - 1):
        solver.iterate(t, GO + 2 + t, GO + B - 2 - t)


def solve_outer_kernel(near, far, o_near, o_far, *refs):
    state = refs[13:26]
    out, rows, flat = refs[26:]
    solver = Solver(state)
    even, odd = parity()
    place = lax.axis_index("space")
    bottom = lax.axis_index("slab") == 0
    tail = slice(4 * B * ITERS, 4 * B * ITERS + 16)
    for halo, others, top in ((near, o_near, even), (far, o_far, odd)):
        for t in range(ITERS):
            part = slice(4 * B * t, 4 * B * (t + 1))
            solver.put(1 + t + (GO + B - 1) * top, halo[part], others[part])
        solver.s0[(N - 1) * top] = solver.window(joined(halo[tail], others[tail])[0])

    loop(1, GO + 1, solver.force)
    loop(GO + B - 1, N - 1, solver.force)
    solver.wi[1] = 1.0 + 0.5 * (solver.ex[1] + solver.ex[2])
    loop(2, GO + 1, solver.weigh)
    loop(GO + B - 1, N - 2, solver.weigh)

    @pl.when(place == 0)
    def _():
        solver.wi[GO - 1] = jnp.zeros((J, K), jnp.float32)

    @pl.when(place == lax.axis_size("space") - 1)
    def _():
        solver.wi[GO + B - 1] = jnp.zeros((J, K), jnp.float32)

    for t in range(ITERS - 1):
        solver.iterate(t, 2 + t, GO + 2 + t)
        solver.iterate(t, GO + B - 2 - t, N - 2 - t)

    third = lax.broadcasted_iota(jnp.int32, (B, K), 1) % 3
    target = lax.broadcasted_iota(jnp.int32, (K // 3, K), 0)
    source = lax.broadcasted_iota(jnp.int32, (K // 3, K), 1) // 3
    pick = jnp.where(target == source, 1.0, 0.0).astype(jnp.bfloat16)
    pick = jnp.concatenate([pick, pick], 1)
    rows[9 * B :] = jnp.zeros((128 - 9 * B, K), jnp.float32)

    def finish(i):
        a = i + GO
        for c, (v, new) in enumerate(solver.advance(ITERS - 1, a)):
            total = solver.sol[c, i] + v + new
            mine = jnp.where(bottom, total[:B], total[J - B :])
            for q in range(3):
                g = 3 * c + q
                rows[B * g : B * g + B] = jnp.where(third == q, mine, 0.0)
        high, low = halves(rows[...])
        flat[pl.ds(i, K // 3, stride=B), :] = lax.dot_general(
            pick,
            jnp.concatenate([high, low], 1),
            (((1,), (1,)), ((), ())),
            preferred_element_type=jnp.float32,
        )

    loop(0, B, finish)
    for n in range(out.shape[0]):
        out[n] = flat[B * n : B * (n + 1), :]


def unpack_kernel(got, out, flat):
    for n in range(got.shape[0]):
        flat[B * n : B * (n + 1), :] = got[n]
    for t in range(flat.shape[0] // 128):
        turned = flat[128 * t : 128 * (t + 1), :].T
        for c in range(3):
            for q in range(3):
                g = 3 * c + q
                out[c, q, :, 128 * t : 128 * (t + 1)] = turned[B * g : B * g + B]


def call(kernel, shapes, inputs, scratch=(), grant=8, extra=(), aliases={}, hbm_in=(), hbm_out=()):
    return pl.pallas_call(
        kernel,
        out_shape=[
            s if hasattr(s, "dtype") else jax.ShapeDtypeStruct(s, jnp.float32) for s in shapes
        ],
        in_specs=[HBM if n in hbm_in else VMEM for n in range(len(inputs))],
        out_specs=[HBM if n in hbm_out else VMEM for n in range(len(shapes))],
        scratch_shapes=[pltpu.VMEM(s, jnp.float32) for s in scratch] + list(extra),
        input_output_aliases=aliases,
        compiler_params=pltpu.CompilerParams(vmem_limit_bytes=int(grant * 1024 * 1024)),
    )(*inputs)


def program(phases, mobility, active, variants):
    count = lax.axis_size("space")

    def pairs(first):
        forward = [(i, i + 1) for i in range(first, count - 1, 2)]
        return forward + [(b, a) for a, b in forward]

    def exchange(to_near, to_far):
        far = lax.ppermute(to_far, "space", pairs(1))
        near = lax.ppermute(to_near, "space", pairs(0))
        return near, far

    def swap(array):
        return lax.ppermute(array, "slab", [(0, 1), (1, 0)])

    ph = jnp.transpose(phases, (1, 2, 0, 3))
    rates = mobility[:, None] * active[0, 0].T.astype(jnp.float32)
    to_near, to_far, to_other, speed = call(
        pack_kernel, [(H * B + 1, F, K)] * 3 + [(F, K)], [ph, rates], grant=4
    )
    across = swap(to_other)
    near, far = exchange(to_near, to_far)
    block = (B + 2 * H, W + 2, F, K)
    coefs = (B, 4 * B, K)
    first, second, evolved, coef, mix = call(
        relax_inner_kernel,
        [block, block, (B, B, F, K), coefs, jax.ShapeDtypeStruct((12 * B, 3 * B * F), jnp.bfloat16)],
        [ph, speed, across, variants.T],
        [(3, 2, F, K), (B - 6, B, F, K)],
        grant=4,
        extra=[pltpu.SemaphoreType.DMA((B - 6,))],
        hbm_out=(2,),
    )
    message = (4 * B * ITERS + 16, K)
    first, second, evolved, coef, to_near, to_far = call(
        relax_outer_kernel,
        [block, block, (B, B, F, K), coefs, message, message],
        [near, far, swap(near[:REST]), swap(far[:REST]), speed, across, mix, first, second, evolved, coef],
        [(3, 2, F, K), (2 * H, B, F, K)],
        grant=4,
        aliases={7: 0, 8: 1, 9: 2, 10: 3},
        extra=[pltpu.SemaphoreType.DMA((2 * H,))],
        hbm_in=(9,),
        hbm_out=(2,),
    )
    o_coef = swap(coef)
    near, far = exchange(to_near, to_far)
    shapes = [(N, J, K), (N, 2 * B, K)] + [(N, J, K)] * 8 + [(3, N, J, K)] * 2 + [(3, B, J, K)]
    state = call(solve_inner_kernel, shapes, [coef, o_coef], grant=4)
    packed = call(
        solve_outer_kernel,
        shapes + [(K // 3, B, 128)],
        [near, far, swap(near), swap(far), *state],
        [(128, K), (K // 3 * B, 128)],
        grant=8,
        aliases={4 + n: n for n in range(13)},
    )[-1]
    arrived = lax.all_to_all(packed, "space", 0, 0, tiled=True)
    (displacement,) = call(
        unpack_kernel, [(3, K // count, B, count * B)], [arrived], [(count * B, 128)]
    )
    return jnp.transpose(evolved, (2, 0, 1, 3)), displacement


def solution(mesh):
    placed = (P(None, "space", "slab", None), P(), P("space", "slab", None, None), P())
    return jax.shard_map(
        program,
        mesh=mesh,
        in_specs=placed,
        out_specs=(P(None, "space", "slab", None), P(None, "space", "slab", None)),
        check_vma=False,
    )
```

```python
import jax
import jax.numpy as jnp
from jax import lax
from jax.experimental import pallas as pl
from jax.experimental.pallas import tpu as pltpu
from jax.sharding import PartitionSpec as P


ITERS = 4
DIAGONAL_SHIFT = 3.0
SPECTRUM_CENTRE = 12.0
SPECTRUM_RADIUS = 9.0

B = 12
F = 8
K = 384
H = 3
W = B + H
REST = H * H + 1
GO = ITERS + 1
HIGHEST = lax.Precision.HIGHEST
VMEM = pl.BlockSpec(memory_space=pltpu.VMEM)
HBM = pl.BlockSpec(memory_space=pltpu.HBM)


def roll(x, shift, axis):
    return pltpu.roll(x, shift % x.shape[axis], axis)


def parity():
    even = 1 - lax.axis_index("space") % 2
    return even, 1 - even


def pack_kernel(ph, rates, to_near, to_far, to_other, speed_out):
    even, odd = parity()
    slab = lax.axis_index("slab")
    start = (B - H) * (1 - slab)
    for message, top in ((to_far, odd), (to_near, even)):
        for t in range(H):
            source = ph.at[(B - H) * top + t]
            message[H * t : H * (t + 1)] = source[pl.ds(start, H)]
            rest = REST + (B - H) * t
            message[rest : rest + B - H] = source[pl.ds(H * slab, B - H)]
    for i in range(B):
        to_other[H * i : H * (i + 1)] = ph[i, pl.ds(start, H)]
    bricks = K // B
    brick = lax.broadcasted_iota(jnp.int32, (bricks, K), 0)
    spread = jnp.where(brick == lax.broadcasted_iota(jnp.int32, (bricks, K), 1) // B, 1.0, 0.0)
    speed = jnp.dot(
        rates[...], spread, precision=HIGHEST, preferred_element_type=jnp.float32
    )
    to_near[REST - 1] = speed
    to_far[REST - 1] = speed
    to_other[H * B] = speed
    speed_out[...] = speed


def update(x, around, s):
    lane = lax.broadcasted_iota(jnp.int32, (F, K), 1)
    square = x * x
    total = square + roll(square, 4, 0)
    total = total + roll(total, 2, 0)
    total = total + roll(total, 1, 0)
    left = jnp.where(lane == 0, 0.0, roll(x, 1, 1))
    right = jnp.where(lane == K - 1, 0.0, roll(x, -1, 1))
    summed = around + (left + right)
    return x - s * (x * (5.0 + 3.0 * total - 2.0 * square) - summed)


def window_step(src, dst, speed, depth, count, place):
    slab = lax.axis_index("slab")

    def plane(n, _):
        a = place(n)
        group = (a >= H).astype(jnp.int32) + (a >= H + B).astype(jnp.int32)
        edge = depth * slab
        before = src[a, edge]
        x = src[a, edge + 1]
        for w in range(W - depth):
            after = src[a, edge + w + 2]
            whose = slab if w < H - depth else (1 - slab if w >= B else 0)
            around = (before + after) + (src[a - 1, edge + w + 1] + src[a + 1, edge + w + 1])
            dst[a, edge + w + 1] = update(x, around, speed[group, whose])
            before, x = x, after
        return 0

    lax.fori_loop(0, count, plane, 0)


def halves(x):
    high = x.astype(jnp.bfloat16)
    return high, (x - high.astype(jnp.float32)).astype(jnp.bfloat16)


def last_step(src, own_speed, mix, ev, coef, count, place, staged, sems):
    own = 1 + H * lax.axis_index("slab")
    row = lax.broadcasted_iota(jnp.int32, (4 * B, K), 0)
    is_excess = (row >= B) & (row < 2 * B)

    def plane(n, _):
        a = place(n)
        before = src[a, own - 1]
        x = src[a, own]
        for j in range(B):
            after = src[a, own + j + 1]
            around = (before + after) + (src[a - 1, own + j] + src[a + 1, own + j])
            staged[n, j] = update(x, around, own_speed[...])
            before, x = x, after
        pltpu.make_async_copy(staged.at[n], ev.at[a - H], sems.at[n]).start()
        return 0

    lax.fori_loop(0, count, plane, 0)
    for n in range(count):
        values = staged[n].reshape(B * F, K)
        high, low = halves(values * values)
        mixed = jnp.dot(
            mix[...],
            jnp.concatenate([high, low, high], 0),
            preferred_element_type=jnp.float32,
        )
        total = mixed[: 4 * B]
        strain = mixed[4 * B : 8 * B]
        dilation = mixed[8 * B :]
        saturation = total / (1.0 + total)
        excess = 0.5 * saturation
        stress = (1.5 + saturation) * dilation + 2.0 * (1.0 + excess) * strain
        coef[place(n) - H] = jnp.where(is_excess, excess, stress)

    def settle(n, _):
        pltpu.make_async_copy(staged.at[n], ev.at[place(n) - H], sems.at[n]).wait()
        return 0

    lax.fori_loop(0, count, settle, 0)


def relax_inner_kernel(
    ph, mine, across, variants, first, second, ev, coef, mix, speed, staged, sems
):
    slab = lax.axis_index("slab")
    own = 1 + H * slab
    other = 1 + B * (1 - slab)
    zero = jnp.zeros((F, K), jnp.float32)
    speed[1, 0] = mine[...]
    speed[1, 1] = across[H * B]

    v = variants[...]
    each = jnp.concatenate([v[:1], jnp.zeros((1, F)), v[1:]], 0)
    whole = jnp.broadcast_to(v[:1] + v[1:2] + v[2:], (4, F))
    table = jnp.concatenate([jnp.ones((4, F)), each, whole], 0)
    shape = (12 * B, B * F)
    group = lax.broadcasted_iota(jnp.int32, (12 * B, 12), 0) // B
    down = jnp.where(group == lax.broadcasted_iota(jnp.int32, (12 * B, 12), 1), 1.0, 0.0)
    field = lax.broadcasted_iota(jnp.int32, (F, B * F), 1) % F
    along = jnp.where(field == lax.broadcasted_iota(jnp.int32, (F, B * F), 0), 1.0, 0.0)
    table = jnp.dot(down, table, precision=HIGHEST, preferred_element_type=jnp.float32)
    table = jnp.dot(table, along, precision=HIGHEST, preferred_element_type=jnp.float32)
    same = lax.broadcasted_iota(jnp.int32, shape, 0) % B
    same = same == lax.broadcasted_iota(jnp.int32, shape, 1) // F
    high, low = halves(jnp.where(same, table, 0.0))
    mix[...] = jnp.concatenate([high, high, low], 1)

    def clear(a, _):
        for buf in (first, second):
            buf[a, 0] = zero
            buf[a, W + 1] = zero
        return 0

    lax.fori_loop(0, B + 2 * H, clear, 0)

    def fill(i, _):
        for j in range(B):
            first[H + i, own + j] = ph[i, j]
        for t in range(H):
            first[H + i, other + t] = across[H * i + t]
        return 0

    lax.fori_loop(0, B, fill, 0)
    window_step(first, second, speed, 1, B - 2, lambda n: H + 1 + n)
    window_step(second, first, speed, 2, B - 4, lambda n: H + 2 + n)
    last_step(first, speed.at[1, 0], mix, ev, coef, B - 6, lambda n: H + 3 + n, staged, sems)


def relax_outer_kernel(
    near, far, c_near, c_far, mine, across, mix, first_in, second_in, ev_in, coef_in,
    first, second, ev, coef, m_near, m_far, speed, staged, sems,
):
    even, odd = parity()
    slab = lax.axis_index("slab")
    own = 1 + H * slab
    other = 1 + B * (1 - slab)
    speed[1, 0] = mine[...]
    speed[1, 1] = across[H * B]
    for halo, corner, top in ((near, c_near, even), (far, c_far, odd)):
        speed[2 * top, 0] = halo[REST - 1]
        speed[2 * top, 1] = corner[REST - 1]
        for a in range(H):
            for t in range(H):
                first[(H + B) * top + a, own + (B - H) * (1 - slab) + t] = halo[H * a + t]
                first[(H + B) * top + a, other + t] = corner[H * a + t]
            for m in range(B - H):
                first[(H + B) * top + a, own + H * slab + m] = halo[REST + (B - H) * a + m]

    def ends(depth):
        jump = B + H - 2 * depth - 1
        return lambda n: depth + n + (jump + 1 - H) * (n >= H)

    window_step(first, second, speed, 1, 2 * H, ends(1))
    window_step(second, first, speed, 2, 2 * H, ends(2))
    last_step(first, speed.at[1, 0], mix, ev, coef, 2 * H, ends(3), staged, sems)
    for message, top in ((m_near, even), (m_far, odd)):
        for t in range(ITERS):
            message[4 * B * t : 4 * B * (t + 1)] = coef[(B - ITERS) * top + t]
        message[4 * B * ITERS :] = coef[ITERS + (B - 2 * ITERS - 1) * top, :16]


J = B + ITERS
N = B + 2 * GO


def ratios():
    ratio = SPECTRUM_RADIUS / SPECTRUM_CENTRE
    out = []
    for _ in range(ITERS):
        ratio_next = 1.0 / (2.0 * SPECTRUM_CENTRE / SPECTRUM_RADIUS - ratio)
        out.append((ratio_next * ratio, 2.0 * ratio_next / SPECTRUM_RADIUS))
        ratio = ratio_next
    return out


def joined(mine, others):
    bottom = lax.axis_index("slab") == 0
    lo = jnp.where(bottom, mine, others)
    hi = jnp.where(bottom, others, mine)
    n = mine.shape[0] // B
    return [jnp.concatenate([lo[B * c : B * c + B], hi[B * c : B * c + B]], 0) for c in range(n)]


class Solver:
    def __init__(self, state):
        self.s0, self.s1, self.s2, self.ex = state[:4]
        self.dia, self.wi, self.wjp, self.wjm, self.wkp, self.wkm = state[4:10]
        self.even, self.odd, self.sol = state[10:]
        self.row = lax.broadcasted_iota(jnp.int32, (J, K), 0)
        self.lane = lax.broadcasted_iota(jnp.int32, (J, K), 1)

    def window(self, x):
        return jnp.where(lax.axis_index("slab") == 0, x[:J], x[2 * B - J :])

    def put(self, a, mine, others):
        s0, ex, s1, s2 = joined(mine, others)
        self.s1[a] = s1
        self.s0[a], self.ex[a], self.s2[a] = self.window(s0), self.window(ex), self.window(s2)

    def next_j(self, x):
        return jnp.where(self.row == J - 1, 0.0, roll(x, -1, 0))

    def last_j(self, x):
        return jnp.where(self.row == 0, 0.0, roll(x, 1, 0))

    def next_k(self, x):
        return jnp.where(self.lane == K - 1, 0.0, roll(x, -1, 1))

    def last_k(self, x):
        return jnp.where(self.lane == 0, 0.0, roll(x, 1, 1))

    def force(self, a):
        s1 = self.s1[a]
        row = lax.broadcasted_iota(jnp.int32, (2 * B, K), 0)
        ahead = jnp.where(row == 2 * B - 1, 0.0, roll(s1, -1, 0))
        behind = jnp.where(row == 0, 0.0, roll(s1, 1, 0))
        forcing = (
            0.5 * (self.s0[a + 1] - self.s0[a - 1]),
            0.5 * self.window(ahead - behind),
            0.5 * (self.next_k(self.s2[a]) - self.last_k(self.s2[a])),
        )
        for c in range(3):
            self.even[c, a] = forcing[c] / SPECTRUM_CENTRE

    def weigh(self, a):
        e = self.ex[a]
        i_next = 1.0 + 0.5 * (e + self.ex[a + 1])
        i_last = 1.0 + 0.5 * (e + self.ex[a - 1])
        j_next = 1.0 + 0.5 * (e + self.next_j(e))
        j_last = 1.0 + 0.5 * (e + self.last_j(e))
        k_next = 1.0 + 0.5 * (e + self.next_k(e))
        k_last = 1.0 + 0.5 * (e + self.last_k(e))
        ends = (i_next + i_last) + (j_next + j_last) + (k_next + k_last)
        self.dia[a] = DIAGONAL_SHIFT + ends
        self.wi[a] = i_next
        self.wjp[a] = jnp.where(self.row == J - 1, 0.0, j_next)
        self.wjm[a] = jnp.where(self.row == 0, 0.0, j_last)
        self.wkp[a] = jnp.where(self.lane == K - 1, 0.0, k_next)
        self.wkm[a] = jnp.where(self.lane == 0, 0.0, k_last)

    def buffers(self, t):
        return (self.even, self.odd) if t % 2 == 0 else (self.odd, self.even)

    def advance(self, t, a):
        keep, gain = ratios()[t]
        if t == 0:
            now, past = keep + SPECTRUM_CENTRE * gain, 0.0
        else:
            keep_past, gain_past = ratios()[t - 1]
            now, past = keep + gain / gain_past, gain * keep_past / gain_past
        src, dst = self.buffers(t)
        centre = now - gain * self.dia[a]
        out = []
        for c in range(3):
            v = src[c, a]
            side = self.wi[a] * src[c, a + 1] + self.wi[a - 1] * src[c, a - 1]
            side = side + (self.wjp[a] * roll(v, -1, 0) + self.wjm[a] * roll(v, 1, 0))
            side = side + (self.wkp[a] * roll(v, -1, 1) + self.wkm[a] * roll(v, 1, 1))
            new = centre * v + gain * side
            out.append((v, new - past * dst[c, a] if t else new))
        return out

    def iterate(self, t, start, stop):
        dst = self.buffers(t)[1]

        def plane(a, inner):
            for c, (v, new) in enumerate(self.advance(t, a)):
                dst[c, a] = new
                if inner:
                    self.sol[c, a - GO] = v if t == 0 else self.sol[c, a - GO] + v

        low, high = min(max(start, GO), stop), max(min(stop, GO + B), start)
        loop(start, low, lambda a: plane(a, False))
        loop(low, high, lambda a: plane(a, True))
        loop(high, stop, lambda a: plane(a, False))


def loop(start, stop, body):
    if start < stop:
        lax.fori_loop(start, stop, lambda a, _: (body(a), 0)[1], 0)


def solve_inner_kernel(coef, o_coef, *state):
    solver = Solver(state)
    loop(0, B, lambda i: solver.put(i + GO, coef[i], o_coef[i]))
    loop(GO + 1, GO + B - 1, solver.force)
    loop(GO + 1, GO + B - 1, solver.weigh)
    for t in range(ITERS - 1):
        solver.iterate(t, GO + 2 + t, GO + B - 2 - t)


def solve_outer_kernel(near, far, o_near, o_far, *refs):
    state = refs[13:26]
    out, rows = refs[26:]
    solver = Solver(state)
    even, odd = parity()
    place = lax.axis_index("space")
    bottom = lax.axis_index("slab") == 0
    tail = slice(4 * B * ITERS, 4 * B * ITERS + 16)
    for halo, others, top in ((near, o_near, even), (far, o_far, odd)):
        for t in range(ITERS):
            part = slice(4 * B * t, 4 * B * (t + 1))
            solver.put(1 + t + (GO + B - 1) * top, halo[part], others[part])
        solver.s0[(N - 1) * top] = solver.window(joined(halo[tail], others[tail])[0])

    loop(1, GO + 1, solver.force)
    loop(GO + B - 1, N - 1, solver.force)
    solver.wi[1] = 1.0 + 0.5 * (solver.ex[1] + solver.ex[2])
    loop(2, GO + 1, solver.weigh)
    loop(GO + B - 1, N - 2, solver.weigh)

    @pl.when(place == 0)
    def _():
        solver.wi[GO - 1] = jnp.zeros((J, K), jnp.float32)

    @pl.when(place == lax.axis_size("space") - 1)
    def _():
        solver.wi[GO + B - 1] = jnp.zeros((J, K), jnp.float32)

    for t in range(ITERS - 1):
        solver.iterate(t, 2 + t, GO + 2 + t)
        solver.iterate(t, GO + B - 2 - t, N - 2 - t)

    third = lax.broadcasted_iota(jnp.int32, (B, K), 1) % 3
    target = lax.broadcasted_iota(jnp.int32, (K // 3, K), 0)
    source = lax.broadcasted_iota(jnp.int32, (K // 3, K), 1) // 3
    pick = jnp.where(target == source, 1.0, 0.0).astype(jnp.bfloat16)
    pick = jnp.concatenate([pick, pick], 1)
    for i in range(B):
        rows[i, 9 * B :] = jnp.zeros((128 - 9 * B, K), jnp.float32)

    def finish(i):
        a = i + GO
        for c, (v, new) in enumerate(solver.advance(ITERS - 1, a)):
            total = solver.sol[c, i] + v + new
            mine = jnp.where(bottom, total[:B], total[J - B :])
            for q in range(3):
                g = 3 * c + q
                rows[i, B * g : B * g + B] = jnp.where(third == q, mine, 0.0)

    loop(0, B, finish)
    for i in range(B):
        high, low = halves(rows[i])
        out[pl.ds(i, K // 3, stride=B), :] = lax.dot_general(
            pick,
            jnp.concatenate([high, low], 1),
            (((1,), (1,)), ((), ())),
            preferred_element_type=jnp.float32,
        )


def unpack_kernel(got, out):
    for t in range(got.shape[0] // 128):
        turned = got[128 * t : 128 * (t + 1), :].T
        for c in range(3):
            for q in range(3):
                g = 3 * c + q
                out[c, q, :, 128 * t : 128 * (t + 1)] = turned[B * g : B * g + B]


def call(kernel, shapes, inputs, scratch=(), grant=8, extra=(), aliases={}, hbm_in=(), hbm_out=()):
    return pl.pallas_call(
        kernel,
        out_shape=[
            s if hasattr(s, "dtype") else jax.ShapeDtypeStruct(s, jnp.float32) for s in shapes
        ],
        in_specs=[HBM if n in hbm_in else VMEM for n in range(len(inputs))],
        out_specs=[HBM if n in hbm_out else VMEM for n in range(len(shapes))],
        scratch_shapes=[pltpu.VMEM(s, jnp.float32) for s in scratch] + list(extra),
        input_output_aliases=aliases,
        compiler_params=pltpu.CompilerParams(vmem_limit_bytes=int(grant * 1024 * 1024)),
    )(*inputs)


def program(phases, mobility, active, variants):
    count = lax.axis_size("space")

    def pairs(first):
        forward = [(i, i + 1) for i in range(first, count - 1, 2)]
        return forward + [(b, a) for a, b in forward]

    def exchange(to_near, to_far):
        far = lax.ppermute(to_far, "space", pairs(1))
        near = lax.ppermute(to_near, "space", pairs(0))
        return near, far

    def swap(array):
        return lax.ppermute(array, "slab", [(0, 1), (1, 0)])

    ph = jnp.transpose(phases, (1, 2, 0, 3))
    rates = mobility[:, None] * active[0, 0].T.astype(jnp.float32)
    to_near, to_far, to_other, speed = call(
        pack_kernel, [(H * B + 1, F, K)] * 3 + [(F, K)], [ph, rates], grant=4
    )
    across = swap(to_other)
    near, far = exchange(to_near, to_far)
    block = (B + 2 * H, W + 2, F, K)
    coefs = (B, 4 * B, K)
    first, second, evolved, coef, mix = call(
        relax_inner_kernel,
        [block, block, (B, B, F, K), coefs, jax.ShapeDtypeStruct((12 * B, 3 * B * F), jnp.bfloat16)],
        [ph, speed, across, variants.T],
        [(3, 2, F, K), (B - 6, B, F, K)],
        grant=4,
        extra=[pltpu.SemaphoreType.DMA((B - 6,))],
        hbm_out=(2,),
    )
    message = (4 * B * ITERS + 16, K)
    first, second, evolved, coef, to_near, to_far = call(
        relax_outer_kernel,
        [block, block, (B, B, F, K), coefs, message, message],
        [near, far, swap(near[:REST]), swap(far[:REST]), speed, across, mix, first, second, evolved, coef],
        [(3, 2, F, K), (2 * H, B, F, K)],
        grant=4,
        aliases={7: 0, 8: 1, 9: 2, 10: 3},
        extra=[pltpu.SemaphoreType.DMA((2 * H,))],
        hbm_in=(9,),
        hbm_out=(2,),
    )
    o_coef = swap(coef)
    near, far = exchange(to_near, to_far)
    shapes = [(N, J, K), (N, 2 * B, K)] + [(N, J, K)] * 8 + [(3, N, J, K)] * 2 + [(3, B, J, K)]
    state = call(solve_inner_kernel, shapes, [coef, o_coef], grant=4)
    packed = call(
        solve_outer_kernel,
        shapes + [(K // 3 * B, 128)],
        [near, far, swap(near), swap(far), *state],
        [(B, 128, K)],
        grant=8,
        aliases={4 + n: n for n in range(13)},
    )[-1]
    packed = packed.reshape(count, 1, B * 128)
    arrived = lax.all_to_all(packed, "space", 0, 0, tiled=True)
    (displacement,) = call(
        unpack_kernel, [(3, K // count, B, count * B)], [arrived.reshape(count * B, 128)]
    )
    return jnp.transpose(evolved, (2, 0, 1, 3)), displacement


def solution(mesh):
    placed = (P(None, "space", "slab", None), P(), P("space", "slab", None, None), P())
    return jax.shard_map(
        program,
        mesh=mesh,
        in_specs=placed,
        out_specs=(P(None, "space", "slab", None), P(None, "space", "slab", None)),
        check_vma=False,
    )
```

```python
import jax
import jax.numpy as jnp
from jax import lax
from jax.experimental import pallas as pl
from jax.experimental.pallas import tpu as pltpu
from jax.sharding import PartitionSpec as P


ITERS = 4
DIAGONAL_SHIFT = 3.0
SPECTRUM_CENTRE = 12.0
SPECTRUM_RADIUS = 9.0

B = 12
F = 8
K = 384
H = 3
W = B + H
REST = H * H + 1
GO = ITERS + 1
HIGHEST = lax.Precision.HIGHEST
VMEM = pl.BlockSpec(memory_space=pltpu.VMEM)
HBM = pl.BlockSpec(memory_space=pltpu.HBM)


def roll(x, shift, axis):
    return pltpu.roll(x, shift % x.shape[axis], axis)


def parity():
    even = 1 - lax.axis_index("space") % 2
    return even, 1 - even


def pack_kernel(ph, rates, to_near, to_far, to_other, speed_out):
    even, odd = parity()
    slab = lax.axis_index("slab")
    start = (B - H) * (1 - slab)
    for message, top in ((to_far, odd), (to_near, even)):
        for t in range(H):
            source = ph.at[(B - H) * top + t]
            message[H * t : H * (t + 1)] = source[pl.ds(start, H)]
            rest = REST + (B - H) * t
            message[rest : rest + B - H] = source[pl.ds(H * slab, B - H)]
    for i in range(B):
        to_other[H * i : H * (i + 1)] = ph[i, pl.ds(start, H)]
    bricks = K // B
    brick = lax.broadcasted_iota(jnp.int32, (bricks, K), 0)
    spread = jnp.where(brick == lax.broadcasted_iota(jnp.int32, (bricks, K), 1) // B, 1.0, 0.0)
    speed = jnp.dot(
        rates[...], spread, precision=HIGHEST, preferred_element_type=jnp.float32
    )
    to_near[REST - 1] = speed
    to_far[REST - 1] = speed
    to_other[H * B] = speed
    speed_out[...] = speed


def update(x, around, s):
    lane = lax.broadcasted_iota(jnp.int32, (F, K), 1)
    square = x * x
    total = square + roll(square, 4, 0)
    total = total + roll(total, 2, 0)
    total = total + roll(total, 1, 0)
    left = jnp.where(lane == 0, 0.0, roll(x, 1, 1))
    right = jnp.where(lane == K - 1, 0.0, roll(x, -1, 1))
    summed = around + (left + right)
    return x - s * (x * (5.0 + 3.0 * total - 2.0 * square) - summed)


def window_step(src, dst, speed, depth, count, place):
    slab = lax.axis_index("slab")

    def plane(n, _):
        a = place(n)
        group = (a >= H).astype(jnp.int32) + (a >= H + B).astype(jnp.int32)
        edge = depth * slab
        before = src[a, edge]
        x = src[a, edge + 1]
        for w in range(W - depth):
            after = src[a, edge + w + 2]
            whose = slab if w < H - depth else (1 - slab if w >= B else 0)
            around = (before + after) + (src[a - 1, edge + w + 1] + src[a + 1, edge + w + 1])
            dst[a, edge + w + 1] = update(x, around, speed[group, whose])
            before, x = x, after
        return 0

    lax.fori_loop(0, count, plane, 0)


def halves(x):
    high = x.astype(jnp.bfloat16)
    return high, (x - high.astype(jnp.float32)).astype(jnp.bfloat16)


def last_step(src, own_speed, mix, ev, coef, count, place, staged, sems):
    own = 1 + H * lax.axis_index("slab")
    row = lax.broadcasted_iota(jnp.int32, (4 * B, K), 0)
    is_excess = (row >= B) & (row < 2 * B)

    def plane(n, _):
        a = place(n)
        before = src[a, own - 1]
        x = src[a, own]
        for j in range(B):
            after = src[a, own + j + 1]
            around = (before + after) + (src[a - 1, own + j] + src[a + 1, own + j])
            staged[n, j] = update(x, around, own_speed[...])
            before, x = x, after
        pltpu.make_async_copy(staged.at[n], ev.at[a - H], sems.at[n]).start()
        return 0

    lax.fori_loop(0, count, plane, 0)
    for n in range(count):
        values = staged[n].reshape(B * F, K)
        high, low = halves(values * values)
        mixed = jnp.dot(
            mix[...],
            jnp.concatenate([high, low, high], 0),
            preferred_element_type=jnp.float32,
        )
        total = mixed[: 4 * B]
        strain = mixed[4 * B : 8 * B]
        dilation = mixed[8 * B :]
        saturation = total / (1.0 + total)
        excess = 0.5 * saturation
        stress = (1.5 + saturation) * dilation + 2.0 * (1.0 + excess) * strain
        coef[place(n) - H] = jnp.where(is_excess, excess, stress)

    def settle(n, _):
        pltpu.make_async_copy(staged.at[n], ev.at[place(n) - H], sems.at[n]).wait()
        return 0

    lax.fori_loop(0, count, settle, 0)


def relax_inner_kernel(
    ph, mine, across, variants, first, second, ev, coef, mix, e_near, e_far, speed, staged, sems
):
    slab = lax.axis_index("slab")
    own = 1 + H * slab
    other = 1 + B * (1 - slab)
    zero = jnp.zeros((F, K), jnp.float32)
    speed[1, 0] = mine[...]
    speed[1, 1] = across[H * B]

    v = variants[...]
    each = jnp.concatenate([v[:1], jnp.zeros((1, F)), v[1:]], 0)
    whole = jnp.broadcast_to(v[:1] + v[1:2] + v[2:], (4, F))
    table = jnp.concatenate([jnp.ones((4, F)), each, whole], 0)
    shape = (12 * B, B * F)
    group = lax.broadcasted_iota(jnp.int32, (12 * B, 12), 0) // B
    down = jnp.where(group == lax.broadcasted_iota(jnp.int32, (12 * B, 12), 1), 1.0, 0.0)
    field = lax.broadcasted_iota(jnp.int32, (F, B * F), 1) % F
    along = jnp.where(field == lax.broadcasted_iota(jnp.int32, (F, B * F), 0), 1.0, 0.0)
    table = jnp.dot(down, table, precision=HIGHEST, preferred_element_type=jnp.float32)
    table = jnp.dot(table, along, precision=HIGHEST, preferred_element_type=jnp.float32)
    same = lax.broadcasted_iota(jnp.int32, shape, 0) % B
    same = same == lax.broadcasted_iota(jnp.int32, shape, 1) // F
    high, low = halves(jnp.where(same, table, 0.0))
    mix[...] = jnp.concatenate([high, high, low], 1)

    def clear(a, _):
        for buf in (first, second):
            buf[a, 0] = zero
            buf[a, W + 1] = zero
        return 0

    lax.fori_loop(0, B + 2 * H, clear, 0)

    def fill(i, _):
        for j in range(B):
            first[H + i, own + j] = ph[i, j]
        for t in range(H):
            first[H + i, other + t] = across[H * i + t]
        return 0

    lax.fori_loop(0, B, fill, 0)
    window_step(first, second, speed, 1, B - 2, lambda n: H + 1 + n)
    window_step(second, first, speed, 2, B - 4, lambda n: H + 2 + n)
    last_step(first, speed.at[1, 0], mix, ev, coef, B - 6, lambda n: H + 3 + n, staged, sems)
    even, odd = parity()
    for message, top in ((e_near, even), (e_far, odd)):
        message[: 4 * B] = coef[H + (B - 2 * H - 1) * top]
        message[4 * B :] = coef[H + 1 + (B - 2 * H - 3) * top, :16]


def relax_outer_kernel(
    near, far, c_near, c_far, mine, across, mix, first_in, second_in, ev_in, coef_in,
    first, second, ev, coef, m_near, m_far, speed, staged, sems,
):
    even, odd = parity()
    slab = lax.axis_index("slab")
    own = 1 + H * slab
    other = 1 + B * (1 - slab)
    speed[1, 0] = mine[...]
    speed[1, 1] = across[H * B]
    for halo, corner, top in ((near, c_near, even), (far, c_far, odd)):
        speed[2 * top, 0] = halo[REST - 1]
        speed[2 * top, 1] = corner[REST - 1]
        for a in range(H):
            for t in range(H):
                first[(H + B) * top + a, own + (B - H) * (1 - slab) + t] = halo[H * a + t]
                first[(H + B) * top + a, other + t] = corner[H * a + t]
            for m in range(B - H):
                first[(H + B) * top + a, own + H * slab + m] = halo[REST + (B - H) * a + m]

    def ends(depth):
        jump = B + H - 2 * depth - 1
        return lambda n: depth + n + (jump + 1 - H) * (n >= H)

    window_step(first, second, speed, 1, 2 * H, ends(1))
    window_step(second, first, speed, 2, 2 * H, ends(2))
    last_step(first, speed.at[1, 0], mix, ev, coef, 2 * H, ends(3), staged, sems)
    for message, top in ((m_near, even), (m_far, odd)):
        for t in range(H):
            message[4 * B * t : 4 * B * (t + 1)] = coef[(B - H) * top + t]


J = B + ITERS
N = B + 2 * GO


def ratios():
    ratio = SPECTRUM_RADIUS / SPECTRUM_CENTRE
    out = []
    for _ in range(ITERS):
        ratio_next = 1.0 / (2.0 * SPECTRUM_CENTRE / SPECTRUM_RADIUS - ratio)
        out.append((ratio_next * ratio, 2.0 * ratio_next / SPECTRUM_RADIUS))
        ratio = ratio_next
    return out


def joined(mine, others):
    bottom = lax.axis_index("slab") == 0
    lo = jnp.where(bottom, mine, others)
    hi = jnp.where(bottom, others, mine)
    n = mine.shape[0] // B
    return [jnp.concatenate([lo[B * c : B * c + B], hi[B * c : B * c + B]], 0) for c in range(n)]


class Solver:
    def __init__(self, state):
        self.s0, self.s1, self.s2, self.ex = state[:4]
        self.dia, self.wi, self.wjp, self.wjm, self.wkp, self.wkm = state[4:10]
        self.even, self.odd, self.sol = state[10:]
        self.row = lax.broadcasted_iota(jnp.int32, (J, K), 0)
        self.lane = lax.broadcasted_iota(jnp.int32, (J, K), 1)

    def window(self, x):
        return jnp.where(lax.axis_index("slab") == 0, x[:J], x[2 * B - J :])

    def put(self, a, mine, others):
        s0, ex, s1, s2 = joined(mine, others)
        self.s1[a] = s1
        self.s0[a], self.ex[a], self.s2[a] = self.window(s0), self.window(ex), self.window(s2)

    def next_j(self, x):
        return jnp.where(self.row == J - 1, 0.0, roll(x, -1, 0))

    def last_j(self, x):
        return jnp.where(self.row == 0, 0.0, roll(x, 1, 0))

    def next_k(self, x):
        return jnp.where(self.lane == K - 1, 0.0, roll(x, -1, 1))

    def last_k(self, x):
        return jnp.where(self.lane == 0, 0.0, roll(x, 1, 1))

    def force(self, a):
        s1 = self.s1[a]
        row = lax.broadcasted_iota(jnp.int32, (2 * B, K), 0)
        ahead = jnp.where(row == 2 * B - 1, 0.0, roll(s1, -1, 0))
        behind = jnp.where(row == 0, 0.0, roll(s1, 1, 0))
        forcing = (
            0.5 * (self.s0[a + 1] - self.s0[a - 1]),
            0.5 * self.window(ahead - behind),
            0.5 * (self.next_k(self.s2[a]) - self.last_k(self.s2[a])),
        )
        for c in range(3):
            self.even[c, a] = forcing[c] / SPECTRUM_CENTRE

    def weigh(self, a):
        e = self.ex[a]
        i_next = 1.0 + 0.5 * (e + self.ex[a + 1])
        i_last = 1.0 + 0.5 * (e + self.ex[a - 1])
        j_next = 1.0 + 0.5 * (e + self.next_j(e))
        j_last = 1.0 + 0.5 * (e + self.last_j(e))
        k_next = 1.0 + 0.5 * (e + self.next_k(e))
        k_last = 1.0 + 0.5 * (e + self.last_k(e))
        ends = (i_next + i_last) + (j_next + j_last) + (k_next + k_last)
        self.dia[a] = DIAGONAL_SHIFT + ends
        self.wi[a] = i_next
        self.wjp[a] = jnp.where(self.row == J - 1, 0.0, j_next)
        self.wjm[a] = jnp.where(self.row == 0, 0.0, j_last)
        self.wkp[a] = jnp.where(self.lane == K - 1, 0.0, k_next)
        self.wkm[a] = jnp.where(self.lane == 0, 0.0, k_last)

    def buffers(self, t):
        return (self.even, self.odd) if t % 2 == 0 else (self.odd, self.even)

    def advance(self, t, a):
        keep, gain = ratios()[t]
        if t == 0:
            now, past = keep + SPECTRUM_CENTRE * gain, 0.0
        else:
            keep_past, gain_past = ratios()[t - 1]
            now, past = keep + gain / gain_past, gain * keep_past / gain_past
        src, dst = self.buffers(t)
        centre = now - gain * self.dia[a]
        out = []
        for c in range(3):
            v = src[c, a]
            side = self.wi[a] * src[c, a + 1] + self.wi[a - 1] * src[c, a - 1]
            side = side + (self.wjp[a] * roll(v, -1, 0) + self.wjm[a] * roll(v, 1, 0))
            side = side + (self.wkp[a] * roll(v, -1, 1) + self.wkm[a] * roll(v, 1, 1))
            new = centre * v + gain * side
            out.append((v, new - past * dst[c, a] if t else new))
        return out

    def iterate(self, t, start, stop):
        dst = self.buffers(t)[1]

        def plane(a, inner):
            for c, (v, new) in enumerate(self.advance(t, a)):
                dst[c, a] = new
                if inner:
                    self.sol[c, a - GO] = v if t == 0 else self.sol[c, a - GO] + v

        low, high = min(max(start, GO), stop), max(min(stop, GO + B), start)
        loop(start, low, lambda a: plane(a, False))
        loop(low, high, lambda a: plane(a, True))
        loop(high, stop, lambda a: plane(a, False))


def loop(start, stop, body):
    if start < stop:
        lax.fori_loop(start, stop, lambda a, _: (body(a), 0)[1], 0)


def solve_inner_kernel(coef, o_coef, *state):
    solver = Solver(state)
    loop(0, B, lambda i: solver.put(i + GO, coef[i], o_coef[i]))
    loop(GO + 1, GO + B - 1, solver.force)
    loop(GO + 1, GO + B - 1, solver.weigh)
    for t in range(ITERS - 1):
        solver.iterate(t, GO + 2 + t, GO + B - 2 - t)


def solve_outer_kernel(near, far, o_near, o_far, e_near, e_far, oe_near, oe_far, *refs):
    state = refs[13:26]
    out, rows = refs[26:]
    solver = Solver(state)
    even, odd = parity()
    place = lax.axis_index("space")
    bottom = lax.axis_index("slab") == 0
    sides = (
        (near, o_near, e_near, oe_near, even),
        (far, o_far, e_far, oe_far, odd),
    )
    for halo, others, early, others_early, top in sides:
        for t in range(H):
            part = slice(4 * B * t, 4 * B * (t + 1))
            solver.put(2 + t + (GO + B - 2) * top, halo[part], others[part])
        whole, tail = slice(0, 4 * B), slice(4 * B, 4 * B + 16)
        solver.put(1 + (N - 3) * top, early[whole], others_early[whole])
        solver.s0[(N - 1) * top] = solver.window(joined(early[tail], others_early[tail])[0])

    loop(1, GO + 1, solver.force)
    loop(GO + B - 1, N - 1, solver.force)
    solver.wi[1] = 1.0 + 0.5 * (solver.ex[1] + solver.ex[2])
    loop(2, GO + 1, solver.weigh)
    loop(GO + B - 1, N - 2, solver.weigh)

    @pl.when(place == 0)
    def _():
        solver.wi[GO - 1] = jnp.zeros((J, K), jnp.float32)

    @pl.when(place == lax.axis_size("space") - 1)
    def _():
        solver.wi[GO + B - 1] = jnp.zeros((J, K), jnp.float32)

    for t in range(ITERS - 1):
        solver.iterate(t, 2 + t, GO + 2 + t)
        solver.iterate(t, GO + B - 2 - t, N - 2 - t)

    third = lax.broadcasted_iota(jnp.int32, (B, K), 1) % 3
    target = lax.broadcasted_iota(jnp.int32, (K // 3, K), 0)
    source = lax.broadcasted_iota(jnp.int32, (K // 3, K), 1) // 3
    pick = jnp.where(target == source, 1.0, 0.0).astype(jnp.bfloat16)
    pick = jnp.concatenate([pick, pick], 1)
    for i in range(B):
        rows[i, 9 * B :] = jnp.zeros((128 - 9 * B, K), jnp.float32)

    def finish(i):
        a = i + GO
        for c, (v, new) in enumerate(solver.advance(ITERS - 1, a)):
            total = solver.sol[c, i] + v + new
            mine = jnp.where(bottom, total[:B], total[J - B :])
            for q in range(3):
                g = 3 * c + q
                rows[i, B * g : B * g + B] = jnp.where(third == q, mine, 0.0)

    loop(0, B, finish)
    for i in range(B):
        high, low = halves(rows[i])
        out[pl.ds(i, K // 3, stride=B), :] = lax.dot_general(
            pick,
            jnp.concatenate([high, low], 1),
            (((1,), (1,)), ((), ())),
            preferred_element_type=jnp.float32,
        )


def unpack_kernel(got, out):
    for t in range(got.shape[0] // 128):
        turned = got[128 * t : 128 * (t + 1), :].T
        for c in range(3):
            for q in range(3):
                g = 3 * c + q
                out[c, q, :, 128 * t : 128 * (t + 1)] = turned[B * g : B * g + B]


def call(kernel, shapes, inputs, scratch=(), grant=8, extra=(), aliases={}, hbm_in=(), hbm_out=()):
    return pl.pallas_call(
        kernel,
        out_shape=[
            s if hasattr(s, "dtype") else jax.ShapeDtypeStruct(s, jnp.float32) for s in shapes
        ],
        in_specs=[HBM if n in hbm_in else VMEM for n in range(len(inputs))],
        out_specs=[HBM if n in hbm_out else VMEM for n in range(len(shapes))],
        scratch_shapes=[pltpu.VMEM(s, jnp.float32) for s in scratch] + list(extra),
        input_output_aliases=aliases,
        compiler_params=pltpu.CompilerParams(vmem_limit_bytes=int(grant * 1024 * 1024)),
    )(*inputs)


def program(phases, mobility, active, variants):
    count = lax.axis_size("space")

    def pairs(first):
        forward = [(i, i + 1) for i in range(first, count - 1, 2)]
        return forward + [(b, a) for a, b in forward]

    def exchange(to_near, to_far):
        far = lax.ppermute(to_far, "space", pairs(1))
        near = lax.ppermute(to_near, "space", pairs(0))
        return near, far

    def swap(array):
        return lax.ppermute(array, "slab", [(0, 1), (1, 0)])

    ph = jnp.transpose(phases, (1, 2, 0, 3))
    rates = mobility[:, None] * active[0, 0].T.astype(jnp.float32)
    to_near, to_far, to_other, speed = call(
        pack_kernel, [(H * B + 1, F, K)] * 3 + [(F, K)], [ph, rates], grant=4
    )
    across = swap(to_other)
    near, far = exchange(to_near, to_far)
    block = (B + 2 * H, W + 2, F, K)
    coefs = (B, 4 * B, K)
    message = (4 * B + 16, K)
    products = jax.ShapeDtypeStruct((12 * B, 3 * B * F), jnp.bfloat16)
    first, second, evolved, coef, mix, e_near, e_far = call(
        relax_inner_kernel,
        [block, block, (B, B, F, K), coefs, products, message, message],
        [ph, speed, across, variants.T],
        [(3, 2, F, K), (B - 6, B, F, K)],
        grant=4,
        extra=[pltpu.SemaphoreType.DMA((B - 6,))],
        hbm_out=(2,),
    )
    e_near, e_far = exchange(e_near, e_far)
    oe_near, oe_far = swap(e_near), swap(e_far)
    message = (4 * B * H, K)
    first, second, evolved, coef, to_near, to_far = call(
        relax_outer_kernel,
        [block, block, (B, B, F, K), coefs, message, message],
        [near, far, swap(near[:REST]), swap(far[:REST]), speed, across, mix, first, second, evolved, coef],
        [(3, 2, F, K), (2 * H, B, F, K)],
        grant=4,
        aliases={7: 0, 8: 1, 9: 2, 10: 3},
        extra=[pltpu.SemaphoreType.DMA((2 * H,))],
        hbm_in=(9,),
        hbm_out=(2,),
    )
    o_coef = swap(coef)
    near, far = exchange(to_near, to_far)
    shapes = [(N, J, K), (N, 2 * B, K)] + [(N, J, K)] * 8 + [(3, N, J, K)] * 2 + [(3, B, J, K)]
    state = call(solve_inner_kernel, shapes, [coef, o_coef], grant=4)
    packed = call(
        solve_outer_kernel,
        shapes + [(K // 3 * B, 128)],
        [near, far, swap(near), swap(far), e_near, e_far, oe_near, oe_far, *state],
        [(B, 128, K)],
        grant=8,
        aliases={8 + n: n for n in range(13)},
    )[-1]
    packed = packed.reshape(count, 1, B * 128)
    arrived = lax.all_to_all(packed, "space", 0, 0, tiled=True)
    (displacement,) = call(
        unpack_kernel, [(3, K // count, B, count * B)], [arrived.reshape(count * B, 128)]
    )
    return jnp.transpose(evolved, (2, 0, 1, 3)), displacement


def solution(mesh):
    placed = (P(None, "space", "slab", None), P(), P("space", "slab", None, None), P())
    return jax.shard_map(
        program,
        mesh=mesh,
        in_specs=placed,
        out_specs=(P(None, "space", "slab", None), P(None, "space", "slab", None)),
        check_vma=False,
    )
```

```python
import jax
import jax.numpy as jnp
from jax import lax
from jax.experimental import pallas as pl
from jax.experimental.pallas import tpu as pltpu
from jax.sharding import PartitionSpec as P


ITERS = 4
DIAGONAL_SHIFT = 3.0
SPECTRUM_CENTRE = 12.0
SPECTRUM_RADIUS = 9.0

B = 12
F = 8
K = 384
H = 3
W = B + H
REST = H * H + 1
GO = ITERS + 1
HIGHEST = lax.Precision.HIGHEST
VMEM = pl.BlockSpec(memory_space=pltpu.VMEM)
HBM = pl.BlockSpec(memory_space=pltpu.HBM)


def roll(x, shift, axis):
    return pltpu.roll(x, shift % x.shape[axis], axis)


def parity():
    even = 1 - lax.axis_index("space") % 2
    return even, 1 - even


def pack_kernel(ph, rates, to_near, to_far, to_other, speed_out):
    even, odd = parity()
    slab = lax.axis_index("slab")
    start = (B - H) * (1 - slab)
    for message, top in ((to_far, odd), (to_near, even)):
        for t in range(H):
            source = ph.at[(B - H) * top + t]
            message[H * t : H * (t + 1)] = source[pl.ds(start, H)]
            rest = REST + (B - H) * t
            message[rest : rest + B - H] = source[pl.ds(H * slab, B - H)]
    for i in range(B):
        to_other[H * i : H * (i + 1)] = ph[i, pl.ds(start, H)]
    bricks = K // B
    brick = lax.broadcasted_iota(jnp.int32, (bricks, K), 0)
    spread = jnp.where(brick == lax.broadcasted_iota(jnp.int32, (bricks, K), 1) // B, 1.0, 0.0)
    speed = jnp.dot(
        rates[...], spread, precision=HIGHEST, preferred_element_type=jnp.float32
    )
    to_near[REST - 1] = speed
    to_far[REST - 1] = speed
    to_other[H * B] = speed
    speed_out[...] = speed


def update(x, around, s):
    lane = lax.broadcasted_iota(jnp.int32, (F, K), 1)
    square = x * x
    total = square + roll(square, 4, 0)
    total = total + roll(total, 2, 0)
    total = total + roll(total, 1, 0)
    left = jnp.where(lane == 0, 0.0, roll(x, 1, 1))
    right = jnp.where(lane == K - 1, 0.0, roll(x, -1, 1))
    summed = around + (left + right)
    return x - s * (x * (5.0 + 3.0 * total - 2.0 * square) - summed)


def window_step(src, dst, speed, depth, count, place):
    slab = lax.axis_index("slab")

    def plane(n, _):
        a = place(n)
        group = (a >= H).astype(jnp.int32) + (a >= H + B).astype(jnp.int32)
        edge = depth * slab
        before = src[a, edge]
        x = src[a, edge + 1]
        for w in range(W - depth):
            after = src[a, edge + w + 2]
            whose = slab if w < H - depth else (1 - slab if w >= B else 0)
            around = (before + after) + (src[a - 1, edge + w + 1] + src[a + 1, edge + w + 1])
            dst[a, edge + w + 1] = update(x, around, speed[group, whose])
            before, x = x, after
        return 0

    lax.fori_loop(0, count, plane, 0)


def halves(x):
    high = x.astype(jnp.bfloat16)
    return high, (x - high.astype(jnp.float32)).astype(jnp.bfloat16)


def last_step(src, own_speed, mix, ev, coef, count, place, staged, sems):
    own = 1 + H * lax.axis_index("slab")
    row = lax.broadcasted_iota(jnp.int32, (4 * B, K), 0)
    is_excess = (row >= B) & (row < 2 * B)

    def plane(n, _):
        a = place(n)
        before = src[a, own - 1]
        x = src[a, own]
        for j in range(B):
            after = src[a, own + j + 1]
            around = (before + after) + (src[a - 1, own + j] + src[a + 1, own + j])
            staged[n, j] = update(x, around, own_speed[...])
            before, x = x, after
        pltpu.make_async_copy(staged.at[n], ev.at[a - H], sems.at[n]).start()
        return 0

    lax.fori_loop(0, count, plane, 0)
    for n in range(count):
        values = staged[n].reshape(B * F, K)
        high, low = halves(values * values)
        mixed = jnp.dot(
            mix[...],
            jnp.concatenate([high, low, high], 0),
            preferred_element_type=jnp.float32,
        )
        total = mixed[: 4 * B]
        strain = mixed[4 * B : 8 * B]
        dilation = mixed[8 * B :]
        saturation = total / (1.0 + total)
        excess = 0.5 * saturation
        stress = (1.5 + saturation) * dilation + 2.0 * (1.0 + excess) * strain
        coef[place(n) - H] = jnp.where(is_excess, excess, stress)

    def settle(n, _):
        pltpu.make_async_copy(staged.at[n], ev.at[place(n) - H], sems.at[n]).wait()
        return 0

    lax.fori_loop(0, count, settle, 0)


def relax_inner_kernel(
    ph, mine, across, variants, first, second, ev, coef, mix, e_near, e_far, speed, staged, sems
):
    slab = lax.axis_index("slab")
    own = 1 + H * slab
    other = 1 + B * (1 - slab)
    zero = jnp.zeros((F, K), jnp.float32)
    speed[1, 0] = mine[...]
    speed[1, 1] = across[H * B]

    v = variants[...]
    each = jnp.concatenate([v[:1], jnp.zeros((1, F)), v[1:]], 0)
    whole = jnp.broadcast_to(v[:1] + v[1:2] + v[2:], (4, F))
    table = jnp.concatenate([jnp.ones((4, F)), each, whole], 0)
    shape = (12 * B, B * F)
    group = lax.broadcasted_iota(jnp.int32, (12 * B, 12), 0) // B
    down = jnp.where(group == lax.broadcasted_iota(jnp.int32, (12 * B, 12), 1), 1.0, 0.0)
    field = lax.broadcasted_iota(jnp.int32, (F, B * F), 1) % F
    along = jnp.where(field == lax.broadcasted_iota(jnp.int32, (F, B * F), 0), 1.0, 0.0)
    table = jnp.dot(down, table, precision=HIGHEST, preferred_element_type=jnp.float32)
    table = jnp.dot(table, along, precision=HIGHEST, preferred_element_type=jnp.float32)
    same = lax.broadcasted_iota(jnp.int32, shape, 0) % B
    same = same == lax.broadcasted_iota(jnp.int32, shape, 1) // F
    high, low = halves(jnp.where(same, table, 0.0))
    mix[...] = jnp.concatenate([high, high, low], 1)

    def clear(a, _):
        for buf in (first, second):
            buf[a, 0] = zero
            buf[a, W + 1] = zero
        return 0

    lax.fori_loop(0, B + 2 * H, clear, 0)

    def fill(i, _):
        for j in range(B):
            first[H + i, own + j] = ph[i, j]
        for t in range(H):
            first[H + i, other + t] = across[H * i + t]
        return 0

    lax.fori_loop(0, B, fill, 0)
    window_step(first, second, speed, 1, B - 2, lambda n: H + 1 + n)
    window_step(second, first, speed, 2, B - 4, lambda n: H + 2 + n)
    last_step(first, speed.at[1, 0], mix, ev, coef, B - 6, lambda n: H + 3 + n, staged, sems)
    even, odd = parity()
    for message, top in ((e_near, even), (e_far, odd)):
        message[: 4 * B] = coef[H + (B - 2 * H - 1) * top]
        message[4 * B :] = coef[H + 1 + (B - 2 * H - 3) * top, :16]


def relax_outer_kernel(
    near, far, corners, mine, across, mix, first_in, second_in, ev_in, coef_in,
    first, second, ev, coef, m_near, m_far, speed, staged, sems,
):
    even, odd = parity()
    slab = lax.axis_index("slab")
    own = 1 + H * slab
    other = 1 + B * (1 - slab)
    speed[1, 0] = mine[...]
    speed[1, 1] = across[H * B]
    for halo, at, top in ((near, 0, even), (far, REST, odd)):
        speed[2 * top, 0] = halo[REST - 1]
        speed[2 * top, 1] = corners[at + REST - 1]
        for a in range(H):
            for t in range(H):
                first[(H + B) * top + a, own + (B - H) * (1 - slab) + t] = halo[H * a + t]
                first[(H + B) * top + a, other + t] = corners[at + H * a + t]
            for m in range(B - H):
                first[(H + B) * top + a, own + H * slab + m] = halo[REST + (B - H) * a + m]

    def ends(depth):
        jump = B + H - 2 * depth - 1
        return lambda n: depth + n + (jump + 1 - H) * (n >= H)

    window_step(first, second, speed, 1, 2 * H, ends(1))
    window_step(second, first, speed, 2, 2 * H, ends(2))
    last_step(first, speed.at[1, 0], mix, ev, coef, 2 * H, ends(3), staged, sems)
    for message, top in ((m_near, even), (m_far, odd)):
        for t in range(H):
            message[4 * B * t : 4 * B * (t + 1)] = coef[(B - H) * top + t]


J = B + ITERS
N = B + 2 * GO


def ratios():
    ratio = SPECTRUM_RADIUS / SPECTRUM_CENTRE
    out = []
    for _ in range(ITERS):
        ratio_next = 1.0 / (2.0 * SPECTRUM_CENTRE / SPECTRUM_RADIUS - ratio)
        out.append((ratio_next * ratio, 2.0 * ratio_next / SPECTRUM_RADIUS))
        ratio = ratio_next
    return out


def joined(mine, others):
    bottom = lax.axis_index("slab") == 0
    lo = jnp.where(bottom, mine, others)
    hi = jnp.where(bottom, others, mine)
    n = mine.shape[0] // B
    return [jnp.concatenate([lo[B * c : B * c + B], hi[B * c : B * c + B]], 0) for c in range(n)]


class Solver:
    def __init__(self, state):
        self.s0, self.s1, self.s2, self.ex = state[:4]
        self.dia, self.wi, self.wjp, self.wjm, self.wkp, self.wkm = state[4:10]
        self.even, self.odd, self.sol = state[10:]
        self.row = lax.broadcasted_iota(jnp.int32, (J, K), 0)
        self.lane = lax.broadcasted_iota(jnp.int32, (J, K), 1)

    def window(self, x):
        return jnp.where(lax.axis_index("slab") == 0, x[:J], x[2 * B - J :])

    def put(self, a, mine, others):
        s0, ex, s1, s2 = joined(mine, others)
        self.s1[a] = s1
        self.s0[a], self.ex[a], self.s2[a] = self.window(s0), self.window(ex), self.window(s2)

    def next_j(self, x):
        return jnp.where(self.row == J - 1, 0.0, roll(x, -1, 0))

    def last_j(self, x):
        return jnp.where(self.row == 0, 0.0, roll(x, 1, 0))

    def next_k(self, x):
        return jnp.where(self.lane == K - 1, 0.0, roll(x, -1, 1))

    def last_k(self, x):
        return jnp.where(self.lane == 0, 0.0, roll(x, 1, 1))

    def force(self, a):
        s1 = self.s1[a]
        row = lax.broadcasted_iota(jnp.int32, (2 * B, K), 0)
        ahead = jnp.where(row == 2 * B - 1, 0.0, roll(s1, -1, 0))
        behind = jnp.where(row == 0, 0.0, roll(s1, 1, 0))
        forcing = (
            0.5 * (self.s0[a + 1] - self.s0[a - 1]),
            0.5 * self.window(ahead - behind),
            0.5 * (self.next_k(self.s2[a]) - self.last_k(self.s2[a])),
        )
        for c in range(3):
            self.even[c, a] = forcing[c] / SPECTRUM_CENTRE

    def weigh(self, a):
        e = self.ex[a]
        i_next = 1.0 + 0.5 * (e + self.ex[a + 1])
        i_last = 1.0 + 0.5 * (e + self.ex[a - 1])
        j_next = 1.0 + 0.5 * (e + self.next_j(e))
        j_last = 1.0 + 0.5 * (e + self.last_j(e))
        k_next = 1.0 + 0.5 * (e + self.next_k(e))
        k_last = 1.0 + 0.5 * (e + self.last_k(e))
        ends = (i_next + i_last) + (j_next + j_last) + (k_next + k_last)
        self.dia[a] = DIAGONAL_SHIFT + ends
        self.wi[a] = i_next
        self.wjp[a] = jnp.where(self.row == J - 1, 0.0, j_next)
        self.wjm[a] = jnp.where(self.row == 0, 0.0, j_last)
        self.wkp[a] = jnp.where(self.lane == K - 1, 0.0, k_next)
        self.wkm[a] = jnp.where(self.lane == 0, 0.0, k_last)

    def buffers(self, t):
        return (self.even, self.odd) if t % 2 == 0 else (self.odd, self.even)

    def advance(self, t, a):
        keep, gain = ratios()[t]
        if t == 0:
            now, past = keep + SPECTRUM_CENTRE * gain, 0.0
        else:
            keep_past, gain_past = ratios()[t - 1]
            now, past = keep + gain / gain_past, gain * keep_past / gain_past
        src, dst = self.buffers(t)
        centre = now - gain * self.dia[a]
        out = []
        for c in range(3):
            v = src[c, a]
            side = self.wi[a] * src[c, a + 1] + self.wi[a - 1] * src[c, a - 1]
            side = side + (self.wjp[a] * roll(v, -1, 0) + self.wjm[a] * roll(v, 1, 0))
            side = side + (self.wkp[a] * roll(v, -1, 1) + self.wkm[a] * roll(v, 1, 1))
            new = centre * v + gain * side
            out.append((v, new - past * dst[c, a] if t else new))
        return out

    def iterate(self, t, start, stop):
        dst = self.buffers(t)[1]

        def plane(a, inner):
            for c, (v, new) in enumerate(self.advance(t, a)):
                dst[c, a] = new
                if inner:
                    self.sol[c, a - GO] = v if t == 0 else self.sol[c, a - GO] + v

        low, high = min(max(start, GO), stop), max(min(stop, GO + B), start)
        loop(start, low, lambda a: plane(a, False))
        loop(low, high, lambda a: plane(a, True))
        loop(high, stop, lambda a: plane(a, False))


def loop(start, stop, body):
    if start < stop:
        lax.fori_loop(start, stop, lambda a, _: (body(a), 0)[1], 0)


def solve_inner_kernel(coef, o_coef, *state):
    solver = Solver(state)
    loop(0, B, lambda i: solver.put(i + GO, coef[i], o_coef[i]))
    loop(GO + 1, GO + B - 1, solver.force)
    loop(GO + 1, GO + B - 1, solver.weigh)
    for t in range(ITERS - 1):
        solver.iterate(t, GO + 2 + t, GO + B - 2 - t)


def solve_outer_kernel(near, far, o_near, o_far, e_near, e_far, oe_near, oe_far, *refs):
    state = refs[13:26]
    out, rows = refs[26:]
    solver = Solver(state)
    even, odd = parity()
    place = lax.axis_index("space")
    bottom = lax.axis_index("slab") == 0
    sides = (
        (near, o_near, e_near, oe_near, even),
        (far, o_far, e_far, oe_far, odd),
    )
    for halo, others, early, others_early, top in sides:
        for t in range(H):
            part = slice(4 * B * t, 4 * B * (t + 1))
            solver.put(2 + t + (GO + B - 2) * top, halo[part], others[part])
        whole, tail = slice(0, 4 * B), slice(4 * B, 4 * B + 16)
        solver.put(1 + (N - 3) * top, early[whole], others_early[whole])
        solver.s0[(N - 1) * top] = solver.window(joined(early[tail], others_early[tail])[0])

    loop(1, GO + 1, solver.force)
    loop(GO + B - 1, N - 1, solver.force)
    solver.wi[1] = 1.0 + 0.5 * (solver.ex[1] + solver.ex[2])
    loop(2, GO + 1, solver.weigh)
    loop(GO + B - 1, N - 2, solver.weigh)

    @pl.when(place == 0)
    def _():
        solver.wi[GO - 1] = jnp.zeros((J, K), jnp.float32)

    @pl.when(place == lax.axis_size("space") - 1)
    def _():
        solver.wi[GO + B - 1] = jnp.zeros((J, K), jnp.float32)

    for t in range(ITERS - 1):
        solver.iterate(t, 2 + t, GO + 2 + t)
        solver.iterate(t, GO + B - 2 - t, N - 2 - t)

    target = 3 * lax.broadcasted_iota(jnp.int32, (K // 3, K), 0)
    source = lax.broadcasted_iota(jnp.int32, (K // 3, K), 1)
    picks = [jnp.where(source == target + q, 1.0, 0.0).astype(jnp.bfloat16) for q in range(3)]
    picks = [jnp.concatenate([pick, pick], 1) for pick in picks]
    for g in range(B // 3):
        rows[g, 9 * B :] = jnp.zeros((128 - 9 * B, K), jnp.float32)

    def finish(g):
        for p in range(3):
            i = 3 * g + p
            for c, (v, new) in enumerate(solver.advance(ITERS - 1, i + GO)):
                total = solver.sol[c, i] + v + new
                mine = jnp.where(bottom, total[:B], total[J - B :])
                at = B * (3 * p + c)
                rows[g, at : at + B] = mine

    loop(0, B // 3, finish)
    lane = lax.broadcasted_iota(jnp.int32, (K // 3, 128), 1)
    for g in range(B // 3):
        both = jnp.concatenate(halves(rows[g]), 1)
        parts = [
            lax.dot_general(
                pick, both, (((1,), (1,)), ((), ())), preferred_element_type=jnp.float32
            )
            for pick in picks
        ]
        for p in range(3):
            moved = [
                part if q == p else roll(part, 3 * B * (q - p), 1) for q, part in enumerate(parts)
            ]
            value = jnp.where(lane < 6 * B, jnp.where(lane < 3 * B, moved[0], moved[1]), moved[2])
            out[pl.ds(3 * g + p, K // 3, stride=B), :] = value


def unpack_kernel(got, out):
    for t in range(got.shape[0] // 128):
        turned = got[128 * t : 128 * (t + 1), :].T
        for c in range(3):
            for q in range(3):
                g = 3 * q + c
                out[c, q, :, 128 * t : 128 * (t + 1)] = turned[B * g : B * g + B]


def call(kernel, shapes, inputs, scratch=(), grant=8, extra=(), aliases={}, hbm_in=(), hbm_out=()):
    return pl.pallas_call(
        kernel,
        out_shape=[
            s if hasattr(s, "dtype") else jax.ShapeDtypeStruct(s, jnp.float32) for s in shapes
        ],
        in_specs=[HBM if n in hbm_in else VMEM for n in range(len(inputs))],
        out_specs=[HBM if n in hbm_out else VMEM for n in range(len(shapes))],
        scratch_shapes=[pltpu.VMEM(s, jnp.float32) for s in scratch] + list(extra),
        input_output_aliases=aliases,
        compiler_params=pltpu.CompilerParams(vmem_limit_bytes=int(grant * 1024 * 1024)),
    )(*inputs)


def program(phases, mobility, active, variants):
    count = lax.axis_size("space")

    def pairs(first):
        forward = [(i, i + 1) for i in range(first, count - 1, 2)]
        return forward + [(b, a) for a, b in forward]

    def exchange(to_near, to_far):
        far = lax.ppermute(to_far, "space", pairs(1))
        near = lax.ppermute(to_near, "space", pairs(0))
        return near, far

    def swap(array):
        return lax.ppermute(array, "slab", [(0, 1), (1, 0)])

    ph = jnp.transpose(phases, (1, 2, 0, 3))
    rates = mobility[:, None] * active[0, 0].T.astype(jnp.float32)
    to_near, to_far, to_other, speed = call(
        pack_kernel, [(H * B + 1, F, K)] * 3 + [(F, K)], [ph, rates], grant=4
    )
    across = swap(to_other)
    near, far = exchange(to_near, to_far)
    block = (B + 2 * H, W + 2, F, K)
    coefs = (B, 4 * B, K)
    message = (4 * B + 16, K)
    products = jax.ShapeDtypeStruct((12 * B, 3 * B * F), jnp.bfloat16)
    first, second, evolved, coef, mix, e_near, e_far = call(
        relax_inner_kernel,
        [block, block, (B, B, F, K), coefs, products, message, message],
        [ph, speed, across, variants.T],
        [(3, 2, F, K), (B - 6, B, F, K)],
        grant=4,
        extra=[pltpu.SemaphoreType.DMA((B - 6,))],
        hbm_out=(2,),
    )
    e_near, e_far = exchange(e_near, e_far)
    oe_near, oe_far = swap(e_near), swap(e_far)
    message = (4 * B * H, K)
    corners = swap(jnp.concatenate([near[:REST], far[:REST]]))
    first, second, evolved, coef, to_near, to_far = call(
        relax_outer_kernel,
        [block, block, (B, B, F, K), coefs, message, message],
        [near, far, corners, speed, across, mix, first, second, evolved, coef],
        [(3, 2, F, K), (2 * H, B, F, K)],
        grant=4,
        aliases={6: 0, 7: 1, 8: 2, 9: 3},
        extra=[pltpu.SemaphoreType.DMA((2 * H,))],
        hbm_in=(8,),
        hbm_out=(2,),
    )
    o_coef = swap(coef)
    near, far = exchange(to_near, to_far)
    shapes = [(N, J, K), (N, 2 * B, K)] + [(N, J, K)] * 8 + [(3, N, J, K)] * 2 + [(3, B, J, K)]
    state = call(solve_inner_kernel, shapes, [coef, o_coef], grant=4)
    packed = call(
        solve_outer_kernel,
        shapes + [(K // 3 * B, 128)],
        [near, far, swap(near), swap(far), e_near, e_far, oe_near, oe_far, *state],
        [(B // 3, 128, K)],
        grant=8,
        aliases={8 + n: n for n in range(13)},
    )[-1]
    packed = packed.reshape(count, 1, B * 128)
    arrived = lax.all_to_all(packed, "space", 0, 0, tiled=True)
    (displacement,) = call(
        unpack_kernel, [(3, K // count, B, count * B)], [arrived.reshape(count * B, 128)]
    )
    return jnp.transpose(evolved, (2, 0, 1, 3)), displacement


def solution(mesh):
    placed = (P(None, "space", "slab", None), P(), P("space", "slab", None, None), P())
    return jax.shard_map(
        program,
        mesh=mesh,
        in_specs=placed,
        out_specs=(P(None, "space", "slab", None), P(None, "space", "slab", None)),
        check_vma=False,
    )
```

```python
import jax
import jax.numpy as jnp
from jax import lax
from jax.experimental import pallas as pl
from jax.experimental.pallas import tpu as pltpu
from jax.sharding import PartitionSpec as P


ITERS = 4
DIAGONAL_SHIFT = 3.0
SPECTRUM_CENTRE = 12.0
SPECTRUM_RADIUS = 9.0

B = 12
F = 8
K = 384
H = 3
W = B + H
REST = H * H + 1
GO = ITERS + 1
HIGHEST = lax.Precision.HIGHEST
VMEM = pl.BlockSpec(memory_space=pltpu.VMEM)
HBM = pl.BlockSpec(memory_space=pltpu.HBM)


def roll(x, shift, axis):
    return pltpu.roll(x, shift % x.shape[axis], axis)


def parity():
    even = 1 - lax.axis_index("space") % 2
    return even, 1 - even


def pack_kernel(ph, rates, to_near, to_far, to_other, speed_out):
    even, odd = parity()
    slab = lax.axis_index("slab")
    start = (B - H) * (1 - slab)
    for message, top in ((to_far, odd), (to_near, even)):
        for t in range(H):
            source = ph.at[(B - H) * top + t]
            message[H * t : H * (t + 1)] = source[pl.ds(start, H)]
            rest = REST + (B - H) * t
            message[rest : rest + B - H] = source[pl.ds(H * slab, B - H)]
    for i in range(B):
        to_other[H * i : H * (i + 1)] = ph[i, pl.ds(start, H)]
    bricks = K // B
    brick = lax.broadcasted_iota(jnp.int32, (bricks, K), 0)
    spread = jnp.where(brick == lax.broadcasted_iota(jnp.int32, (bricks, K), 1) // B, 1.0, 0.0)
    speed = jnp.dot(
        rates[...], spread, precision=HIGHEST, preferred_element_type=jnp.float32
    )
    to_near[REST - 1] = speed
    to_far[REST - 1] = speed
    to_other[H * B] = speed
    speed_out[...] = speed


def update(x, around, s):
    lane = lax.broadcasted_iota(jnp.int32, (F, K), 1)
    square = x * x
    total = square + roll(square, 4, 0)
    total = total + roll(total, 2, 0)
    total = total + roll(total, 1, 0)
    left = jnp.where(lane == 0, 0.0, roll(x, 1, 1))
    right = jnp.where(lane == K - 1, 0.0, roll(x, -1, 1))
    summed = around + (left + right)
    return x - s * (x * (5.0 + 3.0 * total - 2.0 * square) - summed)


def window_step(src, dst, speed, depth, count, place):
    slab = lax.axis_index("slab")

    def plane(n, _):
        a = place(n)
        group = (a >= H).astype(jnp.int32) + (a >= H + B).astype(jnp.int32)
        edge = depth * slab
        before = src[a, edge]
        x = src[a, edge + 1]
        for w in range(W - depth):
            after = src[a, edge + w + 2]
            whose = slab if w < H - depth else (1 - slab if w >= B else 0)
            around = (before + after) + (src[a - 1, edge + w + 1] + src[a + 1, edge + w + 1])
            dst[a, edge + w + 1] = update(x, around, speed[group, whose])
            before, x = x, after
        return 0

    lax.fori_loop(0, count, plane, 0)


def halves(x):
    high = x.astype(jnp.bfloat16)
    return high, (x - high.astype(jnp.float32)).astype(jnp.bfloat16)


def last_step(src, own_speed, mix, ev, coef, count, place, staged, sems):
    own = 1 + H * lax.axis_index("slab")
    row = lax.broadcasted_iota(jnp.int32, (4 * B, K), 0)
    is_excess = (row >= B) & (row < 2 * B)

    def plane(n, _):
        a = place(n)
        before = src[a, own - 1]
        x = src[a, own]
        for j in range(B):
            after = src[a, own + j + 1]
            around = (before + after) + (src[a - 1, own + j] + src[a + 1, own + j])
            staged[n, j] = update(x, around, own_speed[...])
            before, x = x, after
        pltpu.make_async_copy(staged.at[n], ev.at[a - H], sems.at[n]).start()
        return 0

    lax.fori_loop(0, count, plane, 0)
    for n in range(count):
        values = staged[n].reshape(B * F, K)
        high, low = halves(values * values)
        mixed = jnp.dot(
            mix[...],
            jnp.concatenate([high, low, high], 0),
            preferred_element_type=jnp.float32,
        )
        total = mixed[: 4 * B]
        strain = mixed[4 * B : 8 * B]
        dilation = mixed[8 * B :]
        saturation = total / (1.0 + total)
        excess = 0.5 * saturation
        stress = (1.5 + saturation) * dilation + 2.0 * (1.0 + excess) * strain
        coef[place(n) - H] = jnp.where(is_excess, excess, stress)

    def settle(n, _):
        pltpu.make_async_copy(staged.at[n], ev.at[place(n) - H], sems.at[n]).wait()
        return 0

    lax.fori_loop(0, count, settle, 0)


def relax_inner_kernel(
    ph, mine, across, variants, first, second, ev, coef, mix, e_near, e_far, speed, staged, sems
):
    slab = lax.axis_index("slab")
    own = 1 + H * slab
    other = 1 + B * (1 - slab)
    zero = jnp.zeros((F, K), jnp.float32)
    speed[1, 0] = mine[...]
    speed[1, 1] = across[H * B]

    v = variants[...]
    each = jnp.concatenate([v[:1], jnp.zeros((1, F)), v[1:]], 0)
    whole = jnp.broadcast_to(v[:1] + v[1:2] + v[2:], (4, F))
    table = jnp.concatenate([jnp.ones((4, F)), each, whole], 0)
    shape = (12 * B, B * F)
    group = lax.broadcasted_iota(jnp.int32, (12 * B, 12), 0) // B
    down = jnp.where(group == lax.broadcasted_iota(jnp.int32, (12 * B, 12), 1), 1.0, 0.0)
    field = lax.broadcasted_iota(jnp.int32, (F, B * F), 1) % F
    along = jnp.where(field == lax.broadcasted_iota(jnp.int32, (F, B * F), 0), 1.0, 0.0)
    table = jnp.dot(down, table, precision=HIGHEST, preferred_element_type=jnp.float32)
    table = jnp.dot(table, along, precision=HIGHEST, preferred_element_type=jnp.float32)
    same = lax.broadcasted_iota(jnp.int32, shape, 0) % B
    same = same == lax.broadcasted_iota(jnp.int32, shape, 1) // F
    high, low = halves(jnp.where(same, table, 0.0))
    mix[...] = jnp.concatenate([high, high, low], 1)

    def clear(a, _):
        for buf in (first, second):
            buf[a, 0] = zero
            buf[a, W + 1] = zero
        return 0

    lax.fori_loop(0, B + 2 * H, clear, 0)

    def fill(i, _):
        for j in range(B):
            first[H + i, own + j] = ph[i, j]
        for t in range(H):
            first[H + i, other + t] = across[H * i + t]
        return 0

    lax.fori_loop(0, B, fill, 0)
    window_step(first, second, speed, 1, B - 2, lambda n: H + 1 + n)
    window_step(second, first, speed, 2, B - 4, lambda n: H + 2 + n)
    last_step(first, speed.at[1, 0], mix, ev, coef, B - 6, lambda n: H + 3 + n, staged, sems)
    even, odd = parity()
    for message, top in ((e_near, even), (e_far, odd)):
        message[: 4 * B] = coef[H + (B - 2 * H - 1) * top]
        message[4 * B :] = coef[H + 1 + (B - 2 * H - 3) * top, :16]


def relax_outer_kernel(
    near, far, corners, mine, across, mix, first_in, second_in, ev_in, coef_in,
    first, second, ev, coef, m_near, m_far, speed, staged, sems,
):
    even, odd = parity()
    slab = lax.axis_index("slab")
    own = 1 + H * slab
    other = 1 + B * (1 - slab)
    speed[1, 0] = mine[...]
    speed[1, 1] = across[H * B]
    for halo, at, top in ((near, 0, even), (far, REST, odd)):
        speed[2 * top, 0] = halo[REST - 1]
        speed[2 * top, 1] = corners[at + REST - 1]
        for a in range(H):
            for t in range(H):
                first[(H + B) * top + a, own + (B - H) * (1 - slab) + t] = halo[H * a + t]
                first[(H + B) * top + a, other + t] = corners[at + H * a + t]
            for m in range(B - H):
                first[(H + B) * top + a, own + H * slab + m] = halo[REST + (B - H) * a + m]

    def ends(depth):
        jump = B + H - 2 * depth - 1
        return lambda n: depth + n + (jump + 1 - H) * (n >= H)

    window_step(first, second, speed, 1, 2 * H, ends(1))
    window_step(second, first, speed, 2, 2 * H, ends(2))
    last_step(first, speed.at[1, 0], mix, ev, coef, 2 * H, ends(3), staged, sems)
    for message, top in ((m_near, even), (m_far, odd)):
        for t in range(H):
            message[4 * B * t : 4 * B * (t + 1)] = coef[(B - H) * top + t]


J = B + ITERS
N = B + 2 * GO


def ratios():
    ratio = SPECTRUM_RADIUS / SPECTRUM_CENTRE
    out = []
    for _ in range(ITERS):
        ratio_next = 1.0 / (2.0 * SPECTRUM_CENTRE / SPECTRUM_RADIUS - ratio)
        out.append((ratio_next * ratio, 2.0 * ratio_next / SPECTRUM_RADIUS))
        ratio = ratio_next
    return out


def joined(mine, others):
    bottom = lax.axis_index("slab") == 0
    lo = jnp.where(bottom, mine, others)
    hi = jnp.where(bottom, others, mine)
    n = mine.shape[0] // B
    return [jnp.concatenate([lo[B * c : B * c + B], hi[B * c : B * c + B]], 0) for c in range(n)]


class Solver:
    def __init__(self, state):
        self.s0, self.s1, self.s2, self.ex = state[:4]
        self.dia, self.wi, self.wjp, self.wjm, self.wkp, self.wkm = state[4:10]
        self.even, self.odd, self.sol = state[10:]
        self.row = lax.broadcasted_iota(jnp.int32, (J, K), 0)
        self.lane = lax.broadcasted_iota(jnp.int32, (J, K), 1)

    def window(self, x):
        return jnp.where(lax.axis_index("slab") == 0, x[:J], x[2 * B - J :])

    def put(self, a, mine, others):
        s0, ex, s1, s2 = joined(mine, others)
        self.s1[a] = s1
        self.s0[a], self.ex[a], self.s2[a] = self.window(s0), self.window(ex), self.window(s2)

    def next_j(self, x):
        return jnp.where(self.row == J - 1, 0.0, roll(x, -1, 0))

    def last_j(self, x):
        return jnp.where(self.row == 0, 0.0, roll(x, 1, 0))

    def next_k(self, x):
        return jnp.where(self.lane == K - 1, 0.0, roll(x, -1, 1))

    def last_k(self, x):
        return jnp.where(self.lane == 0, 0.0, roll(x, 1, 1))

    def force(self, a):
        s1 = self.s1[a]
        row = lax.broadcasted_iota(jnp.int32, (2 * B, K), 0)
        ahead = jnp.where(row == 2 * B - 1, 0.0, roll(s1, -1, 0))
        behind = jnp.where(row == 0, 0.0, roll(s1, 1, 0))
        forcing = (
            0.5 * (self.s0[a + 1] - self.s0[a - 1]),
            0.5 * self.window(ahead - behind),
            0.5 * (self.next_k(self.s2[a]) - self.last_k(self.s2[a])),
        )
        for c in range(3):
            self.even[c, a] = forcing[c] / SPECTRUM_CENTRE

    def weigh(self, a):
        e = self.ex[a]
        i_next = 1.0 + 0.5 * (e + self.ex[a + 1])
        i_last = 1.0 + 0.5 * (e + self.ex[a - 1])
        j_next = 1.0 + 0.5 * (e + self.next_j(e))
        j_last = 1.0 + 0.5 * (e + self.last_j(e))
        k_next = 1.0 + 0.5 * (e + self.next_k(e))
        k_last = 1.0 + 0.5 * (e + self.last_k(e))
        ends = (i_next + i_last) + (j_next + j_last) + (k_next + k_last)
        self.dia[a] = DIAGONAL_SHIFT + ends
        self.wi[a] = i_next
        self.wjp[a] = jnp.where(self.row == J - 1, 0.0, j_next)
        self.wjm[a] = jnp.where(self.row == 0, 0.0, j_last)
        self.wkp[a] = jnp.where(self.lane == K - 1, 0.0, k_next)
        self.wkm[a] = jnp.where(self.lane == 0, 0.0, k_last)

    def buffers(self, t):
        return (self.even, self.odd) if t % 2 == 0 else (self.odd, self.even)

    def advance(self, t, a):
        keep, gain = ratios()[t]
        if t == 0:
            now, past = keep + SPECTRUM_CENTRE * gain, 0.0
        else:
            keep_past, gain_past = ratios()[t - 1]
            now, past = keep + gain / gain_past, gain * keep_past / gain_past
        src, dst = self.buffers(t)
        centre = now - gain * self.dia[a]
        out = []
        for c in range(3):
            v = src[c, a]
            side = self.wi[a] * src[c, a + 1] + self.wi[a - 1] * src[c, a - 1]
            side = side + (self.wjp[a] * roll(v, -1, 0) + self.wjm[a] * roll(v, 1, 0))
            side = side + (self.wkp[a] * roll(v, -1, 1) + self.wkm[a] * roll(v, 1, 1))
            new = centre * v + gain * side
            out.append((v, new - past * dst[c, a] if t else new))
        return out

    def iterate(self, t, start, stop, static=False):
        dst = self.buffers(t)[1]

        def plane(a, inner):
            for c, (v, new) in enumerate(self.advance(t, a)):
                dst[c, a] = new
                if inner:
                    self.sol[c, a - GO] = v if t == 0 else self.sol[c, a - GO] + v

        low, high = min(max(start, GO), stop), max(min(stop, GO + B), start)
        loop(start, low, lambda a: plane(a, False), static)
        loop(low, high, lambda a: plane(a, True), static)
        loop(high, stop, lambda a: plane(a, False), static)


def loop(start, stop, body, static=False):
    if static:
        for a in range(start, stop):
            body(a)
    elif start < stop:
        lax.fori_loop(start, stop, lambda a, _: (body(a), 0)[1], 0)


def solve_inner_kernel(coef, o_coef, *state):
    solver = Solver(state)
    loop(0, B, lambda i: solver.put(i + GO, coef[i], o_coef[i]))
    loop(GO + 1, GO + B - 1, solver.force)
    loop(GO + 1, GO + B - 1, solver.weigh)
    for t in range(ITERS - 1):
        solver.iterate(t, GO + 2 + t, GO + B - 2 - t)


def solve_outer_kernel(near, far, o_near, o_far, e_near, e_far, oe_near, oe_far, *refs):
    state = refs[13:26]
    out, rows = refs[26:]
    solver = Solver(state)
    even, odd = parity()
    place = lax.axis_index("space")
    bottom = lax.axis_index("slab") == 0
    sides = (
        (near, o_near, e_near, oe_near, even),
        (far, o_far, e_far, oe_far, odd),
    )
    for halo, others, early, others_early, top in sides:
        for t in range(H):
            part = slice(4 * B * t, 4 * B * (t + 1))
            solver.put(2 + t + (GO + B - 2) * top, halo[part], others[part])
        whole, tail = slice(0, 4 * B), slice(4 * B, 4 * B + 16)
        solver.put(1 + (N - 3) * top, early[whole], others_early[whole])
        solver.s0[(N - 1) * top] = solver.window(joined(early[tail], others_early[tail])[0])

    loop(1, GO + 1, solver.force, True)
    loop(GO + B - 1, N - 1, solver.force, True)
    solver.wi[1] = 1.0 + 0.5 * (solver.ex[1] + solver.ex[2])
    loop(2, GO + 1, solver.weigh, True)
    loop(GO + B - 1, N - 2, solver.weigh, True)

    @pl.when(place == 0)
    def _():
        solver.wi[GO - 1] = jnp.zeros((J, K), jnp.float32)

    @pl.when(place == lax.axis_size("space") - 1)
    def _():
        solver.wi[GO + B - 1] = jnp.zeros((J, K), jnp.float32)

    for t in range(ITERS - 1):
        solver.iterate(t, 2 + t, GO + 2 + t, True)
        solver.iterate(t, GO + B - 2 - t, N - 2 - t, True)

    target = 3 * lax.broadcasted_iota(jnp.int32, (K // 3, K), 0)
    source = lax.broadcasted_iota(jnp.int32, (K // 3, K), 1)
    picks = [jnp.where(source == target + q, 1.0, 0.0).astype(jnp.bfloat16) for q in range(3)]
    picks = [jnp.concatenate([pick, pick], 1) for pick in picks]
    for g in range(B // 3):
        rows[g, 9 * B :] = jnp.zeros((128 - 9 * B, K), jnp.float32)

    def finish(g):
        for p in range(3):
            i = 3 * g + p
            for c, (v, new) in enumerate(solver.advance(ITERS - 1, i + GO)):
                total = solver.sol[c, i] + v + new
                mine = jnp.where(bottom, total[:B], total[J - B :])
                at = B * (3 * p + c)
                rows[g, at : at + B] = mine

    loop(0, B // 3, finish, True)
    lane = lax.broadcasted_iota(jnp.int32, (K // 3, 128), 1)
    for g in range(B // 3):
        both = jnp.concatenate(halves(rows[g]), 1)
        parts = [
            lax.dot_general(
                pick, both, (((1,), (1,)), ((), ())), preferred_element_type=jnp.float32
            )
            for pick in picks
        ]
        for p in range(3):
            moved = [
                part if q == p else roll(part, 3 * B * (q - p), 1) for q, part in enumerate(parts)
            ]
            value = jnp.where(lane < 6 * B, jnp.where(lane < 3 * B, moved[0], moved[1]), moved[2])
            out[pl.ds(3 * g + p, K // 3, stride=B), :] = value


def unpack_kernel(got, out):
    for t in range(got.shape[0] // 128):
        turned = got[128 * t : 128 * (t + 1), :].T
        for c in range(3):
            for q in range(3):
                g = 3 * q + c
                out[c, q, :, 128 * t : 128 * (t + 1)] = turned[B * g : B * g + B]


def call(kernel, shapes, inputs, scratch=(), grant=8, extra=(), aliases={}, hbm_in=(), hbm_out=()):
    return pl.pallas_call(
        kernel,
        out_shape=[
            s if hasattr(s, "dtype") else jax.ShapeDtypeStruct(s, jnp.float32) for s in shapes
        ],
        in_specs=[HBM if n in hbm_in else VMEM for n in range(len(inputs))],
        out_specs=[HBM if n in hbm_out else VMEM for n in range(len(shapes))],
        scratch_shapes=[pltpu.VMEM(s, jnp.float32) for s in scratch] + list(extra),
        input_output_aliases=aliases,
        compiler_params=pltpu.CompilerParams(vmem_limit_bytes=int(grant * 1024 * 1024)),
    )(*inputs)


def program(phases, mobility, active, variants):
    count = lax.axis_size("space")

    def pairs(first):
        forward = [(i, i + 1) for i in range(first, count - 1, 2)]
        return forward + [(b, a) for a, b in forward]

    def exchange(to_near, to_far):
        far = lax.ppermute(to_far, "space", pairs(1))
        near = lax.ppermute(to_near, "space", pairs(0))
        return near, far

    def swap(array):
        return lax.ppermute(array, "slab", [(0, 1), (1, 0)])

    ph = jnp.transpose(phases, (1, 2, 0, 3))
    rates = mobility[:, None] * active[0, 0].T.astype(jnp.float32)
    to_near, to_far, to_other, speed = call(
        pack_kernel, [(H * B + 1, F, K)] * 3 + [(F, K)], [ph, rates], grant=4
    )
    across = swap(to_other)
    near, far = exchange(to_near, to_far)
    block = (B + 2 * H, W + 2, F, K)
    coefs = (B, 4 * B, K)
    message = (4 * B + 16, K)
    products = jax.ShapeDtypeStruct((12 * B, 3 * B * F), jnp.bfloat16)
    first, second, evolved, coef, mix, e_near, e_far = call(
        relax_inner_kernel,
        [block, block, (B, B, F, K), coefs, products, message, message],
        [ph, speed, across, variants.T],
        [(3, 2, F, K), (B - 6, B, F, K)],
        grant=4,
        extra=[pltpu.SemaphoreType.DMA((B - 6,))],
        hbm_out=(2,),
    )
    e_near, e_far = exchange(e_near, e_far)
    oe_near, oe_far = swap(e_near), swap(e_far)
    message = (4 * B * H, K)
    corners = swap(jnp.concatenate([near[:REST], far[:REST]]))
    first, second, evolved, coef, to_near, to_far = call(
        relax_outer_kernel,
        [block, block, (B, B, F, K), coefs, message, message],
        [near, far, corners, speed, across, mix, first, second, evolved, coef],
        [(3, 2, F, K), (2 * H, B, F, K)],
        grant=4,
        aliases={6: 0, 7: 1, 8: 2, 9: 3},
        extra=[pltpu.SemaphoreType.DMA((2 * H,))],
        hbm_in=(8,),
        hbm_out=(2,),
    )
    o_coef = swap(coef)
    near, far = exchange(to_near, to_far)
    shapes = [(N, J, K), (N, 2 * B, K)] + [(N, J, K)] * 8 + [(3, N, J, K)] * 2 + [(3, B, J, K)]
    state = call(solve_inner_kernel, shapes, [coef, o_coef], grant=4)
    packed = call(
        solve_outer_kernel,
        shapes + [(K // 3 * B, 128)],
        [near, far, swap(near), swap(far), e_near, e_far, oe_near, oe_far, *state],
        [(B // 3, 128, K)],
        grant=8,
        aliases={8 + n: n for n in range(13)},
    )[-1]
    packed = packed.reshape(count, 1, B * 128)
    arrived = lax.all_to_all(packed, "space", 0, 0, tiled=True)
    (displacement,) = call(
        unpack_kernel, [(3, K // count, B, count * B)], [arrived.reshape(count * B, 128)]
    )
    return jnp.transpose(evolved, (2, 0, 1, 3)), displacement


def solution(mesh):
    placed = (P(None, "space", "slab", None), P(), P("space", "slab", None, None), P())
    return jax.shard_map(
        program,
        mesh=mesh,
        in_specs=placed,
        out_specs=(P(None, "space", "slab", None), P(None, "space", "slab", None)),
        check_vma=False,
    )
```

```python
import jax
import jax.numpy as jnp
from jax import lax
from jax.experimental import pallas as pl
from jax.experimental.pallas import tpu as pltpu
from jax.sharding import PartitionSpec as P


ITERS = 4
DIAGONAL_SHIFT = 3.0
SPECTRUM_CENTRE = 12.0
SPECTRUM_RADIUS = 9.0

B = 12
F = 8
K = 384
H = 3
W = B + H
REST = H * H + 1
GO = ITERS + 1
HIGHEST = lax.Precision.HIGHEST
VMEM = pl.BlockSpec(memory_space=pltpu.VMEM)
HBM = pl.BlockSpec(memory_space=pltpu.HBM)


def roll(x, shift, axis):
    return pltpu.roll(x, shift % x.shape[axis], axis)


def parity():
    even = 1 - lax.axis_index("space") % 2
    return even, 1 - even


def pack_kernel(ph, rates, to_near, to_far, to_other, speed_out):
    even, odd = parity()
    slab = lax.axis_index("slab")
    start = (B - H) * (1 - slab)
    for message, top in ((to_far, odd), (to_near, even)):
        for t in range(H):
            source = ph.at[(B - H) * top + t]
            message[H * t : H * (t + 1)] = source[pl.ds(start, H)]
            rest = REST + (B - H) * t
            message[rest : rest + B - H] = source[pl.ds(H * slab, B - H)]
    for i in range(B):
        to_other[H * i : H * (i + 1)] = ph[i, pl.ds(start, H)]
    bricks = K // B
    brick = lax.broadcasted_iota(jnp.int32, (bricks, K), 0)
    spread = jnp.where(brick == lax.broadcasted_iota(jnp.int32, (bricks, K), 1) // B, 1.0, 0.0)
    speed = jnp.dot(
        rates[...], spread, precision=HIGHEST, preferred_element_type=jnp.float32
    )
    to_near[REST - 1] = speed
    to_far[REST - 1] = speed
    to_other[H * B] = speed
    speed_out[...] = speed


def update(x, around, s):
    lane = lax.broadcasted_iota(jnp.int32, (F, K), 1)
    square = x * x
    total = square + roll(square, 4, 0)
    total = total + roll(total, 2, 0)
    total = total + roll(total, 1, 0)
    left = jnp.where(lane == 0, 0.0, roll(x, 1, 1))
    right = jnp.where(lane == K - 1, 0.0, roll(x, -1, 1))
    summed = around + (left + right)
    return x - s * (x * (5.0 + 3.0 * total - 2.0 * square) - summed)


def window_step(src, dst, speed, depth, count, place, static=False):
    slab = lax.axis_index("slab")

    def plane(n):
        a = place(n)
        group = (a >= H) * 1 + (a >= H + B) * 1
        edge = depth * slab
        before = src[a, edge]
        x = src[a, edge + 1]
        for w in range(W - depth):
            after = src[a, edge + w + 2]
            whose = slab if w < H - depth else (1 - slab if w >= B else 0)
            around = (before + after) + (src[a - 1, edge + w + 1] + src[a + 1, edge + w + 1])
            dst[a, edge + w + 1] = update(x, around, speed[group, whose])
            before, x = x, after

    loop(0, count, plane, static)


def halves(x):
    high = x.astype(jnp.bfloat16)
    return high, (x - high.astype(jnp.float32)).astype(jnp.bfloat16)


def last_step(src, own_speed, mix, ev, coef, count, place, staged, sems, static=False):
    own = 1 + H * lax.axis_index("slab")
    row = lax.broadcasted_iota(jnp.int32, (4 * B, K), 0)
    is_excess = (row >= B) & (row < 2 * B)

    def plane(n):
        a = place(n)
        before = src[a, own - 1]
        x = src[a, own]
        for j in range(B):
            after = src[a, own + j + 1]
            around = (before + after) + (src[a - 1, own + j] + src[a + 1, own + j])
            staged[n, j] = update(x, around, own_speed[...])
            before, x = x, after
        pltpu.make_async_copy(staged.at[n], ev.at[a - H], sems.at[n]).start()

    loop(0, count, plane, static)
    for n in range(count):
        values = staged[n].reshape(B * F, K)
        high, low = halves(values * values)
        mixed = jnp.dot(
            mix[...],
            jnp.concatenate([high, low, high], 0),
            preferred_element_type=jnp.float32,
        )
        total = mixed[: 4 * B]
        strain = mixed[4 * B : 8 * B]
        dilation = mixed[8 * B :]
        saturation = total / (1.0 + total)
        excess = 0.5 * saturation
        stress = (1.5 + saturation) * dilation + 2.0 * (1.0 + excess) * strain
        coef[place(n) - H] = jnp.where(is_excess, excess, stress)

    def settle(n, _):
        pltpu.make_async_copy(staged.at[n], ev.at[place(n) - H], sems.at[n]).wait()
        return 0

    lax.fori_loop(0, count, settle, 0)


def relax_inner_kernel(
    ph, mine, across, variants, first, second, ev, coef, mix, e_near, e_far, speed, staged, sems
):
    slab = lax.axis_index("slab")
    own = 1 + H * slab
    other = 1 + B * (1 - slab)
    zero = jnp.zeros((F, K), jnp.float32)
    speed[1, 0] = mine[...]
    speed[1, 1] = across[H * B]

    v = variants[...]
    each = jnp.concatenate([v[:1], jnp.zeros((1, F)), v[1:]], 0)
    whole = jnp.broadcast_to(v[:1] + v[1:2] + v[2:], (4, F))
    table = jnp.concatenate([jnp.ones((4, F)), each, whole], 0)
    shape = (12 * B, B * F)
    group = lax.broadcasted_iota(jnp.int32, (12 * B, 12), 0) // B
    down = jnp.where(group == lax.broadcasted_iota(jnp.int32, (12 * B, 12), 1), 1.0, 0.0)
    field = lax.broadcasted_iota(jnp.int32, (F, B * F), 1) % F
    along = jnp.where(field == lax.broadcasted_iota(jnp.int32, (F, B * F), 0), 1.0, 0.0)
    table = jnp.dot(down, table, precision=HIGHEST, preferred_element_type=jnp.float32)
    table = jnp.dot(table, along, precision=HIGHEST, preferred_element_type=jnp.float32)
    same = lax.broadcasted_iota(jnp.int32, shape, 0) % B
    same = same == lax.broadcasted_iota(jnp.int32, shape, 1) // F
    high, low = halves(jnp.where(same, table, 0.0))
    mix[...] = jnp.concatenate([high, high, low], 1)

    def clear(a, _):
        for buf in (first, second):
            buf[a, 0] = zero
            buf[a, W + 1] = zero
        return 0

    lax.fori_loop(0, B + 2 * H, clear, 0)

    def fill(i, _):
        for j in range(B):
            first[H + i, own + j] = ph[i, j]
        for t in range(H):
            first[H + i, other + t] = across[H * i + t]
        return 0

    lax.fori_loop(0, B, fill, 0)
    window_step(first, second, speed, 1, B - 2, lambda n: H + 1 + n)
    window_step(second, first, speed, 2, B - 4, lambda n: H + 2 + n)
    last_step(first, speed.at[1, 0], mix, ev, coef, B - 6, lambda n: H + 3 + n, staged, sems)
    even, odd = parity()
    for message, top in ((e_near, even), (e_far, odd)):
        message[: 4 * B] = coef[H + (B - 2 * H - 1) * top]
        message[4 * B :] = coef[H + 1 + (B - 2 * H - 3) * top, :16]


def relax_outer_kernel(
    near, far, corners, mine, across, mix, first_in, second_in, ev_in, coef_in,
    first, second, ev, coef, m_near, m_far, speed, staged, sems,
):
    even, odd = parity()
    slab = lax.axis_index("slab")
    own = 1 + H * slab
    other = 1 + B * (1 - slab)
    speed[1, 0] = mine[...]
    speed[1, 1] = across[H * B]
    for halo, at, top in ((near, 0, even), (far, REST, odd)):
        speed[2 * top, 0] = halo[REST - 1]
        speed[2 * top, 1] = corners[at + REST - 1]
        for a in range(H):
            for t in range(H):
                first[(H + B) * top + a, own + (B - H) * (1 - slab) + t] = halo[H * a + t]
                first[(H + B) * top + a, other + t] = corners[at + H * a + t]
            for m in range(B - H):
                first[(H + B) * top + a, own + H * slab + m] = halo[REST + (B - H) * a + m]

    def ends(depth):
        jump = B + H - 2 * depth - 1
        return lambda n: depth + n + (jump + 1 - H) * (n >= H)

    window_step(first, second, speed, 1, 2 * H, ends(1), True)
    window_step(second, first, speed, 2, 2 * H, ends(2), True)
    last_step(first, speed.at[1, 0], mix, ev, coef, 2 * H, ends(3), staged, sems, True)
    for message, top in ((m_near, even), (m_far, odd)):
        for t in range(H):
            message[4 * B * t : 4 * B * (t + 1)] = coef[(B - H) * top + t]


J = B + ITERS
N = B + 2 * GO


def ratios():
    ratio = SPECTRUM_RADIUS / SPECTRUM_CENTRE
    out = []
    for _ in range(ITERS):
        ratio_next = 1.0 / (2.0 * SPECTRUM_CENTRE / SPECTRUM_RADIUS - ratio)
        out.append((ratio_next * ratio, 2.0 * ratio_next / SPECTRUM_RADIUS))
        ratio = ratio_next
    return out


def joined(mine, others):
    bottom = lax.axis_index("slab") == 0
    lo = jnp.where(bottom, mine, others)
    hi = jnp.where(bottom, others, mine)
    n = mine.shape[0] // B
    return [jnp.concatenate([lo[B * c : B * c + B], hi[B * c : B * c + B]], 0) for c in range(n)]


class Solver:
    def __init__(self, state):
        self.s0, self.s1, self.s2, self.ex = state[:4]
        self.dia, self.wi, self.wjp, self.wjm, self.wkp, self.wkm = state[4:10]
        self.even, self.odd, self.sol = state[10:]
        self.row = lax.broadcasted_iota(jnp.int32, (J, K), 0)
        self.lane = lax.broadcasted_iota(jnp.int32, (J, K), 1)

    def window(self, x):
        return jnp.where(lax.axis_index("slab") == 0, x[:J], x[2 * B - J :])

    def put(self, a, mine, others):
        s0, ex, s1, s2 = joined(mine, others)
        self.s1[a] = s1
        self.s0[a], self.ex[a], self.s2[a] = self.window(s0), self.window(ex), self.window(s2)

    def next_j(self, x):
        return jnp.where(self.row == J - 1, 0.0, roll(x, -1, 0))

    def last_j(self, x):
        return jnp.where(self.row == 0, 0.0, roll(x, 1, 0))

    def next_k(self, x):
        return jnp.where(self.lane == K - 1, 0.0, roll(x, -1, 1))

    def last_k(self, x):
        return jnp.where(self.lane == 0, 0.0, roll(x, 1, 1))

    def force(self, a):
        s1 = self.s1[a]
        row = lax.broadcasted_iota(jnp.int32, (2 * B, K), 0)
        ahead = jnp.where(row == 2 * B - 1, 0.0, roll(s1, -1, 0))
        behind = jnp.where(row == 0, 0.0, roll(s1, 1, 0))
        forcing = (
            0.5 * (self.s0[a + 1] - self.s0[a - 1]),
            0.5 * self.window(ahead - behind),
            0.5 * (self.next_k(self.s2[a]) - self.last_k(self.s2[a])),
        )
        for c in range(3):
            self.even[c, a] = forcing[c] / SPECTRUM_CENTRE

    def weigh(self, a):
        e = self.ex[a]
        i_next = 1.0 + 0.5 * (e + self.ex[a + 1])
        i_last = 1.0 + 0.5 * (e + self.ex[a - 1])
        j_next = 1.0 + 0.5 * (e + self.next_j(e))
        j_last = 1.0 + 0.5 * (e + self.last_j(e))
        k_next = 1.0 + 0.5 * (e + self.next_k(e))
        k_last = 1.0 + 0.5 * (e + self.last_k(e))
        ends = (i_next + i_last) + (j_next + j_last) + (k_next + k_last)
        self.dia[a] = DIAGONAL_SHIFT + ends
        self.wi[a] = i_next
        self.wjp[a] = jnp.where(self.row == J - 1, 0.0, j_next)
        self.wjm[a] = jnp.where(self.row == 0, 0.0, j_last)
        self.wkp[a] = jnp.where(self.lane == K - 1, 0.0, k_next)
        self.wkm[a] = jnp.where(self.lane == 0, 0.0, k_last)

    def buffers(self, t):
        return (self.even, self.odd) if t % 2 == 0 else (self.odd, self.even)

    def advance(self, t, a):
        keep, gain = ratios()[t]
        if t == 0:
            now, past = keep + SPECTRUM_CENTRE * gain, 0.0
        else:
            keep_past, gain_past = ratios()[t - 1]
            now, past = keep + gain / gain_past, gain * keep_past / gain_past
        src, dst = self.buffers(t)
        centre = now - gain * self.dia[a]
        out = []
        for c in range(3):
            v = src[c, a]
            side = self.wi[a] * src[c, a + 1] + self.wi[a - 1] * src[c, a - 1]
            side = side + (self.wjp[a] * roll(v, -1, 0) + self.wjm[a] * roll(v, 1, 0))
            side = side + (self.wkp[a] * roll(v, -1, 1) + self.wkm[a] * roll(v, 1, 1))
            new = centre * v + gain * side
            out.append((v, new - past * dst[c, a] if t else new))
        return out

    def iterate(self, t, start, stop, static=False):
        dst = self.buffers(t)[1]

        def plane(a, inner):
            for c, (v, new) in enumerate(self.advance(t, a)):
                dst[c, a] = new
                if inner:
                    self.sol[c, a - GO] = v if t == 0 else self.sol[c, a - GO] + v

        low, high = min(max(start, GO), stop), max(min(stop, GO + B), start)
        loop(start, low, lambda a: plane(a, False), static)
        loop(low, high, lambda a: plane(a, True), static)
        loop(high, stop, lambda a: plane(a, False), static)


def loop(start, stop, body, static=False):
    if static:
        for a in range(start, stop):
            body(a)
    elif start < stop:
        lax.fori_loop(start, stop, lambda a, _: (body(a), 0)[1], 0)


def solve_inner_kernel(coef, o_coef, *state):
    solver = Solver(state)
    loop(0, B, lambda i: solver.put(i + GO, coef[i], o_coef[i]))
    loop(GO + 1, GO + B - 1, solver.force)
    loop(GO + 1, GO + B - 1, solver.weigh)
    for t in range(ITERS - 1):
        solver.iterate(t, GO + 2 + t, GO + B - 2 - t)


def solve_outer_kernel(near, far, o_near, o_far, e_near, e_far, oe_near, oe_far, *refs):
    state = refs[13:26]
    out, rows = refs[26:]
    solver = Solver(state)
    even, odd = parity()
    place = lax.axis_index("space")
    bottom = lax.axis_index("slab") == 0
    sides = (
        (near, o_near, e_near, oe_near, even),
        (far, o_far, e_far, oe_far, odd),
    )
    for halo, others, early, others_early, top in sides:
        for t in range(H):
            part = slice(4 * B * t, 4 * B * (t + 1))
            solver.put(2 + t + (GO + B - 2) * top, halo[part], others[part])
        whole, tail = slice(0, 4 * B), slice(4 * B, 4 * B + 16)
        solver.put(1 + (N - 3) * top, early[whole], others_early[whole])
        solver.s0[(N - 1) * top] = solver.window(joined(early[tail], others_early[tail])[0])

    loop(1, GO + 1, solver.force, True)
    loop(GO + B - 1, N - 1, solver.force, True)
    solver.wi[1] = 1.0 + 0.5 * (solver.ex[1] + solver.ex[2])
    loop(2, GO + 1, solver.weigh, True)
    loop(GO + B - 1, N - 2, solver.weigh, True)

    @pl.when(place == 0)
    def _():
        solver.wi[GO - 1] = jnp.zeros((J, K), jnp.float32)

    @pl.when(place == lax.axis_size("space") - 1)
    def _():
        solver.wi[GO + B - 1] = jnp.zeros((J, K), jnp.float32)

    for t in range(ITERS - 1):
        solver.iterate(t, 2 + t, GO + 2 + t, True)
        solver.iterate(t, GO + B - 2 - t, N - 2 - t, True)

    target = 3 * lax.broadcasted_iota(jnp.int32, (K // 3, K), 0)
    source = lax.broadcasted_iota(jnp.int32, (K // 3, K), 1)
    picks = [jnp.where(source == target + q, 1.0, 0.0).astype(jnp.bfloat16) for q in range(3)]
    picks = [jnp.concatenate([pick, pick], 1) for pick in picks]
    for g in range(B // 3):
        rows[g, 9 * B :] = jnp.zeros((128 - 9 * B, K), jnp.float32)

    def finish(g):
        for p in range(3):
            i = 3 * g + p
            for c, (v, new) in enumerate(solver.advance(ITERS - 1, i + GO)):
                total = solver.sol[c, i] + v + new
                mine = jnp.where(bottom, total[:B], total[J - B :])
                at = B * (3 * p + c)
                rows[g, at : at + B] = mine

    loop(0, B // 3, finish, True)
    lane = lax.broadcasted_iota(jnp.int32, (K // 3, 128), 1)
    for g in range(B // 3):
        both = jnp.concatenate(halves(rows[g]), 1)
        parts = [
            lax.dot_general(
                pick, both, (((1,), (1,)), ((), ())), preferred_element_type=jnp.float32
            )
            for pick in picks
        ]
        for p in range(3):
            moved = [
                part if q == p else roll(part, 3 * B * (q - p), 1) for q, part in enumerate(parts)
            ]
            value = jnp.where(lane < 6 * B, jnp.where(lane < 3 * B, moved[0], moved[1]), moved[2])
            out[pl.ds(3 * g + p, K // 3, stride=B), :] = value


def unpack_kernel(got, out):
    for t in range(got.shape[0] // 128):
        turned = got[128 * t : 128 * (t + 1), :].T
        for c in range(3):
            for q in range(3):
                g = 3 * q + c
                out[c, q, :, 128 * t : 128 * (t + 1)] = turned[B * g : B * g + B]


def call(kernel, shapes, inputs, scratch=(), grant=8, extra=(), aliases={}, hbm_in=(), hbm_out=()):
    return pl.pallas_call(
        kernel,
        out_shape=[
            s if hasattr(s, "dtype") else jax.ShapeDtypeStruct(s, jnp.float32) for s in shapes
        ],
        in_specs=[HBM if n in hbm_in else VMEM for n in range(len(inputs))],
        out_specs=[HBM if n in hbm_out else VMEM for n in range(len(shapes))],
        scratch_shapes=[pltpu.VMEM(s, jnp.float32) for s in scratch] + list(extra),
        input_output_aliases=aliases,
        compiler_params=pltpu.CompilerParams(vmem_limit_bytes=int(grant * 1024 * 1024)),
    )(*inputs)


def program(phases, mobility, active, variants):
    count = lax.axis_size("space")

    def pairs(first):
        forward = [(i, i + 1) for i in range(first, count - 1, 2)]
        return forward + [(b, a) for a, b in forward]

    def exchange(to_near, to_far):
        far = lax.ppermute(to_far, "space", pairs(1))
        near = lax.ppermute(to_near, "space", pairs(0))
        return near, far

    def swap(array):
        return lax.ppermute(array, "slab", [(0, 1), (1, 0)])

    ph = jnp.transpose(phases, (1, 2, 0, 3))
    rates = mobility[:, None] * active[0, 0].T.astype(jnp.float32)
    to_near, to_far, to_other, speed = call(
        pack_kernel, [(H * B + 1, F, K)] * 3 + [(F, K)], [ph, rates], grant=4
    )
    across = swap(to_other)
    near, far = exchange(to_near, to_far)
    block = (B + 2 * H, W + 2, F, K)
    coefs = (B, 4 * B, K)
    message = (4 * B + 16, K)
    products = jax.ShapeDtypeStruct((12 * B, 3 * B * F), jnp.bfloat16)
    first, second, evolved, coef, mix, e_near, e_far = call(
        relax_inner_kernel,
        [block, block, (B, B, F, K), coefs, products, message, message],
        [ph, speed, across, variants.T],
        [(3, 2, F, K), (B - 6, B, F, K)],
        grant=4,
        extra=[pltpu.SemaphoreType.DMA((B - 6,))],
        hbm_out=(2,),
    )
    e_near, e_far = exchange(e_near, e_far)
    oe_near, oe_far = swap(e_near), swap(e_far)
    message = (4 * B * H, K)
    corners = swap(jnp.concatenate([near[:REST], far[:REST]]))
    first, second, evolved, coef, to_near, to_far = call(
        relax_outer_kernel,
        [block, block, (B, B, F, K), coefs, message, message],
        [near, far, corners, speed, across, mix, first, second, evolved, coef],
        [(3, 2, F, K), (2 * H, B, F, K)],
        grant=4,
        aliases={6: 0, 7: 1, 8: 2, 9: 3},
        extra=[pltpu.SemaphoreType.DMA((2 * H,))],
        hbm_in=(8,),
        hbm_out=(2,),
    )
    o_coef = swap(coef)
    near, far = exchange(to_near, to_far)
    shapes = [(N, J, K), (N, 2 * B, K)] + [(N, J, K)] * 8 + [(3, N, J, K)] * 2 + [(3, B, J, K)]
    state = call(solve_inner_kernel, shapes, [coef, o_coef], grant=4)
    packed = call(
        solve_outer_kernel,
        shapes + [(K // 3 * B, 128)],
        [near, far, swap(near), swap(far), e_near, e_far, oe_near, oe_far, *state],
        [(B // 3, 128, K)],
        grant=8,
        aliases={8 + n: n for n in range(13)},
    )[-1]
    packed = packed.reshape(count, 1, B * 128)
    arrived = lax.all_to_all(packed, "space", 0, 0, tiled=True)
    (displacement,) = call(
        unpack_kernel, [(3, K // count, B, count * B)], [arrived.reshape(count * B, 128)]
    )
    return jnp.transpose(evolved, (2, 0, 1, 3)), displacement


def solution(mesh):
    placed = (P(None, "space", "slab", None), P(), P("space", "slab", None, None), P())
    return jax.shard_map(
        program,
        mesh=mesh,
        in_specs=placed,
        out_specs=(P(None, "space", "slab", None), P(None, "space", "slab", None)),
        check_vma=False,
    )
```

```python
import jax
import jax.numpy as jnp
from jax import lax
from jax.experimental import pallas as pl
from jax.experimental.pallas import tpu as pltpu
from jax.sharding import PartitionSpec as P


ITERS = 4
DIAGONAL_SHIFT = 3.0
SPECTRUM_CENTRE = 12.0
SPECTRUM_RADIUS = 9.0

B = 12
F = 8
K = 384
H = 3
W = B + H
REST = H * H + 1
GO = ITERS + 1
HIGHEST = lax.Precision.HIGHEST
VMEM = pl.BlockSpec(memory_space=pltpu.VMEM)
HBM = pl.BlockSpec(memory_space=pltpu.HBM)


def roll(x, shift, axis):
    return pltpu.roll(x, shift % x.shape[axis], axis)


def parity():
    even = 1 - lax.axis_index("space") % 2
    return even, 1 - even


def pack_kernel(ph, rates, to_near, to_far, to_other, speed_out):
    even, odd = parity()
    slab = lax.axis_index("slab")
    start = (B - H) * (1 - slab)
    for message, top in ((to_far, odd), (to_near, even)):
        for t in range(H):
            source = ph.at[(B - H) * top + t]
            message[H * t : H * (t + 1)] = source[pl.ds(start, H)]
            rest = REST + (B - H) * t
            message[rest : rest + B - H] = source[pl.ds(H * slab, B - H)]
    for i in range(B):
        to_other[H * i : H * (i + 1)] = ph[i, pl.ds(start, H)]
    bricks = K // B
    brick = lax.broadcasted_iota(jnp.int32, (bricks, K), 0)
    spread = jnp.where(brick == lax.broadcasted_iota(jnp.int32, (bricks, K), 1) // B, 1.0, 0.0)
    speed = jnp.dot(
        rates[...], spread, precision=HIGHEST, preferred_element_type=jnp.float32
    )
    to_near[REST - 1] = speed
    to_far[REST - 1] = speed
    to_other[H * B] = speed
    speed_out[...] = speed


def update(x, around, s):
    lane = lax.broadcasted_iota(jnp.int32, (F, K), 1)
    square = x * x
    total = square + roll(square, 4, 0)
    total = total + roll(total, 2, 0)
    total = total + roll(total, 1, 0)
    left = jnp.where(lane == 0, 0.0, roll(x, 1, 1))
    right = jnp.where(lane == K - 1, 0.0, roll(x, -1, 1))
    summed = around + (left + right)
    return x - s * (x * (5.0 + 3.0 * total - 2.0 * square) - summed)


def window_step(src, dst, speed, depth, count, place, static=False):
    slab = lax.axis_index("slab")

    def plane(n):
        a = place(n)
        group = (a >= H) * 1 + (a >= H + B) * 1
        edge = depth * slab
        before = src[a, edge]
        x = src[a, edge + 1]
        for w in range(W - depth):
            after = src[a, edge + w + 2]
            whose = slab if w < H - depth else (1 - slab if w >= B else 0)
            around = (before + after) + (src[a - 1, edge + w + 1] + src[a + 1, edge + w + 1])
            dst[a, edge + w + 1] = update(x, around, speed[group, whose])
            before, x = x, after

    loop(0, count, plane, static)


def halves(x):
    high = x.astype(jnp.bfloat16)
    return high, (x - high.astype(jnp.float32)).astype(jnp.bfloat16)


def last_step(src, own_speed, mix, ev, coef, count, place, staged, sems, static=False):
    own = 1 + H * lax.axis_index("slab")
    row = lax.broadcasted_iota(jnp.int32, (4 * B, K), 0)
    is_excess = (row >= B) & (row < 2 * B)

    def plane(n):
        a = place(n)
        before = src[a, own - 1]
        x = src[a, own]
        for j in range(B):
            after = src[a, own + j + 1]
            around = (before + after) + (src[a - 1, own + j] + src[a + 1, own + j])
            staged[n, j] = update(x, around, own_speed[...])
            before, x = x, after
        pltpu.make_async_copy(staged.at[n], ev.at[a - H], sems.at[n]).start()

    loop(0, count, plane, static)
    for n in range(count):
        values = staged[n].reshape(B * F, K)
        high, low = halves(values * values)
        mixed = jnp.dot(
            mix[...],
            jnp.concatenate([high, low, high], 0),
            preferred_element_type=jnp.float32,
        )
        total = mixed[: 4 * B]
        strain = mixed[4 * B : 8 * B]
        dilation = mixed[8 * B :]
        saturation = total / (1.0 + total)
        excess = 0.5 * saturation
        stress = (1.5 + saturation) * dilation + 2.0 * (1.0 + excess) * strain
        coef[place(n) - H] = jnp.where(is_excess, excess, stress)

    def settle(n, _):
        pltpu.make_async_copy(staged.at[n], ev.at[place(n) - H], sems.at[n]).wait()
        return 0

    lax.fori_loop(0, count, settle, 0)


def relax_inner_kernel(
    ph, mine, across, variants, first, second, ev, coef, mix, e_near, e_far, speed, staged, sems
):
    slab = lax.axis_index("slab")
    own = 1 + H * slab
    other = 1 + B * (1 - slab)
    zero = jnp.zeros((F, K), jnp.float32)
    speed[1, 0] = mine[...]
    speed[1, 1] = across[H * B]

    v = variants[...]
    each = jnp.concatenate([v[:1], jnp.zeros((1, F)), v[1:]], 0)
    whole = jnp.broadcast_to(v[:1] + v[1:2] + v[2:], (4, F))
    table = jnp.concatenate([jnp.ones((4, F)), each, whole], 0)
    shape = (12 * B, B * F)
    group = lax.broadcasted_iota(jnp.int32, (12 * B, 12), 0) // B
    down = jnp.where(group == lax.broadcasted_iota(jnp.int32, (12 * B, 12), 1), 1.0, 0.0)
    field = lax.broadcasted_iota(jnp.int32, (F, B * F), 1) % F
    along = jnp.where(field == lax.broadcasted_iota(jnp.int32, (F, B * F), 0), 1.0, 0.0)
    table = jnp.dot(down, table, precision=HIGHEST, preferred_element_type=jnp.float32)
    table = jnp.dot(table, along, precision=HIGHEST, preferred_element_type=jnp.float32)
    same = lax.broadcasted_iota(jnp.int32, shape, 0) % B
    same = same == lax.broadcasted_iota(jnp.int32, shape, 1) // F
    high, low = halves(jnp.where(same, table, 0.0))
    mix[...] = jnp.concatenate([high, high, low], 1)

    def clear(a, _):
        for buf in (first, second):
            buf[a, 0] = zero
            buf[a, W + 1] = zero
        return 0

    lax.fori_loop(0, B + 2 * H, clear, 0)

    def fill(i, _):
        for j in range(B):
            first[H + i, own + j] = ph[i, j]
        for t in range(H):
            first[H + i, other + t] = across[H * i + t]
        return 0

    lax.fori_loop(0, B, fill, 0)
    window_step(first, second, speed, 1, B - 2, lambda n: H + 1 + n)
    window_step(second, first, speed, 2, B - 4, lambda n: H + 2 + n)
    last_step(first, speed.at[1, 0], mix, ev, coef, B - 6, lambda n: H + 3 + n, staged, sems)
    even, odd = parity()
    for message, top in ((e_near, even), (e_far, odd)):
        message[: 4 * B] = coef[H + (B - 2 * H - 1) * top]
        message[4 * B :] = coef[H + 1 + (B - 2 * H - 3) * top, :16]


def relax_outer_kernel(
    near, far, corners, mine, across, mix, first_in, second_in, ev_in, coef_in,
    first, second, ev, coef, m_near, m_far, speed, staged, sems,
):
    even, odd = parity()
    slab = lax.axis_index("slab")
    own = 1 + H * slab
    other = 1 + B * (1 - slab)
    speed[1, 0] = mine[...]
    speed[1, 1] = across[H * B]
    for halo, at, top in ((near, 0, even), (far, REST, odd)):
        speed[2 * top, 0] = halo[REST - 1]
        speed[2 * top, 1] = corners[at + REST - 1]
        for a in range(H):
            for t in range(H):
                first[(H + B) * top + a, own + (B - H) * (1 - slab) + t] = halo[H * a + t]
                first[(H + B) * top + a, other + t] = corners[at + H * a + t]
            for m in range(B - H):
                first[(H + B) * top + a, own + H * slab + m] = halo[REST + (B - H) * a + m]

    def ends(depth):
        jump = B + H - 2 * depth - 1
        return lambda n: depth + n + (jump + 1 - H) * (n >= H)

    window_step(first, second, speed, 1, 2 * H, ends(1), True)
    window_step(second, first, speed, 2, 2 * H, ends(2), True)
    last_step(first, speed.at[1, 0], mix, ev, coef, 2 * H, ends(3), staged, sems, True)
    for message, top in ((m_near, even), (m_far, odd)):
        for t in range(H):
            message[4 * B * t : 4 * B * (t + 1)] = coef[(B - H) * top + t]


J = B + ITERS
N = B + 2 * GO


def ratios():
    ratio = SPECTRUM_RADIUS / SPECTRUM_CENTRE
    out = []
    for _ in range(ITERS):
        ratio_next = 1.0 / (2.0 * SPECTRUM_CENTRE / SPECTRUM_RADIUS - ratio)
        out.append((ratio_next * ratio, 2.0 * ratio_next / SPECTRUM_RADIUS))
        ratio = ratio_next
    return out


def joined(mine, others):
    bottom = lax.axis_index("slab") == 0
    lo = jnp.where(bottom, mine, others)
    hi = jnp.where(bottom, others, mine)
    n = mine.shape[0] // B
    return [jnp.concatenate([lo[B * c : B * c + B], hi[B * c : B * c + B]], 0) for c in range(n)]


class Solver:
    def __init__(self, state):
        self.s0, self.s1, self.s2, self.ex = state[:4]
        self.dia, self.wi, self.wjp, self.wjm, self.wkp, self.wkm = state[4:10]
        self.even, self.odd, self.sol = state[10:]
        self.row = lax.broadcasted_iota(jnp.int32, (J, K), 0)
        self.lane = lax.broadcasted_iota(jnp.int32, (J, K), 1)

    def window(self, x):
        return jnp.where(lax.axis_index("slab") == 0, x[:J], x[2 * B - J :])

    def put(self, a, mine, others):
        s0, ex, s1, s2 = joined(mine, others)
        self.s1[a] = s1
        self.s0[a], self.ex[a], self.s2[a] = self.window(s0), self.window(ex), self.window(s2)

    def next_j(self, x):
        return jnp.where(self.row == J - 1, 0.0, roll(x, -1, 0))

    def last_j(self, x):
        return jnp.where(self.row == 0, 0.0, roll(x, 1, 0))

    def next_k(self, x):
        return jnp.where(self.lane == K - 1, 0.0, roll(x, -1, 1))

    def last_k(self, x):
        return jnp.where(self.lane == 0, 0.0, roll(x, 1, 1))

    def force(self, a):
        s1 = self.s1[a]
        row = lax.broadcasted_iota(jnp.int32, (2 * B, K), 0)
        ahead = jnp.where(row == 2 * B - 1, 0.0, roll(s1, -1, 0))
        behind = jnp.where(row == 0, 0.0, roll(s1, 1, 0))
        forcing = (
            0.5 * (self.s0[a + 1] - self.s0[a - 1]),
            0.5 * self.window(ahead - behind),
            0.5 * (self.next_k(self.s2[a]) - self.last_k(self.s2[a])),
        )
        for c in range(3):
            self.even[c, a] = forcing[c] / SPECTRUM_CENTRE

    def weigh(self, a):
        e = self.ex[a]
        i_next = 1.0 + 0.5 * (e + self.ex[a + 1])
        i_last = 1.0 + 0.5 * (e + self.ex[a - 1])
        j_next = 1.0 + 0.5 * (e + self.next_j(e))
        j_last = 1.0 + 0.5 * (e + self.last_j(e))
        k_next = 1.0 + 0.5 * (e + self.next_k(e))
        k_last = 1.0 + 0.5 * (e + self.last_k(e))
        ends = (i_next + i_last) + (j_next + j_last) + (k_next + k_last)
        self.dia[a] = DIAGONAL_SHIFT + ends
        self.wi[a] = i_next
        self.wjp[a] = jnp.where(self.row == J - 1, 0.0, j_next)
        self.wjm[a] = jnp.where(self.row == 0, 0.0, j_last)
        self.wkp[a] = jnp.where(self.lane == K - 1, 0.0, k_next)
        self.wkm[a] = jnp.where(self.lane == 0, 0.0, k_last)

    def buffers(self, t):
        return (self.even, self.odd) if t % 2 == 0 else (self.odd, self.even)

    def advance(self, t, a):
        keep, gain = ratios()[t]
        if t == 0:
            now, past = keep + SPECTRUM_CENTRE * gain, 0.0
        else:
            keep_past, gain_past = ratios()[t - 1]
            now, past = keep + gain / gain_past, gain * keep_past / gain_past
        src, dst = self.buffers(t)
        centre = now - gain * self.dia[a]
        out = []
        for c in range(3):
            v = src[c, a]
            side = self.wi[a] * src[c, a + 1] + self.wi[a - 1] * src[c, a - 1]
            side = side + (self.wjp[a] * roll(v, -1, 0) + self.wjm[a] * roll(v, 1, 0))
            side = side + (self.wkp[a] * roll(v, -1, 1) + self.wkm[a] * roll(v, 1, 1))
            new = centre * v + gain * side
            out.append((v, new - past * dst[c, a] if t else new))
        return out

    def iterate(self, t, start, stop, static=False):
        dst = self.buffers(t)[1]

        def plane(a, inner):
            for c, (v, new) in enumerate(self.advance(t, a)):
                dst[c, a] = new
                if inner:
                    self.sol[c, a - GO] = v if t == 0 else self.sol[c, a - GO] + v

        low, high = min(max(start, GO), stop), max(min(stop, GO + B), start)
        loop(start, low, lambda a: plane(a, False), static)
        loop(low, high, lambda a: plane(a, True), static)
        loop(high, stop, lambda a: plane(a, False), static)


def loop(start, stop, body, static=False):
    if static:
        for a in range(start, stop):
            body(a)
    elif start < stop:
        lax.fori_loop(start, stop, lambda a, _: (body(a), 0)[1], 0)


def solve_inner_kernel(coef, o_coef, *state):
    solver = Solver(state)
    loop(0, B, lambda i: solver.put(i + GO, coef[i], o_coef[i]))
    loop(GO + 1, GO + B - 1, solver.force, True)
    loop(GO + 1, GO + B - 1, solver.weigh, True)
    for t in range(ITERS - 1):
        solver.iterate(t, GO + 2 + t, GO + B - 2 - t, True)


def solve_outer_kernel(near, far, o_near, o_far, e_near, e_far, oe_near, oe_far, *refs):
    state = refs[13:26]
    out, rows = refs[26:]
    solver = Solver(state)
    even, odd = parity()
    place = lax.axis_index("space")
    bottom = lax.axis_index("slab") == 0
    sides = (
        (near, o_near, e_near, oe_near, even),
        (far, o_far, e_far, oe_far, odd),
    )
    for halo, others, early, others_early, top in sides:
        for t in range(H):
            part = slice(4 * B * t, 4 * B * (t + 1))
            solver.put(2 + t + (GO + B - 2) * top, halo[part], others[part])
        whole, tail = slice(0, 4 * B), slice(4 * B, 4 * B + 16)
        solver.put(1 + (N - 3) * top, early[whole], others_early[whole])
        solver.s0[(N - 1) * top] = solver.window(joined(early[tail], others_early[tail])[0])

    loop(1, GO + 1, solver.force, True)
    loop(GO + B - 1, N - 1, solver.force, True)
    solver.wi[1] = 1.0 + 0.5 * (solver.ex[1] + solver.ex[2])
    loop(2, GO + 1, solver.weigh, True)
    loop(GO + B - 1, N - 2, solver.weigh, True)

    @pl.when(place == 0)
    def _():
        solver.wi[GO - 1] = jnp.zeros((J, K), jnp.float32)

    @pl.when(place == lax.axis_size("space") - 1)
    def _():
        solver.wi[GO + B - 1] = jnp.zeros((J, K), jnp.float32)

    for t in range(ITERS - 1):
        solver.iterate(t, 2 + t, GO + 2 + t, True)
        solver.iterate(t, GO + B - 2 - t, N - 2 - t, True)

    target = 3 * lax.broadcasted_iota(jnp.int32, (K // 3, K), 0)
    source = lax.broadcasted_iota(jnp.int32, (K // 3, K), 1)
    picks = [jnp.where(source == target + q, 1.0, 0.0).astype(jnp.bfloat16) for q in range(3)]
    picks = [jnp.concatenate([pick, pick], 1) for pick in picks]
    for g in range(B // 3):
        rows[g, 9 * B :] = jnp.zeros((128 - 9 * B, K), jnp.float32)

    def finish(g):
        for p in range(3):
            i = 3 * g + p
            for c, (v, new) in enumerate(solver.advance(ITERS - 1, i + GO)):
                total = solver.sol[c, i] + v + new
                mine = jnp.where(bottom, total[:B], total[J - B :])
                at = B * (3 * p + c)
                rows[g, at : at + B] = mine

    loop(0, B // 3, finish, True)
    lane = lax.broadcasted_iota(jnp.int32, (K // 3, 128), 1)
    for g in range(B // 3):
        both = jnp.concatenate(halves(rows[g]), 1)
        parts = [
            lax.dot_general(
                pick, both, (((1,), (1,)), ((), ())), preferred_element_type=jnp.float32
            )
            for pick in picks
        ]
        for p in range(3):
            moved = [
                part if q == p else roll(part, 3 * B * (q - p), 1) for q, part in enumerate(parts)
            ]
            value = jnp.where(lane < 6 * B, jnp.where(lane < 3 * B, moved[0], moved[1]), moved[2])
            out[pl.ds(3 * g + p, K // 3, stride=B), :] = value


def unpack_kernel(got, out):
    for t in range(got.shape[0] // 128):
        turned = got[128 * t : 128 * (t + 1), :].T
        for c in range(3):
            for q in range(3):
                g = 3 * q + c
                out[c, q, :, 128 * t : 128 * (t + 1)] = turned[B * g : B * g + B]


def call(kernel, shapes, inputs, scratch=(), grant=8, extra=(), aliases={}, hbm_in=(), hbm_out=()):
    return pl.pallas_call(
        kernel,
        out_shape=[
            s if hasattr(s, "dtype") else jax.ShapeDtypeStruct(s, jnp.float32) for s in shapes
        ],
        in_specs=[HBM if n in hbm_in else VMEM for n in range(len(inputs))],
        out_specs=[HBM if n in hbm_out else VMEM for n in range(len(shapes))],
        scratch_shapes=[pltpu.VMEM(s, jnp.float32) for s in scratch] + list(extra),
        input_output_aliases=aliases,
        compiler_params=pltpu.CompilerParams(vmem_limit_bytes=int(grant * 1024 * 1024)),
    )(*inputs)


def program(phases, mobility, active, variants):
    count = lax.axis_size("space")

    def pairs(first):
        forward = [(i, i + 1) for i in range(first, count - 1, 2)]
        return forward + [(b, a) for a, b in forward]

    def exchange(to_near, to_far):
        far = lax.ppermute(to_far, "space", pairs(1))
        near = lax.ppermute(to_near, "space", pairs(0))
        return near, far

    def swap(array):
        return lax.ppermute(array, "slab", [(0, 1), (1, 0)])

    ph = jnp.transpose(phases, (1, 2, 0, 3))
    rates = mobility[:, None] * active[0, 0].T.astype(jnp.float32)
    to_near, to_far, to_other, speed = call(
        pack_kernel, [(H * B + 1, F, K)] * 3 + [(F, K)], [ph, rates], grant=4
    )
    across = swap(to_other)
    near, far = exchange(to_near, to_far)
    block = (B + 2 * H, W + 2, F, K)
    coefs = (B, 4 * B, K)
    message = (4 * B + 16, K)
    products = jax.ShapeDtypeStruct((12 * B, 3 * B * F), jnp.bfloat16)
    first, second, evolved, coef, mix, e_near, e_far = call(
        relax_inner_kernel,
        [block, block, (B, B, F, K), coefs, products, message, message],
        [ph, speed, across, variants.T],
        [(3, 2, F, K), (B - 6, B, F, K)],
        grant=4,
        extra=[pltpu.SemaphoreType.DMA((B - 6,))],
        hbm_out=(2,),
    )
    e_near, e_far = exchange(e_near, e_far)
    oe_near, oe_far = swap(e_near), swap(e_far)
    message = (4 * B * H, K)
    corners = swap(jnp.concatenate([near[:REST], far[:REST]]))
    first, second, evolved, coef, to_near, to_far = call(
        relax_outer_kernel,
        [block, block, (B, B, F, K), coefs, message, message],
        [near, far, corners, speed, across, mix, first, second, evolved, coef],
        [(3, 2, F, K), (2 * H, B, F, K)],
        grant=4,
        aliases={6: 0, 7: 1, 8: 2, 9: 3},
        extra=[pltpu.SemaphoreType.DMA((2 * H,))],
        hbm_in=(8,),
        hbm_out=(2,),
    )
    o_coef = swap(coef)
    near, far = exchange(to_near, to_far)
    shapes = [(N, J, K), (N, 2 * B, K)] + [(N, J, K)] * 8 + [(3, N, J, K)] * 2 + [(3, B, J, K)]
    state = call(solve_inner_kernel, shapes, [coef, o_coef], grant=4)
    packed = call(
        solve_outer_kernel,
        shapes + [(K // 3 * B, 128)],
        [near, far, swap(near), swap(far), e_near, e_far, oe_near, oe_far, *state],
        [(B // 3, 128, K)],
        grant=8,
        aliases={8 + n: n for n in range(13)},
    )[-1]
    packed = packed.reshape(count, 1, B * 128)
    arrived = lax.all_to_all(packed, "space", 0, 0, tiled=True)
    (displacement,) = call(
        unpack_kernel, [(3, K // count, B, count * B)], [arrived.reshape(count * B, 128)]
    )
    return jnp.transpose(evolved, (2, 0, 1, 3)), displacement


def solution(mesh):
    placed = (P(None, "space", "slab", None), P(), P("space", "slab", None, None), P())
    return jax.shard_map(
        program,
        mesh=mesh,
        in_specs=placed,
        out_specs=(P(None, "space", "slab", None), P(None, "space", "slab", None)),
        check_vma=False,
    )
```

```python
import jax
import jax.numpy as jnp
from jax import lax
from jax.experimental import pallas as pl
from jax.experimental.pallas import tpu as pltpu
from jax.sharding import PartitionSpec as P


ITERS = 4
DIAGONAL_SHIFT = 3.0
SPECTRUM_CENTRE = 12.0
SPECTRUM_RADIUS = 9.0

B = 12
F = 8
K = 384
H = 3
W = B + H
REST = H * H + 1
GO = ITERS + 1
HIGHEST = lax.Precision.HIGHEST
VMEM = pl.BlockSpec(memory_space=pltpu.VMEM)
HBM = pl.BlockSpec(memory_space=pltpu.HBM)


def roll(x, shift, axis):
    return pltpu.roll(x, shift % x.shape[axis], axis)


def parity():
    even = 1 - lax.axis_index("space") % 2
    return even, 1 - even


def pack_kernel(ph, rates, to_near, to_far, to_other, speed_out):
    even, odd = parity()
    slab = lax.axis_index("slab")
    start = (B - H) * (1 - slab)
    for message, top in ((to_far, odd), (to_near, even)):
        for t in range(H):
            source = ph.at[(B - H) * top + t]
            message[H * t : H * (t + 1)] = source[pl.ds(start, H)]
            rest = REST + (B - H) * t
            message[rest : rest + B - H] = source[pl.ds(H * slab, B - H)]
    for i in range(B):
        to_other[H * i : H * (i + 1)] = ph[i, pl.ds(start, H)]
    bricks = K // B
    brick = lax.broadcasted_iota(jnp.int32, (bricks, K), 0)
    spread = jnp.where(brick == lax.broadcasted_iota(jnp.int32, (bricks, K), 1) // B, 1.0, 0.0)
    speed = jnp.dot(
        rates[...], spread, precision=HIGHEST, preferred_element_type=jnp.float32
    )
    to_near[REST - 1] = speed
    to_far[REST - 1] = speed
    to_other[H * B] = speed
    speed_out[...] = speed


def update(x, around, s):
    lane = lax.broadcasted_iota(jnp.int32, (F, K), 1)
    square = x * x
    total = square + roll(square, 4, 0)
    total = total + roll(total, 2, 0)
    total = total + roll(total, 1, 0)
    left = jnp.where(lane == 0, 0.0, roll(x, 1, 1))
    right = jnp.where(lane == K - 1, 0.0, roll(x, -1, 1))
    summed = around + (left + right)
    return x - s * (x * (5.0 + 3.0 * total - 2.0 * square) - summed)


def window_step(src, dst, speed, depth, count, place, static=False):
    slab = lax.axis_index("slab")

    def plane(n):
        a = place(n)
        group = (a >= H) * 1 + (a >= H + B) * 1
        edge = depth * slab
        before = src[a, edge]
        x = src[a, edge + 1]
        for w in range(W - depth):
            after = src[a, edge + w + 2]
            whose = slab if w < H - depth else (1 - slab if w >= B else 0)
            around = (before + after) + (src[a - 1, edge + w + 1] + src[a + 1, edge + w + 1])
            dst[a, edge + w + 1] = update(x, around, speed[group, whose])
            before, x = x, after

    loop(0, count, plane, static)


def halves(x):
    high = x.astype(jnp.bfloat16)
    return high, (x - high.astype(jnp.float32)).astype(jnp.bfloat16)


def last_step(src, own_speed, mix, ev, coef, count, place, staged, sems, static=False):
    own = 1 + H * lax.axis_index("slab")
    row = lax.broadcasted_iota(jnp.int32, (4 * B, K), 0)
    is_excess = (row >= B) & (row < 2 * B)

    def plane(n):
        a = place(n)
        before = src[a, own - 1]
        x = src[a, own]
        for j in range(B):
            after = src[a, own + j + 1]
            around = (before + after) + (src[a - 1, own + j] + src[a + 1, own + j])
            staged[n, j] = update(x, around, own_speed[...])
            before, x = x, after
        pltpu.make_async_copy(staged.at[n], ev.at[a - H], sems.at[n]).start()

    loop(0, count, plane, static)
    for n in range(count):
        values = staged[n].reshape(B * F, K)
        high, low = halves(values * values)
        mixed = jnp.dot(
            mix[...],
            jnp.concatenate([high, low, high], 0),
            preferred_element_type=jnp.float32,
        )
        total = mixed[: 4 * B]
        strain = mixed[4 * B : 8 * B]
        dilation = mixed[8 * B :]
        saturation = total / (1.0 + total)
        excess = 0.5 * saturation
        stress = (1.5 + saturation) * dilation + 2.0 * (1.0 + excess) * strain
        coef[place(n) - H] = jnp.where(is_excess, excess, stress)

    def settle(n, _):
        pltpu.make_async_copy(staged.at[n], ev.at[place(n) - H], sems.at[n]).wait()
        return 0

    lax.fori_loop(0, count, settle, 0)


def relax_inner_kernel(
    ph, mine, across, variants, first, second, ev, coef, mix, e_near, e_far, speed, staged, sems
):
    slab = lax.axis_index("slab")
    own = 1 + H * slab
    other = 1 + B * (1 - slab)
    zero = jnp.zeros((F, K), jnp.float32)
    speed[1, 0] = mine[...]
    speed[1, 1] = across[H * B]

    v = variants[...]
    each = jnp.concatenate([v[:1], jnp.zeros((1, F)), v[1:]], 0)
    whole = jnp.broadcast_to(v[:1] + v[1:2] + v[2:], (4, F))
    table = jnp.concatenate([jnp.ones((4, F)), each, whole], 0)
    shape = (12 * B, B * F)
    group = lax.broadcasted_iota(jnp.int32, (12 * B, 12), 0) // B
    down = jnp.where(group == lax.broadcasted_iota(jnp.int32, (12 * B, 12), 1), 1.0, 0.0)
    field = lax.broadcasted_iota(jnp.int32, (F, B * F), 1) % F
    along = jnp.where(field == lax.broadcasted_iota(jnp.int32, (F, B * F), 0), 1.0, 0.0)
    table = jnp.dot(down, table, precision=HIGHEST, preferred_element_type=jnp.float32)
    table = jnp.dot(table, along, precision=HIGHEST, preferred_element_type=jnp.float32)
    same = lax.broadcasted_iota(jnp.int32, shape, 0) % B
    same = same == lax.broadcasted_iota(jnp.int32, shape, 1) // F
    high, low = halves(jnp.where(same, table, 0.0))
    mix[...] = jnp.concatenate([high, high, low], 1)

    def clear(a, _):
        for buf in (first, second):
            buf[a, 0] = zero
            buf[a, W + 1] = zero
        return 0

    lax.fori_loop(0, B + 2 * H, clear, 0)

    def fill(i, _):
        for j in range(B):
            first[H + i, own + j] = ph[i, j]
        for t in range(H):
            first[H + i, other + t] = across[H * i + t]
        return 0

    lax.fori_loop(0, B, fill, 0)
    window_step(first, second, speed, 1, B - 2, lambda n: H + 1 + n, True)
    window_step(second, first, speed, 2, B - 4, lambda n: H + 2 + n, True)
    last_step(first, speed.at[1, 0], mix, ev, coef, B - 6, lambda n: H + 3 + n, staged, sems, True)
    even, odd = parity()
    for message, top in ((e_near, even), (e_far, odd)):
        message[: 4 * B] = coef[H + (B - 2 * H - 1) * top]
        message[4 * B :] = coef[H + 1 + (B - 2 * H - 3) * top, :16]


def relax_outer_kernel(
    near, far, corners, mine, across, mix, first_in, second_in, ev_in, coef_in,
    first, second, ev, coef, m_near, m_far, speed, staged, sems,
):
    even, odd = parity()
    slab = lax.axis_index("slab")
    own = 1 + H * slab
    other = 1 + B * (1 - slab)
    speed[1, 0] = mine[...]
    speed[1, 1] = across[H * B]
    for halo, at, top in ((near, 0, even), (far, REST, odd)):
        speed[2 * top, 0] = halo[REST - 1]
        speed[2 * top, 1] = corners[at + REST - 1]
        for a in range(H):
            for t in range(H):
                first[(H + B) * top + a, own + (B - H) * (1 - slab) + t] = halo[H * a + t]
                first[(H + B) * top + a, other + t] = corners[at + H * a + t]
            for m in range(B - H):
                first[(H + B) * top + a, own + H * slab + m] = halo[REST + (B - H) * a + m]

    def ends(depth):
        jump = B + H - 2 * depth - 1
        return lambda n: depth + n + (jump + 1 - H) * (n >= H)

    window_step(first, second, speed, 1, 2 * H, ends(1), True)
    window_step(second, first, speed, 2, 2 * H, ends(2), True)
    last_step(first, speed.at[1, 0], mix, ev, coef, 2 * H, ends(3), staged, sems, True)
    for message, top in ((m_near, even), (m_far, odd)):
        for t in range(H):
            message[4 * B * t : 4 * B * (t + 1)] = coef[(B - H) * top + t]


J = B + ITERS
N = B + 2 * GO


def ratios():
    ratio = SPECTRUM_RADIUS / SPECTRUM_CENTRE
    out = []
    for _ in range(ITERS):
        ratio_next = 1.0 / (2.0 * SPECTRUM_CENTRE / SPECTRUM_RADIUS - ratio)
        out.append((ratio_next * ratio, 2.0 * ratio_next / SPECTRUM_RADIUS))
        ratio = ratio_next
    return out


def joined(mine, others):
    bottom = lax.axis_index("slab") == 0
    lo = jnp.where(bottom, mine, others)
    hi = jnp.where(bottom, others, mine)
    n = mine.shape[0] // B
    return [jnp.concatenate([lo[B * c : B * c + B], hi[B * c : B * c + B]], 0) for c in range(n)]


class Solver:
    def __init__(self, state):
        self.s0, self.s1, self.s2, self.ex = state[:4]
        self.dia, self.wi, self.wjp, self.wjm, self.wkp, self.wkm = state[4:10]
        self.even, self.odd, self.sol = state[10:]
        self.row = lax.broadcasted_iota(jnp.int32, (J, K), 0)
        self.lane = lax.broadcasted_iota(jnp.int32, (J, K), 1)

    def window(self, x):
        return jnp.where(lax.axis_index("slab") == 0, x[:J], x[2 * B - J :])

    def put(self, a, mine, others):
        s0, ex, s1, s2 = joined(mine, others)
        self.s1[a] = s1
        self.s0[a], self.ex[a], self.s2[a] = self.window(s0), self.window(ex), self.window(s2)

    def next_j(self, x):
        return jnp.where(self.row == J - 1, 0.0, roll(x, -1, 0))

    def last_j(self, x):
        return jnp.where(self.row == 0, 0.0, roll(x, 1, 0))

    def next_k(self, x):
        return jnp.where(self.lane == K - 1, 0.0, roll(x, -1, 1))

    def last_k(self, x):
        return jnp.where(self.lane == 0, 0.0, roll(x, 1, 1))

    def force(self, a):
        s1 = self.s1[a]
        row = lax.broadcasted_iota(jnp.int32, (2 * B, K), 0)
        ahead = jnp.where(row == 2 * B - 1, 0.0, roll(s1, -1, 0))
        behind = jnp.where(row == 0, 0.0, roll(s1, 1, 0))
        forcing = (
            0.5 * (self.s0[a + 1] - self.s0[a - 1]),
            0.5 * self.window(ahead - behind),
            0.5 * (self.next_k(self.s2[a]) - self.last_k(self.s2[a])),
        )
        for c in range(3):
            self.even[c, a] = forcing[c] / SPECTRUM_CENTRE

    def weigh(self, a):
        e = self.ex[a]
        i_next = 1.0 + 0.5 * (e + self.ex[a + 1])
        i_last = 1.0 + 0.5 * (e + self.ex[a - 1])
        j_next = 1.0 + 0.5 * (e + self.next_j(e))
        j_last = 1.0 + 0.5 * (e + self.last_j(e))
        k_next = 1.0 + 0.5 * (e + self.next_k(e))
        k_last = 1.0 + 0.5 * (e + self.last_k(e))
        ends = (i_next + i_last) + (j_next + j_last) + (k_next + k_last)
        self.dia[a] = DIAGONAL_SHIFT + ends
        self.wi[a] = i_next
        self.wjp[a] = jnp.where(self.row == J - 1, 0.0, j_next)
        self.wjm[a] = jnp.where(self.row == 0, 0.0, j_last)
        self.wkp[a] = jnp.where(self.lane == K - 1, 0.0, k_next)
        self.wkm[a] = jnp.where(self.lane == 0, 0.0, k_last)

    def buffers(self, t):
        return (self.even, self.odd) if t % 2 == 0 else (self.odd, self.even)

    def advance(self, t, a):
        keep, gain = ratios()[t]
        if t == 0:
            now, past = keep + SPECTRUM_CENTRE * gain, 0.0
        else:
            keep_past, gain_past = ratios()[t - 1]
            now, past = keep + gain / gain_past, gain * keep_past / gain_past
        src, dst = self.buffers(t)
        centre = now - gain * self.dia[a]
        out = []
        for c in range(3):
            v = src[c, a]
            side = self.wi[a] * src[c, a + 1] + self.wi[a - 1] * src[c, a - 1]
            side = side + (self.wjp[a] * roll(v, -1, 0) + self.wjm[a] * roll(v, 1, 0))
            side = side + (self.wkp[a] * roll(v, -1, 1) + self.wkm[a] * roll(v, 1, 1))
            new = centre * v + gain * side
            out.append((v, new - past * dst[c, a] if t else new))
        return out

    def iterate(self, t, start, stop, static=False):
        dst = self.buffers(t)[1]

        def plane(a, inner):
            for c, (v, new) in enumerate(self.advance(t, a)):
                dst[c, a] = new
                if inner:
                    self.sol[c, a - GO] = v if t == 0 else self.sol[c, a - GO] + v

        low, high = min(max(start, GO), stop), max(min(stop, GO + B), start)
        loop(start, low, lambda a: plane(a, False), static)
        loop(low, high, lambda a: plane(a, True), static)
        loop(high, stop, lambda a: plane(a, False), static)


def loop(start, stop, body, static=False):
    if static:
        for a in range(start, stop):
            body(a)
    elif start < stop:
        lax.fori_loop(start, stop, lambda a, _: (body(a), 0)[1], 0)


def solve_inner_kernel(coef, o_coef, *state):
    solver = Solver(state)
    loop(0, B, lambda i: solver.put(i + GO, coef[i], o_coef[i]))
    loop(GO + 1, GO + B - 1, solver.force, True)
    loop(GO + 1, GO + B - 1, solver.weigh, True)
    for t in range(ITERS - 1):
        solver.iterate(t, GO + 2 + t, GO + B - 2 - t, True)


def solve_outer_kernel(near, far, o_near, o_far, e_near, e_far, oe_near, oe_far, *refs):
    state = refs[13:26]
    out, rows = refs[26:]
    solver = Solver(state)
    even, odd = parity()
    place = lax.axis_index("space")
    bottom = lax.axis_index("slab") == 0
    sides = (
        (near, o_near, e_near, oe_near, even),
        (far, o_far, e_far, oe_far, odd),
    )
    for halo, others, early, others_early, top in sides:
        for t in range(H):
            part = slice(4 * B * t, 4 * B * (t + 1))
            solver.put(2 + t + (GO + B - 2) * top, halo[part], others[part])
        whole, tail = slice(0, 4 * B), slice(4 * B, 4 * B + 16)
        solver.put(1 + (N - 3) * top, early[whole], others_early[whole])
        solver.s0[(N - 1) * top] = solver.window(joined(early[tail], others_early[tail])[0])

    loop(1, GO + 1, solver.force, True)
    loop(GO + B - 1, N - 1, solver.force, True)
    solver.wi[1] = 1.0 + 0.5 * (solver.ex[1] + solver.ex[2])
    loop(2, GO + 1, solver.weigh, True)
    loop(GO + B - 1, N - 2, solver.weigh, True)

    @pl.when(place == 0)
    def _():
        solver.wi[GO - 1] = jnp.zeros((J, K), jnp.float32)

    @pl.when(place == lax.axis_size("space") - 1)
    def _():
        solver.wi[GO + B - 1] = jnp.zeros((J, K), jnp.float32)

    for t in range(ITERS - 1):
        solver.iterate(t, 2 + t, GO + 2 + t, True)
        solver.iterate(t, GO + B - 2 - t, N - 2 - t, True)

    target = 3 * lax.broadcasted_iota(jnp.int32, (K // 3, K), 0)
    source = lax.broadcasted_iota(jnp.int32, (K // 3, K), 1)
    picks = [jnp.where(source == target + q, 1.0, 0.0).astype(jnp.bfloat16) for q in range(3)]
    picks = [jnp.concatenate([pick, pick], 1) for pick in picks]
    for g in range(B // 3):
        rows[g, 9 * B :] = jnp.zeros((128 - 9 * B, K), jnp.float32)

    def finish(g):
        for p in range(3):
            i = 3 * g + p
            for c, (v, new) in enumerate(solver.advance(ITERS - 1, i + GO)):
                total = solver.sol[c, i] + v + new
                mine = jnp.where(bottom, total[:B], total[J - B :])
                at = B * (3 * p + c)
                rows[g, at : at + B] = mine

    loop(0, B // 3, finish, True)
    lane = lax.broadcasted_iota(jnp.int32, (K // 3, 128), 1)
    for g in range(B // 3):
        both = jnp.concatenate(halves(rows[g]), 1)
        parts = [
            lax.dot_general(
                pick, both, (((1,), (1,)), ((), ())), preferred_element_type=jnp.float32
            )
            for pick in picks
        ]
        for p in range(3):
            moved = [
                part if q == p else roll(part, 3 * B * (q - p), 1) for q, part in enumerate(parts)
            ]
            value = jnp.where(lane < 6 * B, jnp.where(lane < 3 * B, moved[0], moved[1]), moved[2])
            out[pl.ds(3 * g + p, K // 3, stride=B), :] = value


def unpack_kernel(got, out):
    for t in range(got.shape[0] // 128):
        turned = got[128 * t : 128 * (t + 1), :].T
        for c in range(3):
            for q in range(3):
                g = 3 * q + c
                out[c, q, :, 128 * t : 128 * (t + 1)] = turned[B * g : B * g + B]


def call(kernel, shapes, inputs, scratch=(), grant=8, extra=(), aliases={}, hbm_in=(), hbm_out=()):
    return pl.pallas_call(
        kernel,
        out_shape=[
            s if hasattr(s, "dtype") else jax.ShapeDtypeStruct(s, jnp.float32) for s in shapes
        ],
        in_specs=[HBM if n in hbm_in else VMEM for n in range(len(inputs))],
        out_specs=[HBM if n in hbm_out else VMEM for n in range(len(shapes))],
        scratch_shapes=[pltpu.VMEM(s, jnp.float32) for s in scratch] + list(extra),
        input_output_aliases=aliases,
        compiler_params=pltpu.CompilerParams(vmem_limit_bytes=int(grant * 1024 * 1024)),
    )(*inputs)


def program(phases, mobility, active, variants):
    count = lax.axis_size("space")

    def pairs(first):
        forward = [(i, i + 1) for i in range(first, count - 1, 2)]
        return forward + [(b, a) for a, b in forward]

    def exchange(to_near, to_far):
        far = lax.ppermute(to_far, "space", pairs(1))
        near = lax.ppermute(to_near, "space", pairs(0))
        return near, far

    def swap(array):
        return lax.ppermute(array, "slab", [(0, 1), (1, 0)])

    ph = jnp.transpose(phases, (1, 2, 0, 3))
    rates = mobility[:, None] * active[0, 0].T.astype(jnp.float32)
    to_near, to_far, to_other, speed = call(
        pack_kernel, [(H * B + 1, F, K)] * 3 + [(F, K)], [ph, rates], grant=4
    )
    across = swap(to_other)
    near, far = exchange(to_near, to_far)
    block = (B + 2 * H, W + 2, F, K)
    coefs = (B, 4 * B, K)
    message = (4 * B + 16, K)
    products = jax.ShapeDtypeStruct((12 * B, 3 * B * F), jnp.bfloat16)
    first, second, evolved, coef, mix, e_near, e_far = call(
        relax_inner_kernel,
        [block, block, (B, B, F, K), coefs, products, message, message],
        [ph, speed, across, variants.T],
        [(3, 2, F, K), (B - 6, B, F, K)],
        grant=4,
        extra=[pltpu.SemaphoreType.DMA((B - 6,))],
        hbm_out=(2,),
    )
    e_near, e_far = exchange(e_near, e_far)
    oe_near, oe_far = swap(e_near), swap(e_far)
    message = (4 * B * H, K)
    corners = swap(jnp.concatenate([near[:REST], far[:REST]]))
    first, second, evolved, coef, to_near, to_far = call(
        relax_outer_kernel,
        [block, block, (B, B, F, K), coefs, message, message],
        [near, far, corners, speed, across, mix, first, second, evolved, coef],
        [(3, 2, F, K), (2 * H, B, F, K)],
        grant=4,
        aliases={6: 0, 7: 1, 8: 2, 9: 3},
        extra=[pltpu.SemaphoreType.DMA((2 * H,))],
        hbm_in=(8,),
        hbm_out=(2,),
    )
    o_coef = swap(coef)
    near, far = exchange(to_near, to_far)
    shapes = [(N, J, K), (N, 2 * B, K)] + [(N, J, K)] * 8 + [(3, N, J, K)] * 2 + [(3, B, J, K)]
    state = call(solve_inner_kernel, shapes, [coef, o_coef], grant=4)
    packed = call(
        solve_outer_kernel,
        shapes + [(K // 3 * B, 128)],
        [near, far, swap(near), swap(far), e_near, e_far, oe_near, oe_far, *state],
        [(B // 3, 128, K)],
        grant=8,
        aliases={8 + n: n for n in range(13)},
    )[-1]
    packed = packed.reshape(count, 1, B * 128)
    arrived = lax.all_to_all(packed, "space", 0, 0, tiled=True)
    (displacement,) = call(
        unpack_kernel, [(3, K // count, B, count * B)], [arrived.reshape(count * B, 128)]
    )
    return jnp.transpose(evolved, (2, 0, 1, 3)), displacement


def solution(mesh):
    placed = (P(None, "space", "slab", None), P(), P("space", "slab", None, None), P())
    return jax.shard_map(
        program,
        mesh=mesh,
        in_specs=placed,
        out_specs=(P(None, "space", "slab", None), P(None, "space", "slab", None)),
        check_vma=False,
    )
```
